32 devices in a mesh: expert: 8 (over z, x), dp: 4 (over y, core).
Axes of the slice: x: 2, y: 2, z: 4, core: 2. Of those that a mesh axis runs over, the one named last changes fastest.
Arguments:
- sub_inputs: bfloat16 [4096, 4096], P(('expert', 'dp')), may hold values from -6 to 6
- out_grads: bfloat16 [4096, 4096], P(('expert', 'dp')), may hold values from -6 to 6
- expert_outputs: bfloat16 [4096, 4, 2, 1024], P(('expert', 'dp')), may hold values from -6 to 6
- combine_weights: float32 [4096, 4, 2], P(('expert', 'dp')), may hold values from 0.1 to 1
- expert_ids: int32 [4096, 4, 2], P(('expert', 'dp')), may hold values from 0 to 7, as said below
- slot_ids: int32 [4096, 4, 2], P(('expert', 'dp')), may hold values from -1 to 127, as said below
- expert_input_weight: bfloat16 [8, 1024, 1024], P('expert'), may hold values from -0.1875 to 0.1875
- expert_output_weight: bfloat16 [8, 1024, 1024], P('expert'), may hold values from -0.1875 to 0.1875
Outputs:
- d_inputs: bfloat16 [4096, 4096], P(('expert', 'dp'))
- d_gates: float32 [4096, 4, 2], P(('expert', 'dp'))
- dw_in: float32 [8, 1024, 1024], P('expert', 'dp')
- dw_out: float32 [8, 1024, 1024], P('expert', 'dp')
The draws below stay inside these ranges and needn't reach their ends.
Inputs may be any that keep to these rules, and one draw needn't show every extreme that they name: `expert_ids`: the 2 experts of one sub-token differ. `slot_ids`: within the rows of one device, the kept entries that name one expert carry the slots 0, 1, 2, ... each once, so at most 128 of them; in every draw some expert has 128 kept entries from every device.
All inputs are finite; a program needn't handle non-finite values.
Results may differ from the reference program's by a relative error of at most 0.0085.
Values may be sent and summed in bfloat16 or wider, within the bound.
A program may use at most 128 MiB of HBM per device.

```python
import jax
import jax.numpy as jnp
from jax import lax

SUB = 1024
FF = 1024
HEADS = 4
TOP = 2
TOK_DEV = 128
EXPERTS = 8
CAP = 128
TOKENS = 4096
N_DP = 4


def route_tables(key):
    folded = jax.random.fold_in(key, 4111)
    key_hot, key_pick, key_near, key_spread, key_second = jax.random.split(folded, 5)
    hottest = jax.random.randint(key_hot, (), 0, EXPERTS)
    picker = jax.random.randint(key_pick, (TOKENS, HEADS), 0, 4)
    nearby = (hottest + jax.random.randint(key_near, (TOKENS, HEADS), 0, 3)) % EXPERTS
    spread = jax.random.randint(key_spread, (TOKENS, HEADS), 0, EXPERTS)
    first_choice = jnp.where(picker == 0, nearby, spread)
    row_index = (jnp.arange(TOKENS) % TOK_DEV)[:, None] * HEADS + jnp.arange(HEADS)[None, :]
    first_choice = jnp.where(row_index < CAP, hottest, first_choice)
    second_choice = (first_choice + jax.random.randint(key_second, (TOKENS, HEADS), 1, EXPERTS)) % EXPERTS
    routed = jnp.stack([first_choice, second_choice], axis=-1).astype(jnp.int32)
    blocks = TOKENS // TOK_DEV
    ordered = routed.reshape(blocks, TOK_DEV * HEADS, TOP).transpose(0, 2, 1).reshape(blocks, TOP * TOK_DEV * HEADS)

    def block_slots(block_ids):
        onehot = (block_ids[:, None] == jnp.arange(EXPERTS)[None, :]).astype(jnp.int32)
        before = jnp.cumsum(onehot, axis=0) - onehot
        return jnp.sum(before * onehot, axis=1)
    positions = lax.map(block_slots, ordered)
    slot_table = jnp.where(positions < CAP, positions, -1)
    slot_table = slot_table.reshape(blocks, TOP, TOK_DEV * HEADS).transpose(0, 2, 1).reshape(TOKENS, HEADS, TOP)
    return (routed, slot_table.astype(jnp.int32))


def draw_expert_ids(key, part):
    return route_tables(key)[0]


def draw_slot_ids(key, part):
    return route_tables(key)[1]


def level_of(rng, extent, cuts, smallest, largest):
    gain, own = 1.0, jax.random.fold_in(rng, 6)
    for position, parts in cuts:
        heights = jnp.exp(jax.random.uniform(jax.random.fold_in(own, position), (parts,), jnp.float32, smallest / len(cuts), largest / len(cuts)))
        gain = gain * jnp.repeat(heights, extent[position] // parts).reshape([-1 if axis == position else 1 for axis in range(len(extent))])
    return gain


def normal_values(key, extent, deviation, most, cuts=(), kind=jnp.bfloat16):
    drawn = jax.random.normal(key, extent, jnp.float32) * deviation
    if len(cuts) > 0:
        drawn = level_of(key, extent, cuts, -0.22, 0.18) * drawn
    return jnp.clip(drawn, min=-most, max=most).astype(kind)


def setup_inputs(seed: int = 0) -> dict:
    key_of = jax.random.split(jax.random.key(seed), 9)
    sub_inputs = normal_values(key_of[0], (TOKENS, HEADS * SUB), 1.0, 6.0, ((0, 32),))
    out_grads = normal_values(key_of[1], (TOKENS, HEADS * SUB), 1.0, 6.0, ((0, 32),))
    expert_outputs = normal_values(key_of[2], (TOKENS, HEADS, TOP, SUB), 1.0, 6.0, ((0, 32),))
    combine_weights = jnp.clip(0.1 + 0.9 * jax.random.uniform(key_of[3], (TOKENS, HEADS, TOP), jnp.float32) ** level_of(key_of[3], (TOKENS, HEADS, TOP), ((0, 32),), -0.2, 0.2), 0.1, 1.0)
    expert_ids = draw_expert_ids(jax.random.fold_in(key_of[8], 71), 0)
    slot_ids = draw_slot_ids(jax.random.fold_in(key_of[8], 71), 0)
    expert_input_weight = normal_values(key_of[6], (EXPERTS, SUB, FF), SUB ** -0.5, 0.1875, ((0, 8),))
    expert_output_weight = normal_values(key_of[7], (EXPERTS, FF, SUB), FF ** -0.5, 0.1875, ((0, 8),))
    return {"sub_inputs": sub_inputs, "out_grads": out_grads, "expert_outputs": expert_outputs, "combine_weights": combine_weights, "expert_ids": expert_ids, "slot_ids": slot_ids, "expert_input_weight": expert_input_weight, "expert_output_weight": expert_output_weight}


def reference(sub_inputs, out_grads, expert_outputs, combine_weights, expert_ids, slot_ids, expert_input_weight, expert_output_weight):
    blocks = TOKENS // TOK_DEV
    sub_rows = TOK_DEV * HEADS
    name_count = sub_rows * TOP
    kept_mask = slot_ids >= 0
    inputs_split = sub_inputs.reshape(blocks, sub_rows, SUB)
    grads_split = out_grads.reshape(blocks, sub_rows, SUB)
    outputs_split = expert_outputs.reshape(blocks, sub_rows, TOP, SUB)

    def gate_block(packed):
        grads_here, outputs_here = packed
        return jnp.einsum('ns,nks->nk', grads_here.astype(jnp.float32), outputs_here.astype(jnp.float32))
    gate_dots = lax.map(gate_block, (grads_split, outputs_split)).reshape(TOKENS, HEADS, TOP)
    d_gates = jnp.where(kept_mask, gate_dots, jnp.float32(0.0))
    weights_split = combine_weights.reshape(blocks, name_count)
    ids_flat = expert_ids.reshape(blocks, name_count).astype(jnp.int32)
    slots_flat = slot_ids.reshape(blocks, name_count).astype(jnp.int32)
    slot_target = jnp.where(slots_flat >= 0, slots_flat, CAP).astype(jnp.int32)
    block_index = jnp.broadcast_to(jnp.arange(blocks, dtype=jnp.int32)[:, None], (blocks, name_count))
    name_index = jnp.broadcast_to(jnp.arange(name_count, dtype=jnp.int32)[None, :], (blocks, name_count))
    owner_table = jnp.full((blocks, EXPERTS, CAP), -1, jnp.int32)
    owner_table = owner_table.at[block_index, ids_flat, slot_target].set(name_index, mode='drop')

    def replica_sum(left, right):
        groups = blocks // N_DP
        left_split = left.reshape(groups, N_DP, CAP, left.shape[-1]).astype(jnp.float32)
        right_split = right.reshape(groups, N_DP, CAP, right.shape[-1]).astype(jnp.float32)
        partial_value = jnp.einsum('gdca,gdcb->dab', left_split, right_split).astype(jnp.bfloat16)
        partial_value = lax.optimization_barrier(partial_value)
        return lax.optimization_barrier(jnp.sum(partial_value.astype(jnp.float32), axis=0))

    def expert_grads(expert):
        picked = owner_table[:, expert, :]
        present = picked >= 0
        safe_index = jnp.maximum(picked, 0).astype(jnp.int32)
        source = (safe_index // TOP).astype(jnp.int32)
        inputs_here = jnp.take_along_axis(inputs_split, source[:, :, None], axis=1)
        grads_here = jnp.take_along_axis(grads_split, source[:, :, None], axis=1)
        weight_here = jnp.take_along_axis(weights_split, safe_index, axis=1)
        inputs_here = jnp.where(present[:, :, None], inputs_here, jnp.zeros((), jnp.bfloat16))
        inputs_here = inputs_here.astype(jnp.bfloat16).reshape(blocks * CAP, SUB)
        upstream = jnp.where(present[:, :, None], weight_here[:, :, None] * grads_here.astype(jnp.float32), jnp.float32(0.0))
        upstream = upstream.astype(jnp.bfloat16).reshape(blocks * CAP, SUB)
        weight_in = expert_input_weight[expert]
        weight_out = expert_output_weight[expert]
        preactivation_value = jnp.dot(inputs_here, weight_in, preferred_element_type=jnp.float32)
        hidden_activation, gelu_back = jax.vjp(jax.nn.gelu, preactivation_value)
        hidden_activation = hidden_activation.astype(jnp.bfloat16)
        hidden_grad = jnp.dot(upstream, weight_out.T, preferred_element_type=jnp.float32)
        preactivation_gradient = gelu_back(hidden_grad)[0].astype(jnp.bfloat16)
        grad_out = replica_sum(hidden_activation, upstream)
        grad_in = replica_sum(inputs_here, preactivation_gradient)
        input_grad = jnp.dot(preactivation_gradient, weight_in.T, preferred_element_type=jnp.float32).astype(jnp.bfloat16)
        return (grad_in, grad_out, input_grad.reshape(blocks, CAP, SUB))
    dw_in, dw_out, returned = lax.map(expert_grads, jnp.arange(EXPERTS, dtype=jnp.int32))
    returned_rows = returned.reshape(EXPERTS * blocks * CAP, SUB)

    def merge_block(packed):
        ids_here, slots_here, which_block = packed
        flat_index = (ids_here * blocks + which_block) * CAP + slots_here
        flat_index = jnp.where(slots_here >= 0, flat_index, 0).astype(jnp.int32)
        rows_here = returned_rows[flat_index].astype(jnp.float32)
        rows_here = jnp.where((slots_here >= 0)[:, None], rows_here, jnp.float32(0.0))
        return lax.optimization_barrier(jnp.sum(rows_here.reshape(sub_rows, TOP, SUB), axis=1)).astype(jnp.bfloat16)
    merged = lax.map(merge_block, (ids_flat, slots_flat, jnp.arange(blocks, dtype=jnp.int32)))
    d_inputs = merged.reshape(TOKENS, HEADS * SUB)
    return (d_inputs, d_gates, dw_in, dw_out)
```

```python
import functools

import jax
import jax.numpy as jnp
from jax import lax
from jax.experimental import pallas as pl
from jax.experimental.pallas import tpu as pltpu
from jax.sharding import PartitionSpec as P

MESH = pl.DeviceIdType.MESH
F32 = jnp.float32
BF16 = jnp.bfloat16
ROOT = 0.7978845608028654
CUBE = 0.044715


def partner(me, step, count):
    if count & (count - 1):
        return lax.rem(step - me + count, count)
    out, bit = 0, 1
    while bit < count:
        out = out + ((me // bit + step // bit) % 2) * bit
        bit *= 2
    return out


def spread(i, count):
    return lax.rem(i + 1, count)


def dot(a, b, ca, cb):
    return lax.dot_general(a, b, (((ca,), (cb,)), ((), ())), preferred_element_type=F32)


def kernel(
    dims,
    tgt, cw, x_hbm, g_hbm, win_hbm, wout_hbm, eo_hbm,
    dx, dwi, dwo, dg,
    xs, gs, win, wout, sx, sg, rx, rg, rs, rr, hb, fb, acc, po, pi, tpo, tpi, so, si, rpo, rpi,
    ev, load_sem, xg_send, xg_recv, r_send, r_recv, t_send, t_recv, w_send, w_recv,
):
    groups, replicas, cap, heads, tokens, sub, ff = dims
    chunk = max(cap, 128)
    per = chunk // cap
    chunks = groups * cap // chunk
    tile = 256
    me = lax.axis_index("expert")
    mine = lax.axis_index("dp")
    my_chunk = me // per
    halves = replicas // 2
    row, side = mine // 2, mine % 2
    twin = row * 2 + (1 - side)

    loads = []
    for h in range(heads):
        for s, (src, dst) in enumerate(((x_hbm, xs), (g_hbm, gs))):
            loads.append(
                pltpu.make_async_copy(
                    src.at[:, pl.ds(h * sub, sub)], dst.at[pl.ds(h * tokens, tokens)], load_sem.at[2 * h + s]
                )
            )
    wloads = [
        pltpu.make_async_copy(win_hbm.at[0], win, load_sem.at[2 * heads]),
        pltpu.make_async_copy(wout_hbm.at[0], wout, load_sem.at[2 * heads + 1]),
        pltpu.make_async_copy(eo_hbm, ev, load_sem.at[2 * heads + 2]),
    ]
    for c in loads + wloads:
        c.start()

    barrier = pltpu.get_barrier_semaphore()

    @pl.loop(1, groups)
    def _(i):
        pl.semaphore_signal(barrier, inc=1, device_id={"expert": lax.rem(me + i, groups)}, device_id_type=MESH)

    @pl.loop(1, replicas)
    def _(i):
        pl.semaphore_signal(barrier, inc=1, device_id={"dp": lax.rem(mine + i, replicas)}, device_id_type=MESH)

    pl.semaphore_wait(barrier, groups + replicas - 2)
    for c in loads:
        c.wait()

    def rows_of(index, size):
        return pl.ds(pl.multiple_of(index * size, size), size)

    def hot(j):
        slots = lax.broadcasted_iota(jnp.int32, (chunk, tgt.shape[1]), 0) + j * chunk
        return tgt[0:1, :] == slots, tgt[1:2, :] == slots

    def xg_copy(s, peer):
        src, dst = ((sx, rx), (sg, rg))[s]
        return pltpu.make_async_remote_copy(
            src_ref=src.at[rows_of(peer, cap)], dst_ref=dst.at[rows_of(me, cap)],
            send_sem=xg_send.at[s, peer], recv_sem=xg_recv.at[s, me],
            device_id={"expert": peer}, device_id_type=MESH,
        )

    def xg_local(s, src_dev):
        src, dst = ((sx, rx), (sg, rg))[s]
        return pltpu.make_async_copy(
            src.at[rows_of(src_dev, cap)], dst.at[rows_of(src_dev, cap)], xg_recv.at[s, src_dev]
        )

    def r_copy(peer):
        return pltpu.make_async_remote_copy(
            src_ref=rs.at[rows_of(peer, cap)], dst_ref=rr.at[rows_of(me, cap)],
            send_sem=r_send.at[peer], recv_sem=r_recv.at[me],
            device_id={"expert": peer}, device_id_type=MESH,
        )

    def r_local(src_dev):
        return pltpu.make_async_copy(
            rs.at[rows_of(src_dev, cap)], rr.at[rows_of(src_dev, cap)], r_recv.at[src_dev]
        )

    def twin_copy(s, q, t):
        src, dst = ((po, tpo), (pi, tpi))[s]
        return pltpu.make_async_remote_copy(
            src_ref=src.at[q], dst_ref=dst.at[t],
            send_sem=t_send.at[s, t], recv_sem=t_recv.at[s, t],
            device_id={"dp": twin}, device_id_type=MESH,
        )

    def row_copy(s, t):
        src, dst = ((so, rpo), (si, rpi))[s]
        return pltpu.make_async_remote_copy(
            src_ref=src.at[t], dst_ref=dst.at[row],
            send_sem=w_send.at[s, t], recv_sem=w_recv.at[s, row],
            device_id={"dp": 2 * t + side}, device_id_type=MESH,
        )

    def row_got(s, t):
        dst = (rpo, rpi)[s]
        return pltpu.make_async_copy(dst.at[t], dst.at[t], w_recv.at[s, t])

    @pl.loop(0, chunks)
    def _(i):
        j = partner(my_chunk, spread(i, chunks), chunks)
        h0, h1 = hot(j)
        one = (h0 | h1).astype(F32).astype(BF16)
        w = jnp.sum(jnp.where(h0, cw[0:1, :], 0.0) + jnp.where(h1, cw[1:2, :], 0.0), axis=1, keepdims=True)
        sx[rows_of(j, chunk), :] = dot(one, xs[...], 1, 0).astype(BF16)
        sg[rows_of(j, chunk), :] = (dot(one, gs[...], 1, 0) * w).astype(BF16)
        for p in range(per):
            peer = j * per + p

            @pl.when(peer != me)
            def _():
                xg_copy(0, peer).start()
                xg_copy(1, peer).start()

            @pl.when(peer == me)
            def _():
                xg_local(0, me).start()
                xg_local(1, me).start()

    for c in wloads:
        c.wait()

    span = 16
    for h in range(heads):

        @pl.loop(0, tokens // span)
        def _(b):
            grads = gs[rows_of(h * (tokens // span) + b, span), :].astype(F32)
            terms = ev[rows_of(b, span), h].astype(F32) * grads[:, None, :]
            dg[h, rows_of(b, span), :] = jnp.sum(terms, axis=-1)

    @pl.loop(0, chunks)
    def _(i):
        j = partner(my_chunk, spread(lax.rem(i + chunks - 1, chunks), chunks), chunks)
        for p in range(per):
            xg_local(0, j * per + p).wait()
            xg_local(1, j * per + p).wait()
        rows = rows_of(j, chunk)
        for n in range(ff // tile):
            cols = pl.ds(n * tile, tile)
            z = dot(rx[rows, :], win[:, cols], 1, 0)
            e = dot(rg[rows, :], wout[cols, :], 1, 1)
            zz = z * z
            t = jnp.tanh(ROOT * (z + CUBE * (zz * z)))
            half = 0.5 * (1.0 + t)
            hb[rows, cols] = (z * half).astype(BF16)
            slope = half + 0.5 * z * (1.0 - t * t) * (ROOT * (1.0 + 3.0 * CUBE * zz))
            fb[rows, cols] = (e * slope).astype(BF16)
        for n in range(sub // tile):
            cols = pl.ds(n * tile, tile)
            rs[rows, cols] = dot(fb[rows, :], win[cols, :], 1, 1).astype(BF16)
        for p in range(per):
            peer = j * per + p

            @pl.when(peer != me)
            def _():
                r_copy(peer).start()

            @pl.when(peer == me)
            def _():
                r_local(me).start()

    block = dwo.shape[1]
    def product(q):
        cols = rows_of(q, block)
        po[q] = dot(hb[:, cols], rg[...], 0, 0).astype(BF16)
        pi[q] = dot(rx[:, cols], fb[...], 0, 0).astype(BF16)

    @pl.loop(0, halves)
    def _(i):
        t = lax.rem(row + 1 + i, halves)
        product(2 * t + (1 - side))
        twin_copy(0, 2 * t + (1 - side), t).start()
        twin_copy(1, 2 * t + (1 - side), t).start()
        product(2 * t + side)

        @pl.when(t != row)
        def _():
            for s, (own, got, out) in enumerate(((po, tpo, so), (pi, tpi, si))):
                twin_copy(s, 2 * t + side, t).wait_recv()
                out[t] = (own[2 * t + side].astype(F32) + got[t].astype(F32)).astype(BF16)
                row_copy(s, t).start()

    acc[...] = jnp.zeros_like(acc)

    @pl.loop(0, chunks)
    def _(i):
        j = partner(my_chunk, spread(lax.rem(i + chunks - 1, chunks), chunks), chunks)
        for p in range(per):
            r_local(j * per + p).wait()
        h0, h1 = hot(j)
        one = (h0 | h1).astype(F32).astype(BF16)
        acc[...] += dot(one, rr[rows_of(j, chunk), :], 0, 0)

    for h in range(heads):
        dx[:, pl.ds(h * sub, sub)] = acc[pl.ds(h * tokens, tokens), :].astype(BF16)

    for s, (out, own, got, sums) in enumerate(((dwo, po, tpo, rpo), (dwi, pi, tpi, rpi))):
        twin_copy(s, mine, row).wait_recv()
        out[0] = own[mine].astype(F32) + got[row].astype(F32)

        @pl.loop(1, halves)
        def _(i):
            t = lax.rem(row + i, halves)
            row_got(s, t).wait()
            out[0] = out[0] + sums[t].astype(F32)

    @pl.loop(1, groups)
    def _(i):
        peer = lax.rem(me + i, groups)
        xg_copy(0, peer).wait_send()
        xg_copy(1, peer).wait_send()
        r_copy(peer).wait_send()

    for s in range(2):

        @pl.loop(0, halves)
        def _(i):
            twin_copy(s, 2 * i + (1 - side), i).wait_send()

        @pl.loop(1, halves)
        def _(i):
            row_copy(s, lax.rem(row + i, halves)).wait_send()


def plain_call(
    sub_inputs,
    out_grads,
    expert_outputs,
    combine_weights,
    expert_ids,
    slot_ids,
    expert_input_weight,
    expert_output_weight,
):
    tokens, heads, top = expert_ids.shape
    _, sub, ff = expert_input_weight.shape
    groups = lax.axis_size("expert")
    replicas = lax.axis_size("dp")
    cap = top * heads * tokens // groups
    kept = slot_ids >= 0
    target = jnp.where(kept, expert_ids * cap + slot_ids, -1)
    target = target.transpose(2, 1, 0).reshape(top, heads * tokens)
    weight = combine_weights.transpose(2, 1, 0).reshape(top, heads * tokens)
    slots = groups * cap
    part = sub // replicas
    part_out = ff // replicas
    dims = (groups, replicas, cap, heads, tokens, sub, ff)
    any_spec = pl.BlockSpec(memory_space=pltpu.HBM)
    vmem = pl.BlockSpec(memory_space=pltpu.VMEM)
    dma = pltpu.SemaphoreType.DMA
    d_inputs, dw_in, dw_out, gate_dots = pl.pallas_call(
        functools.partial(kernel, dims),
        out_shape=(
            jax.ShapeDtypeStruct((tokens, heads * sub), BF16),
            jax.ShapeDtypeStruct((1, part, ff), F32),
            jax.ShapeDtypeStruct((1, part_out, sub), F32),
            jax.ShapeDtypeStruct((heads, tokens, top), F32),
        ),
        in_specs=[vmem, vmem, any_spec, any_spec, any_spec, any_spec, any_spec],
        out_specs=(vmem, vmem, vmem, vmem),
        scratch_shapes=[
            pltpu.VMEM((heads * tokens, sub), BF16),
            pltpu.VMEM((heads * tokens, sub), BF16),
            pltpu.VMEM((sub, ff), BF16),
            pltpu.VMEM((ff, sub), BF16),
            pltpu.VMEM((slots, sub), BF16),
            pltpu.VMEM((slots, sub), BF16),
            pltpu.VMEM((slots, sub), BF16),
            pltpu.VMEM((slots, sub), BF16),
            pltpu.VMEM((slots, sub), BF16),
            pltpu.VMEM((slots, sub), BF16),
            pltpu.VMEM((slots, ff), BF16),
            pltpu.VMEM((slots, ff), BF16),
            pltpu.VMEM((heads * tokens, sub), F32),
            pltpu.VMEM((replicas, part_out, sub), BF16),
            pltpu.VMEM((replicas, part, ff), BF16),
            *[pltpu.VMEM((replicas // 2, part_out, sub), BF16), pltpu.VMEM((replicas // 2, part, ff), BF16)] * 3,
            pltpu.VMEM((tokens, heads, top, sub), BF16),
            dma((2 * heads + 3,)),
            dma((2, groups)),
            dma((2, groups)),
            dma((groups,)),
            dma((groups,)),
            *[dma((2, replicas // 2))] * 4,
        ],
        compiler_params=pltpu.CompilerParams(
            collective_id=0, has_side_effects=True, vmem_limit_bytes=60 * 1024 * 1024
        ),
        cost_estimate=pl.CostEstimate(flops=20 * 10**9, bytes_accessed=2**24, transcendentals=0),
    )(target, weight, sub_inputs, out_grads, expert_input_weight, expert_output_weight, expert_outputs)
    d_gates = jnp.where(kept, gate_dots.transpose(1, 0, 2), jnp.float32(0.0))
    return (d_inputs, d_gates, dw_in, dw_out)


PIECES = 2


def paired(
    dims,
    ids, slot, cw, x_hbm, g_hbm, win_hbm, wout_hbm, eo_hbm,
    dx, dwi, dwo, dg,
    tgt, xs, gs, win, wout, sx, sg, rx, rg, rs, rr, hb, fb, acc, po, pi, tpo, tpi, so, si, rpo, rpi,
    cpo, cpi, gpo, gpi, ev, gates,
    load_sem, xg_send, xg_recv, r_send, r_recv, wz_send, wz_recv, wt_send, wt_recv, wy_send, wy_recv,
    t_send, t_recv, y_send, y_recv, c_send, c_recv,
):
    groups, replicas, cap, heads, tokens, sub, ff = dims
    tile = 256
    me = lax.axis_index("expert")
    mine = lax.axis_index("dp")
    half = groups // 2
    halves = replicas // 2
    low = lax.rem(me, half)
    base = me - low
    opposite = lax.rem(me + half, groups)
    outer = me // half == low // (half // 2)
    row, side = mine // 2, mine % 2
    twin = row * 2 + (1 - side)
    near = range(1, half)

    def rows_of(index, size):
        return pl.ds(pl.multiple_of(index * size, size), size)

    def fixed(f, s, n=1):
        return pl.ds((f * half + s) * cap, n * cap)

    def landed(ref, sem):
        return pltpu.make_async_copy(ref, ref, sem)

    def remote(src, dst, send, recv, where):
        return pltpu.make_async_remote_copy(
            src_ref=src, dst_ref=dst, send_sem=send, recv_sem=recv, device_id=where, device_id_type=MESH
        )

    loads = []
    for h in range(heads):
        for s, (src, dst) in enumerate(((x_hbm, xs), (g_hbm, gs))):
            loads.append(
                pltpu.make_async_copy(
                    src.at[:, pl.ds(h * sub, sub)], dst.at[pl.ds(h * tokens, tokens)], load_sem.at[2 * h + s]
                )
            )
    wloads = [
        pltpu.make_async_copy(win_hbm.at[0], win.at[0], load_sem.at[2 * heads]),
        pltpu.make_async_copy(wout_hbm.at[0], wout.at[0], load_sem.at[2 * heads + 1]),
    ]
    eload = pltpu.make_async_copy(eo_hbm, ev, load_sem.at[2 * heads + 2])
    for c in loads + wloads + [eload]:
        c.start()

    barrier = pltpu.get_barrier_semaphore()
    for s in near:
        pl.semaphore_signal(
            barrier, inc=1, device_id={"expert": base + partner(low, s, half)}, device_id_type=MESH
        )
    pl.semaphore_signal(barrier, inc=1, device_id={"expert": opposite}, device_id_type=MESH)
    for i in range(1, replicas):
        pl.semaphore_signal(barrier, inc=1, device_id={"dp": lax.rem(mine + i, replicas)}, device_id_type=MESH)
    pl.semaphore_wait(barrier, half + replicas - 1)

    def owner(s):
        return base + partner(low, s, half)

    def part_of(m, quarter, n):
        size = (sub, ff)[m] // replicas // PIECES
        return rows_of(quarter * PIECES + n, size)

    def held(m, quarter, n):
        return (win, wout)[m].at[1, part_of(m, quarter, n)]

    def w_cross(m, n):
        return remote(
            (win_hbm, wout_hbm)[m].at[0, part_of(m, mine, n)], held(m, mine, n),
            wz_send.at[m, n], wz_recv.at[m, n], {"expert": opposite},
        )

    def w_twin(m, n, t):
        ref = held(m, 2 * t + side, n)
        return remote(ref, ref, wt_send.at[m, n, t], wt_recv.at[m, n, t], {"dp": twin})

    def w_row(m, n, t):
        ref = held(m, mine, n)
        return remote(ref, ref, wy_send.at[m, n, t], wy_recv.at[m, n, row], {"dp": 2 * t + side})

    def xg_copy(s, f, step):
        src, dst = ((sx, rx), (sg, rg))[s]
        return remote(
            src.at[fixed(f, step)], dst.at[fixed(f, step)],
            xg_send.at[s, f, step], xg_recv.at[s, f, step], {"expert": owner(step)},
        )

    def r_copy(f, step):
        return remote(
            rs.at[fixed(f, step)], rr.at[fixed(f, step)],
            r_send.at[f, step], r_recv.at[f, step], {"expert": owner(step)},
        )

    def twin_copy(f, s, q, t):
        src, dst = ((po, tpo), (pi, tpi))[s]
        return remote(src.at[f, q], dst.at[f, t], t_send.at[f, s, t], t_recv.at[f, s, t], {"dp": twin})

    def row_copy(f, s, t):
        src, dst = ((so, rpo), (si, rpi))[s]
        return remote(
            src.at[f, t], dst.at[f, row], y_send.at[f, s, t], y_recv.at[f, s, row], {"dp": 2 * t + side}
        )

    def row_got(f, s, t):
        ref = (rpo, rpi)[s].at[f, t]
        return landed(ref, y_recv.at[f, s, t])

    def cross_copy(s):
        src, dst = ((cpo, gpo), (cpi, gpi))[s]
        return remote(src, dst, c_send.at[s], c_recv.at[s], {"expert": opposite})

    pieces = [(m, n) for m in range(2) for n in range(PIECES)]

    @pl.when(outer)
    def _():
        for m, n in pieces:
            w_cross(m, n).start()

    tgt[...] = jnp.where(slot[...] >= 0, ids[...] * cap + slot[...], -1)

    def hot(f, step):
        first = lax.rem(owner(step) + f * half, groups) * cap
        slots = lax.broadcasted_iota(jnp.int32, (cap, tgt.shape[1]), 0) + first
        return tgt[0:1, :] == slots, tgt[1:2, :] == slots

    def gather(f, step, out_x, out_g):
        h0, h1 = hot(f, step)
        one = (h0 | h1).astype(F32).astype(BF16)
        w = jnp.sum(jnp.where(h0, cw[0:1, :], 0.0) + jnp.where(h1, cw[1:2, :], 0.0), axis=1, keepdims=True)
        rows = rows_of(f * half + step, cap)
        out_x[rows, :] = dot(one, xs[...], 1, 0).astype(BF16)
        out_g[rows, :] = (dot(one, gs[...], 1, 0) * w).astype(BF16)

    for c in loads:
        c.wait()
    far_steps = range(half // 2, half)
    near_steps = range(1, half // 2)

    for f in (1, 0):

        @pl.loop(0, half - 1)
        def _(i):
            step = lax.rem(i + half // 2 - 1, half - 1) + 1
            gather(f, step, sx, sg)
            if f == 1:
                xg_copy(0, f, step).start()
                xg_copy(1, f, step).start()
            else:

                @pl.when(jnp.logical_or(outer, step < half // 2))
                def _():
                    xg_copy(0, f, step).start()
                    xg_copy(1, f, step).start()

    @pl.loop(0, 2)
    def _(f):
        gather(f, 0, rx, rg)

    eload.wait()
    span = 16
    lane = lax.broadcasted_iota(jnp.int32, (span, gates.shape[1]), 1)

    @pl.loop(0, tokens // span)
    def _(b):
        found = jnp.zeros((span, gates.shape[1]), F32)
        for h in range(heads):
            grads = gs[rows_of(h * (tokens // span) + b, span), :].astype(F32)
            terms = ev[rows_of(b, span), h].astype(F32) * grads[:, None, :]
            sums = jnp.sum(terms, axis=-1)
            for k in range(2):
                found = jnp.where(lane == 2 * h + k, sums[:, k : k + 1], found)
        gates[rows_of(b, span), :] = found

    turned = gates[...].T
    for h in range(heads):
        cols = pl.ds(h * tokens, tokens)
        dg[:, cols] = jnp.where(slot[:, cols] >= 0, turned[2 * h : 2 * h + 2, :], 0.0)

    for c in wloads:
        c.wait()

    others = [lax.rem(row + i, halves) for i in range(1, halves)]

    def from_rows(m, n):
        for t in others:
            landed(held(m, 2 * t + side, n), wy_recv.at[m, n, t]).wait()
            w_twin(m, n, t).start()

    before = None
    for m, n in pieces:
        landed(held(m, mine, n), wz_recv.at[m, n]).wait()
        w_twin(m, n, row).start()
        for t in others:
            w_row(m, n, t).start()
        if before is not None:
            from_rows(*before)
        before = (m, n)

    @pl.when(jnp.logical_not(outer))
    def _():
        for m, n in pieces:
            w_cross(m, n).start()

    from_rows(*before)
    for m, n in pieces:
        for t in range(halves):
            landed(held(m, 2 * t + (1 - side), n), wt_recv.at[m, n, t]).wait()

    def process(f, s, n):
        for step in range(s, s + n):
            if step > 0:
                for v, dst in enumerate((rx, rg)):
                    landed(dst.at[fixed(f, step)], xg_recv.at[v, f, step]).wait()
        rows = fixed(f, s, n)
        for c in range(ff // tile):
            cols = pl.ds(c * tile, tile)
            z = dot(rx[rows, :], win[f, :, cols], 1, 0)
            e = dot(rg[rows, :], wout[f, cols, :], 1, 1)
            zz = z * z
            t = jnp.tanh(ROOT * (z + CUBE * (zz * z)))
            part = 0.5 * (1.0 + t)
            hb[rows, cols] = (z * part).astype(BF16)
            slope = part + 0.5 * z * (1.0 - t * t) * (ROOT * (1.0 + 3.0 * CUBE * zz))
            fb[rows, cols] = (e * slope).astype(BF16)
        for c in range(sub // tile):
            cols = pl.ds(c * tile, tile)
            back = dot(fb[rows, :], win[f, cols, :], 1, 1).astype(BF16)
            for step in range(s, s + n):
                piece = back[(step - s) * cap : (step - s + 1) * cap]
                if step == 0:
                    rr[fixed(f, step), cols] = piece
                else:
                    rs[fixed(f, step), cols] = piece
        for step in range(s, s + n):
            if step > 0:
                r_copy(f, step).start()

    block = dwo.shape[1]

    def product(f, q):
        cols = rows_of(q, block)
        rows = fixed(f, 0, half)
        po[f, q] = dot(hb[rows, cols], rg[rows, :], 0, 0).astype(BF16)
        pi[f, q] = dot(rx[rows, cols], fb[rows, :], 0, 0).astype(BF16)

    def exchange(f):
        @pl.loop(0, halves)
        def _(i):
            t = lax.rem(row + 1 + i, halves)
            product(f, 2 * t + (1 - side))
            twin_copy(f, 0, 2 * t + (1 - side), t).start()
            twin_copy(f, 1, 2 * t + (1 - side), t).start()
            product(f, 2 * t + side)

            @pl.when(t != row)
            def _():
                for s, (own, got, out) in enumerate(((po, tpo, so), (pi, tpi, si))):
                    landed(got.at[f, t], t_recv.at[f, s, t]).wait()
                    out[f, t] = (own[f, 2 * t + side].astype(F32) + got[f, t].astype(F32)).astype(BF16)
                    row_copy(f, s, t).start()

    def total(f, s):
        own, got, sums = ((po, tpo, rpo), (pi, tpi, rpi))[s]
        landed(got.at[f, row], t_recv.at[f, s, row]).wait()
        out = own[f, mine].astype(F32) + got[f, row].astype(F32)
        for t in others:
            row_got(f, s, t).wait()
            out = out + sums[f, t].astype(F32)
        return out

    def scatter(f, s, n, start=False):
        ones = []
        for step in range(s, s + n):
            if step > 0:
                landed(rr.at[fixed(f, step)], r_recv.at[f, step]).wait()
            h0, h1 = hot(f, step)
            ones.append((h0 | h1).astype(F32).astype(BF16))
        more = dot(jnp.concatenate(ones, axis=0), rr[fixed(f, s, n), :], 0, 0)
        acc[...] = more if start else acc[...] + more

    process(1, 0, half // 2)
    process(1, half // 2, half // 2)
    exchange(1)

    @pl.when(jnp.logical_not(outer))
    def _():
        for step in far_steps:
            xg_copy(0, 0, step).start()
            xg_copy(1, 0, step).start()

    process(0, 0, half // 2)
    for s, out in enumerate((cpo, cpi)):
        out[...] = total(1, s).astype(BF16)
        cross_copy(s).start()
    process(0, half // 2, half // 2)
    exchange(0)
    scatter(1, 0, half // 2, True)
    scatter(1, half // 2, half // 2)
    for s, out in enumerate((dwo, dwi)):
        out[0] = total(0, s)
    scatter(0, 0, half // 2)
    scatter(0, half // 2, half // 2)
    for h in range(heads):
        dx[:, pl.ds(h * sub, sub)] = acc[pl.ds(h * tokens, tokens), :].astype(BF16)
    for s, (out, got) in enumerate(((dwo, gpo), (dwi, gpi))):
        landed(got, c_recv.at[s]).wait()
        out[0] = out[0] + got[...].astype(F32)

    for f in range(2):
        for step in near:
            xg_copy(0, f, step).wait_send()
            xg_copy(1, f, step).wait_send()
            r_copy(f, step).wait_send()
        for s in range(2):
            for t in range(halves):
                twin_copy(f, s, 2 * t + (1 - side), t).wait_send()
            for t in others:
                row_copy(f, s, t).wait_send()
    for m, n in pieces:
        w_cross(m, n).wait_send()
        for t in range(halves):
            w_twin(m, n, t).wait_send()
        for t in others:
            w_row(m, n, t).wait_send()
    for s in range(2):
        cross_copy(s).wait_send()


def paired_call(
    sub_inputs,
    out_grads,
    expert_outputs,
    combine_weights,
    expert_ids,
    slot_ids,
    expert_input_weight,
    expert_output_weight,
):
    tokens, heads, top = expert_ids.shape
    _, sub, ff = expert_input_weight.shape
    groups = lax.axis_size("expert")
    replicas = lax.axis_size("dp")
    cap = top * heads * tokens // groups

    def flat(a):
        return a.transpose(2, 1, 0).reshape(top, heads * tokens)

    slots = groups * cap
    half = groups // 2
    halves = replicas // 2
    part = sub // replicas
    part_out = ff // replicas
    dims = (groups, replicas, cap, heads, tokens, sub, ff)
    any_spec = pl.BlockSpec(memory_space=pltpu.HBM)
    vmem = pl.BlockSpec(memory_space=pltpu.VMEM)
    dma = pltpu.SemaphoreType.DMA
    rows = heads * tokens
    d_inputs, dw_in, dw_out, gate_dots = pl.pallas_call(
        functools.partial(paired, dims),
        out_shape=(
            jax.ShapeDtypeStruct((tokens, heads * sub), BF16),
            jax.ShapeDtypeStruct((1, part, ff), F32),
            jax.ShapeDtypeStruct((1, part_out, sub), F32),
            jax.ShapeDtypeStruct((top, heads * tokens), F32),
        ),
        in_specs=[vmem, vmem, vmem, any_spec, any_spec, any_spec, any_spec, any_spec],
        out_specs=(vmem, vmem, vmem, vmem),
        scratch_shapes=[
            pltpu.VMEM((top, rows), jnp.int32),
            pltpu.VMEM((rows, sub), BF16),
            pltpu.VMEM((rows, sub), BF16),
            pltpu.VMEM((2, sub, ff), BF16),
            pltpu.VMEM((2, ff, sub), BF16),
            *[pltpu.VMEM((slots, sub), BF16)] * 6,
            pltpu.VMEM((slots, ff), BF16),
            pltpu.VMEM((slots, ff), BF16),
            pltpu.VMEM((rows, sub), F32),
            pltpu.VMEM((2, replicas, part_out, sub), BF16),
            pltpu.VMEM((2, replicas, part, ff), BF16),
            *[pltpu.VMEM((2, halves, part_out, sub), BF16), pltpu.VMEM((2, halves, part, ff), BF16)] * 3,
            *[pltpu.VMEM((part_out, sub), BF16), pltpu.VMEM((part, ff), BF16)] * 2,
            pltpu.VMEM((tokens, heads, top, sub), BF16),
            pltpu.VMEM((tokens, 128), F32),
            dma((2 * heads + 3,)),
            *[dma((2, 2, half))] * 2,
            *[dma((2, half))] * 2,
            *[dma((2, PIECES))] * 2,
            *[dma((2, PIECES, halves))] * 4,
            *[dma((2, 2, halves))] * 4,
            *[dma((2,))] * 2,
        ],
        compiler_params=pltpu.CompilerParams(
            collective_id=0, has_side_effects=True, vmem_limit_bytes=63 * 1024 * 1024
        ),
        cost_estimate=pl.CostEstimate(flops=20 * 10**9, bytes_accessed=2**24, transcendentals=0),
    )(
        flat(expert_ids), flat(slot_ids), flat(combine_weights),
        sub_inputs, out_grads, expert_input_weight, expert_output_weight, expert_outputs,
    )
    d_gates = gate_dots.reshape(top, heads, tokens).transpose(2, 1, 0)
    return (d_inputs, d_gates, dw_in, dw_out)


def on_device(*args):
    tokens, heads, top = args[4].shape
    _, sub, ff = args[6].shape
    groups = lax.axis_size("expert")
    replicas = lax.axis_size("dp")
    cap = top * heads * tokens // groups
    half = groups // 2
    fits = half >= 4 and half & (half - 1) == 0 and replicas % 2 == 0 and cap % 128 == 0 and tokens % 128 == 0
    tokens_cross = half * replicas * cap * 3 * sub
    weights_cross = 4 * sub * ff
    if fits and weights_cross < tokens_cross:
        return paired_call(*args)
    return plain_call(*args)


def solution(mesh):
    rows = P(("expert", "dp"), None)
    table = P(("expert", "dp"), None, None)
    return jax.shard_map(
        on_device,
        mesh=mesh,
        in_specs=(
            rows,
            rows,
            P(("expert", "dp"), None, None, None),
            table,
            table,
            table,
            P("expert", None, None),
            P("expert", None, None),
        ),
        out_specs=(rows, table, P("expert", "dp", None), P("expert", "dp", None)),
        check_vma=False,
    )
```

```python
import functools

import jax
import jax.numpy as jnp
from jax import lax
from jax.experimental import pallas as pl
from jax.experimental.pallas import tpu as pltpu
from jax.sharding import PartitionSpec as P

MESH = pl.DeviceIdType.MESH
F32 = jnp.float32
BF16 = jnp.bfloat16
ROOT = 0.7978845608028654
CUBE = 0.044715


def partner(me, step, count):
    if count & (count - 1):
        return lax.rem(step - me + count, count)
    out, bit = 0, 1
    while bit < count:
        out = out + ((me // bit + step // bit) % 2) * bit
        bit *= 2
    return out


def spread(i, count):
    return lax.rem(i + 1, count)


def dot(a, b, ca, cb):
    return lax.dot_general(a, b, (((ca,), (cb,)), ((), ())), preferred_element_type=F32)


def kernel(
    dims,
    tgt, cw, x_hbm, g_hbm, win_hbm, wout_hbm, eo_hbm,
    dx, dwi, dwo, dg,
    xs, gs, win, wout, sx, sg, rx, rg, rs, rr, hb, fb, acc, po, pi, tpo, tpi, so, si, rpo, rpi,
    ev, load_sem, xg_send, xg_recv, r_send, r_recv, t_send, t_recv, w_send, w_recv,
):
    groups, replicas, cap, heads, tokens, sub, ff = dims
    chunk = max(cap, 128)
    per = chunk // cap
    chunks = groups * cap // chunk
    tile = 256
    me = lax.axis_index("expert")
    mine = lax.axis_index("dp")
    my_chunk = me // per
    halves = replicas // 2
    row, side = mine // 2, mine % 2
    twin = row * 2 + (1 - side)

    loads = []
    for h in range(heads):
        for s, (src, dst) in enumerate(((x_hbm, xs), (g_hbm, gs))):
            loads.append(
                pltpu.make_async_copy(
                    src.at[:, pl.ds(h * sub, sub)], dst.at[pl.ds(h * tokens, tokens)], load_sem.at[2 * h + s]
                )
            )
    wloads = [
        pltpu.make_async_copy(win_hbm.at[0], win, load_sem.at[2 * heads]),
        pltpu.make_async_copy(wout_hbm.at[0], wout, load_sem.at[2 * heads + 1]),
        pltpu.make_async_copy(eo_hbm, ev, load_sem.at[2 * heads + 2]),
    ]
    for c in loads + wloads:
        c.start()

    barrier = pltpu.get_barrier_semaphore()

    @pl.loop(1, groups)
    def _(i):
        pl.semaphore_signal(barrier, inc=1, device_id={"expert": lax.rem(me + i, groups)}, device_id_type=MESH)

    @pl.loop(1, replicas)
    def _(i):
        pl.semaphore_signal(barrier, inc=1, device_id={"dp": lax.rem(mine + i, replicas)}, device_id_type=MESH)

    pl.semaphore_wait(barrier, groups + replicas - 2)
    for c in loads:
        c.wait()

    def rows_of(index, size):
        return pl.ds(pl.multiple_of(index * size, size), size)

    def hot(j):
        slots = lax.broadcasted_iota(jnp.int32, (chunk, tgt.shape[1]), 0) + j * chunk
        return tgt[0:1, :] == slots, tgt[1:2, :] == slots

    def xg_copy(s, peer):
        src, dst = ((sx, rx), (sg, rg))[s]
        return pltpu.make_async_remote_copy(
            src_ref=src.at[rows_of(peer, cap)], dst_ref=dst.at[rows_of(me, cap)],
            send_sem=xg_send.at[s, peer], recv_sem=xg_recv.at[s, me],
            device_id={"expert": peer}, device_id_type=MESH,
        )

    def xg_local(s, src_dev):
        src, dst = ((sx, rx), (sg, rg))[s]
        return pltpu.make_async_copy(
            src.at[rows_of(src_dev, cap)], dst.at[rows_of(src_dev, cap)], xg_recv.at[s, src_dev]
        )

    def r_copy(peer):
        return pltpu.make_async_remote_copy(
            src_ref=rs.at[rows_of(peer, cap)], dst_ref=rr.at[rows_of(me, cap)],
            send_sem=r_send.at[peer], recv_sem=r_recv.at[me],
            device_id={"expert": peer}, device_id_type=MESH,
        )

    def r_local(src_dev):
        return pltpu.make_async_copy(
            rs.at[rows_of(src_dev, cap)], rr.at[rows_of(src_dev, cap)], r_recv.at[src_dev]
        )

    def twin_copy(s, q, t):
        src, dst = ((po, tpo), (pi, tpi))[s]
        return pltpu.make_async_remote_copy(
            src_ref=src.at[q], dst_ref=dst.at[t],
            send_sem=t_send.at[s, t], recv_sem=t_recv.at[s, t],
            device_id={"dp": twin}, device_id_type=MESH,
        )

    def row_copy(s, t):
        src, dst = ((so, rpo), (si, rpi))[s]
        return pltpu.make_async_remote_copy(
            src_ref=src.at[t], dst_ref=dst.at[row],
            send_sem=w_send.at[s, t], recv_sem=w_recv.at[s, row],
            device_id={"dp": 2 * t + side}, device_id_type=MESH,
        )

    def row_got(s, t):
        dst = (rpo, rpi)[s]
        return pltpu.make_async_copy(dst.at[t], dst.at[t], w_recv.at[s, t])

    @pl.loop(0, chunks)
    def _(i):
        j = partner(my_chunk, spread(i, chunks), chunks)
        h0, h1 = hot(j)
        one = (h0 | h1).astype(F32).astype(BF16)
        w = jnp.sum(jnp.where(h0, cw[0:1, :], 0.0) + jnp.where(h1, cw[1:2, :], 0.0), axis=1, keepdims=True)
        sx[rows_of(j, chunk), :] = dot(one, xs[...], 1, 0).astype(BF16)
        sg[rows_of(j, chunk), :] = (dot(one, gs[...], 1, 0) * w).astype(BF16)
        for p in range(per):
            peer = j * per + p

            @pl.when(peer != me)
            def _():
                xg_copy(0, peer).start()
                xg_copy(1, peer).start()

            @pl.when(peer == me)
            def _():
                xg_local(0, me).start()
                xg_local(1, me).start()

    for c in wloads:
        c.wait()

    span = 16
    for h in range(heads):

        @pl.loop(0, tokens // span)
        def _(b):
            grads = gs[rows_of(h * (tokens // span) + b, span), :].astype(F32)
            terms = ev[rows_of(b, span), h].astype(F32) * grads[:, None, :]
            dg[h, rows_of(b, span), :] = jnp.sum(terms, axis=-1)

    @pl.loop(0, chunks)
    def _(i):
        j = partner(my_chunk, spread(lax.rem(i + chunks - 1, chunks), chunks), chunks)
        for p in range(per):
            xg_local(0, j * per + p).wait()
            xg_local(1, j * per + p).wait()
        rows = rows_of(j, chunk)
        for n in range(ff // tile):
            cols = pl.ds(n * tile, tile)
            z = dot(rx[rows, :], win[:, cols], 1, 0)
            e = dot(rg[rows, :], wout[cols, :], 1, 1)
            zz = z * z
            t = jnp.tanh(ROOT * (z + CUBE * (zz * z)))
            half = 0.5 * (1.0 + t)
            hb[rows, cols] = (z * half).astype(BF16)
            slope = half + 0.5 * z * (1.0 - t * t) * (ROOT * (1.0 + 3.0 * CUBE * zz))
            fb[rows, cols] = (e * slope).astype(BF16)
        for n in range(sub // tile):
            cols = pl.ds(n * tile, tile)
            rs[rows, cols] = dot(fb[rows, :], win[cols, :], 1, 1).astype(BF16)
        for p in range(per):
            peer = j * per + p

            @pl.when(peer != me)
            def _():
                r_copy(peer).start()

            @pl.when(peer == me)
            def _():
                r_local(me).start()

    block = dwo.shape[1]
    def product(q):
        cols = rows_of(q, block)
        po[q] = dot(hb[:, cols], rg[...], 0, 0).astype(BF16)
        pi[q] = dot(rx[:, cols], fb[...], 0, 0).astype(BF16)

    @pl.loop(0, halves)
    def _(i):
        t = lax.rem(row + 1 + i, halves)
        product(2 * t + (1 - side))
        twin_copy(0, 2 * t + (1 - side), t).start()
        twin_copy(1, 2 * t + (1 - side), t).start()
        product(2 * t + side)

        @pl.when(t != row)
        def _():
            for s, (own, got, out) in enumerate(((po, tpo, so), (pi, tpi, si))):
                twin_copy(s, 2 * t + side, t).wait_recv()
                out[t] = (own[2 * t + side].astype(F32) + got[t].astype(F32)).astype(BF16)
                row_copy(s, t).start()

    acc[...] = jnp.zeros_like(acc)

    @pl.loop(0, chunks)
    def _(i):
        j = partner(my_chunk, spread(lax.rem(i + chunks - 1, chunks), chunks), chunks)
        for p in range(per):
            r_local(j * per + p).wait()
        h0, h1 = hot(j)
        one = (h0 | h1).astype(F32).astype(BF16)
        acc[...] += dot(one, rr[rows_of(j, chunk), :], 0, 0)

    for h in range(heads):
        dx[:, pl.ds(h * sub, sub)] = acc[pl.ds(h * tokens, tokens), :].astype(BF16)

    for s, (out, own, got, sums) in enumerate(((dwo, po, tpo, rpo), (dwi, pi, tpi, rpi))):
        twin_copy(s, mine, row).wait_recv()
        out[0] = own[mine].astype(F32) + got[row].astype(F32)

        @pl.loop(1, halves)
        def _(i):
            t = lax.rem(row + i, halves)
            row_got(s, t).wait()
            out[0] = out[0] + sums[t].astype(F32)

    @pl.loop(1, groups)
    def _(i):
        peer = lax.rem(me + i, groups)
        xg_copy(0, peer).wait_send()
        xg_copy(1, peer).wait_send()
        r_copy(peer).wait_send()

    for s in range(2):

        @pl.loop(0, halves)
        def _(i):
            twin_copy(s, 2 * i + (1 - side), i).wait_send()

        @pl.loop(1, halves)
        def _(i):
            row_copy(s, lax.rem(row + i, halves)).wait_send()


def plain_call(
    sub_inputs,
    out_grads,
    expert_outputs,
    combine_weights,
    expert_ids,
    slot_ids,
    expert_input_weight,
    expert_output_weight,
):
    tokens, heads, top = expert_ids.shape
    _, sub, ff = expert_input_weight.shape
    groups = lax.axis_size("expert")
    replicas = lax.axis_size("dp")
    cap = top * heads * tokens // groups
    kept = slot_ids >= 0
    target = jnp.where(kept, expert_ids * cap + slot_ids, -1)
    target = target.transpose(2, 1, 0).reshape(top, heads * tokens)
    weight = combine_weights.transpose(2, 1, 0).reshape(top, heads * tokens)
    slots = groups * cap
    part = sub // replicas
    part_out = ff // replicas
    dims = (groups, replicas, cap, heads, tokens, sub, ff)
    any_spec = pl.BlockSpec(memory_space=pltpu.HBM)
    vmem = pl.BlockSpec(memory_space=pltpu.VMEM)
    dma = pltpu.SemaphoreType.DMA
    d_inputs, dw_in, dw_out, gate_dots = pl.pallas_call(
        functools.partial(kernel, dims),
        out_shape=(
            jax.ShapeDtypeStruct((tokens, heads * sub), BF16),
            jax.ShapeDtypeStruct((1, part, ff), F32),
            jax.ShapeDtypeStruct((1, part_out, sub), F32),
            jax.ShapeDtypeStruct((heads, tokens, top), F32),
        ),
        in_specs=[vmem, vmem, any_spec, any_spec, any_spec, any_spec, any_spec],
        out_specs=(vmem, vmem, vmem, vmem),
        scratch_shapes=[
            pltpu.VMEM((heads * tokens, sub), BF16),
            pltpu.VMEM((heads * tokens, sub), BF16),
            pltpu.VMEM((sub, ff), BF16),
            pltpu.VMEM((ff, sub), BF16),
            pltpu.VMEM((slots, sub), BF16),
            pltpu.VMEM((slots, sub), BF16),
            pltpu.VMEM((slots, sub), BF16),
            pltpu.VMEM((slots, sub), BF16),
            pltpu.VMEM((slots, sub), BF16),
            pltpu.VMEM((slots, sub), BF16),
            pltpu.VMEM((slots, ff), BF16),
            pltpu.VMEM((slots, ff), BF16),
            pltpu.VMEM((heads * tokens, sub), F32),
            pltpu.VMEM((replicas, part_out, sub), BF16),
            pltpu.VMEM((replicas, part, ff), BF16),
            *[pltpu.VMEM((replicas // 2, part_out, sub), BF16), pltpu.VMEM((replicas // 2, part, ff), BF16)] * 3,
            pltpu.VMEM((tokens, heads, top, sub), BF16),
            dma((2 * heads + 3,)),
            dma((2, groups)),
            dma((2, groups)),
            dma((groups,)),
            dma((groups,)),
            *[dma((2, replicas // 2))] * 4,
        ],
        compiler_params=pltpu.CompilerParams(
            collective_id=0, has_side_effects=True, vmem_limit_bytes=60 * 1024 * 1024
        ),
        cost_estimate=pl.CostEstimate(flops=20 * 10**9, bytes_accessed=2**24, transcendentals=0),
    )(target, weight, sub_inputs, out_grads, expert_input_weight, expert_output_weight, expert_outputs)
    d_gates = jnp.where(kept, gate_dots.transpose(1, 0, 2), jnp.float32(0.0))
    return (d_inputs, d_gates, dw_in, dw_out)


PIECES = 2


def paired(
    dims,
    ids, slot, cw, x_hbm, g_hbm, win_hbm, wout_hbm, eo_hbm,
    dx, dwi, dwo, dg,
    tgt, xs, gs, win, wout, sx, sg, rx, rg, rs, rr, hb, fb, acc, po, pi, tpo, tpi, so, si, rpo, rpi,
    cpo, cpi, gpo, gpi, ev, gates,
    load_sem, xg_send, xg_recv, r_send, r_recv, wz_send, wz_recv, wt_send, wt_recv, wy_send, wy_recv,
    t_send, t_recv, y_send, y_recv, c_send, c_recv,
):
    groups, replicas, cap, heads, tokens, sub, ff = dims
    tile = 256
    me = lax.axis_index("expert")
    mine = lax.axis_index("dp")
    half = groups // 2
    halves = replicas // 2
    low = lax.rem(me, half)
    base = me - low
    opposite = lax.rem(me + half, groups)
    inner = lax.rem(me // half + low // (half // 2), 2)
    outer = inner == 0
    first, second = inner, 1 - inner
    row, side = mine // 2, mine % 2
    twin = row * 2 + (1 - side)
    near = range(1, half)

    def rows_of(index, size):
        return pl.ds(pl.multiple_of(index * size, size), size)

    def fixed(f, s, n=1):
        return pl.ds(pl.multiple_of((f * half + s) * cap, cap), n * cap)

    def landed(ref, sem):
        return pltpu.make_async_copy(ref, ref, sem)

    def remote(src, dst, send, recv, where):
        return pltpu.make_async_remote_copy(
            src_ref=src, dst_ref=dst, send_sem=send, recv_sem=recv, device_id=where, device_id_type=MESH
        )

    loads = []
    for h in range(heads):
        for s, (src, dst) in enumerate(((x_hbm, xs), (g_hbm, gs))):
            loads.append(
                pltpu.make_async_copy(
                    src.at[:, pl.ds(h * sub, sub)], dst.at[pl.ds(h * tokens, tokens)], load_sem.at[2 * h + s]
                )
            )
    wloads = [
        pltpu.make_async_copy(win_hbm.at[0], win.at[0], load_sem.at[2 * heads]),
        pltpu.make_async_copy(wout_hbm.at[0], wout.at[0], load_sem.at[2 * heads + 1]),
    ]
    eload = pltpu.make_async_copy(eo_hbm, ev, load_sem.at[2 * heads + 2])
    for c in loads + wloads + [eload]:
        c.start()

    barrier = pltpu.get_barrier_semaphore()
    for s in near:
        pl.semaphore_signal(
            barrier, inc=1, device_id={"expert": base + partner(low, s, half)}, device_id_type=MESH
        )
    pl.semaphore_signal(barrier, inc=1, device_id={"expert": opposite}, device_id_type=MESH)
    for i in range(1, replicas):
        pl.semaphore_signal(barrier, inc=1, device_id={"dp": lax.rem(mine + i, replicas)}, device_id_type=MESH)
    pl.semaphore_wait(barrier, half + replicas - 1)

    def owner(s):
        return base + partner(low, s, half)

    def part_of(m, quarter, n):
        size = (sub, ff)[m] // replicas // PIECES
        return rows_of(quarter * PIECES + n, size)

    def held(m, quarter, n):
        return (win, wout)[m].at[1, part_of(m, quarter, n)]

    def w_cross(m, n):
        return remote(
            (win_hbm, wout_hbm)[m].at[0, part_of(m, mine, n)], held(m, mine, n),
            wz_send.at[m, n], wz_recv.at[m, n], {"expert": opposite},
        )

    def w_twin(m, n, t):
        ref = held(m, 2 * t + side, n)
        return remote(ref, ref, wt_send.at[m, n, t], wt_recv.at[m, n, t], {"dp": twin})

    def w_row(m, n, t):
        ref = held(m, mine, n)
        return remote(ref, ref, wy_send.at[m, n, t], wy_recv.at[m, n, row], {"dp": 2 * t + side})

    def xg_copy(s, f, step):
        src, dst = ((sx, rx), (sg, rg))[s]
        return remote(
            src.at[fixed(f, step)], dst.at[fixed(f, step)],
            xg_send.at[s, f, step], xg_recv.at[s, f, step], {"expert": owner(step)},
        )

    def r_copy(f, step):
        return remote(
            rs.at[fixed(f, step)], rr.at[fixed(f, step)],
            r_send.at[f, step], r_recv.at[f, step], {"expert": owner(step)},
        )

    def twin_copy(f, s, q, t):
        src, dst = ((po, tpo), (pi, tpi))[s]
        return remote(src.at[f, q], dst.at[f, t], t_send.at[f, s, t], t_recv.at[f, s, t], {"dp": twin})

    def row_copy(f, s, t):
        src, dst = ((so, rpo), (si, rpi))[s]
        return remote(
            src.at[f, t], dst.at[f, row], y_send.at[f, s, t], y_recv.at[f, s, row], {"dp": 2 * t + side}
        )

    def row_got(f, s, t):
        ref = (rpo, rpi)[s].at[f, t]
        return landed(ref, y_recv.at[f, s, t])

    def cross_copy(s):
        src, dst = ((cpo, gpo), (cpi, gpi))[s]
        return remote(src, dst, c_send.at[s], c_recv.at[s], {"expert": opposite})

    pieces = [(m, n) for m in range(2) for n in range(PIECES)]

    @pl.when(outer)
    def _():
        for m, n in pieces:
            w_cross(m, n).start()

    tgt[...] = jnp.where(slot[...] >= 0, ids[...] * cap + slot[...], -1)

    def hot(f, step):
        first = lax.rem(owner(step) + f * half, groups) * cap
        slots = lax.broadcasted_iota(jnp.int32, (cap, tgt.shape[1]), 0) + first
        return tgt[0:1, :] == slots, tgt[1:2, :] == slots

    def gather(f, step, out_x, out_g):
        h0, h1 = hot(f, step)
        one = (h0 | h1).astype(F32).astype(BF16)
        w = jnp.sum(jnp.where(h0, cw[0:1, :], 0.0) + jnp.where(h1, cw[1:2, :], 0.0), axis=1, keepdims=True)
        rows = rows_of(f * half + step, cap)
        out_x[rows, :] = dot(one, xs[...], 1, 0).astype(BF16)
        out_g[rows, :] = (dot(one, gs[...], 1, 0) * w).astype(BF16)

    for c in loads:
        c.wait()
    far_steps = range(half // 2, half)

    def send(f, step):
        xg_copy(0, f, step).start()
        xg_copy(1, f, step).start()

    @pl.loop(0, 2)
    def _(i):
        f_far = second + i * (first - second)
        f_near = first + i * (second - first)

        @pl.loop(half // 2, half)
        def _(step):
            gather(f_far, step, sx, sg)

            @pl.when(jnp.logical_or(outer, i == 0))
            def _():
                send(f_far, step)

        @pl.loop(1, half // 2)
        def _(step):
            gather(f_near, step, sx, sg)
            send(f_near, step)

        gather(f_near, 0, rx, rg)

    eload.wait()
    span = 16
    lane = lax.broadcasted_iota(jnp.int32, (span, gates.shape[1]), 1)

    @pl.loop(0, tokens // span)
    def _(b):
        found = jnp.zeros((span, gates.shape[1]), F32)
        for h in range(heads):
            grads = gs[rows_of(h * (tokens // span) + b, span), :].astype(F32)
            terms = ev[rows_of(b, span), h].astype(F32) * grads[:, None, :]
            sums = jnp.sum(terms, axis=-1)
            for k in range(2):
                found = jnp.where(lane == 2 * h + k, sums[:, k : k + 1], found)
        gates[rows_of(b, span), :] = found

    turned = gates[...].T
    for h in range(heads):
        cols = pl.ds(h * tokens, tokens)
        dg[:, cols] = jnp.where(slot[:, cols] >= 0, turned[2 * h : 2 * h + 2, :], 0.0)

    for c in wloads:
        c.wait()

    others = [lax.rem(row + i, halves) for i in range(1, halves)]

    def from_rows(m, n):
        for t in others:
            landed(held(m, 2 * t + side, n), wy_recv.at[m, n, t]).wait()
            w_twin(m, n, t).start()

    def weights():
        before = None
        for m, n in pieces:
            landed(held(m, mine, n), wz_recv.at[m, n]).wait()
            w_twin(m, n, row).start()
            for t in others:
                w_row(m, n, t).start()
            if before is not None:
                from_rows(*before)
            before = (m, n)

        @pl.when(jnp.logical_not(outer))
        def _():
            for m, n in pieces:
                w_cross(m, n).start()

        from_rows(*before)
        for m, n in pieces:
            for t in range(halves):
                landed(held(m, 2 * t + (1 - side), n), wt_recv.at[m, n, t]).wait()

    def arrive(f, s, n):
        for step in range(s, s + n):
            if step > 0:
                for v, dst in enumerate((rx, rg)):
                    landed(dst.at[fixed(f, step)], xg_recv.at[v, f, step]).wait()

    def process(f, s, n):
        rows = fixed(f, s, n)
        for c in range(ff // tile):
            cols = pl.ds(c * tile, tile)
            z = dot(rx[rows, :], win[f, :, cols], 1, 0)
            e = dot(rg[rows, :], wout[f, cols, :], 1, 1)
            zz = z * z
            t = jnp.tanh(ROOT * (z + CUBE * (zz * z)))
            part = 0.5 * (1.0 + t)
            hb[rows, cols] = (z * part).astype(BF16)
            slope = part + 0.5 * z * (1.0 - t * t) * (ROOT * (1.0 + 3.0 * CUBE * zz))
            fb[rows, cols] = (e * slope).astype(BF16)
        for c in range(sub // tile):
            cols = pl.ds(c * tile, tile)
            back = dot(fb[rows, :], win[f, cols, :], 1, 1).astype(BF16)
            for step in range(s, s + n):
                piece = back[(step - s) * cap : (step - s + 1) * cap]
                if step == 0:
                    rr[fixed(f, step), cols] = piece
                else:
                    rs[fixed(f, step), cols] = piece

    def reply(f, s, n):
        for step in range(s, s + n):
            if step > 0:
                r_copy(f, step).start()

    block = dwo.shape[1]

    def product(f, q):
        cols = rows_of(q, block)
        rows = fixed(f, 0, half)
        po[f, q] = dot(hb[rows, cols], rg[rows, :], 0, 0).astype(BF16)
        pi[f, q] = dot(rx[rows, cols], fb[rows, :], 0, 0).astype(BF16)

    def exchange(f, early):
        @pl.loop(0, halves)
        def _(i):
            t = lax.rem(row + 1 + i, halves)
            product(f, 2 * t + (1 - side))
            twin_copy(f, 0, 2 * t + (1 - side), t).start()
            twin_copy(f, 1, 2 * t + (1 - side), t).start()
            product(f, 2 * t + side)

            @pl.when(t != row)
            def _():
                for s, (own, got, out) in enumerate(((po, tpo, so), (pi, tpi, si))):
                    landed(got.at[f, t], t_recv.at[f, s, t]).wait()
                    out[f, t] = (own[f, 2 * t + side].astype(F32) + got[f, t].astype(F32)).astype(BF16)
                    if s == 0 or not early:
                        row_copy(f, s, t).start()
                    else:
                        pl.when(inner == 1)(lambda s=s: row_copy(f, s, t).start())

    def total(f, s):
        own, got, sums = ((po, tpo, rpo), (pi, tpi, rpi))[s]
        landed(got.at[f, row], t_recv.at[f, s, row]).wait()
        out = own[f, mine].astype(F32) + got[f, row].astype(F32)
        for t in others:
            row_got(f, s, t).wait()
            out = out + sums[f, t].astype(F32)
        return out

    def scatter(f, s, n, start=False):
        ones = []
        for step in range(s, s + n):
            if step > 0:
                landed(rr.at[fixed(f, step)], r_recv.at[f, step]).wait()
            h0, h1 = hot(f, step)
            ones.append((h0 | h1).astype(F32).astype(BF16))
        more = dot(jnp.concatenate(ones, axis=0), rr[fixed(f, s, n), :], 0, 0)
        acc[...] = more if start else acc[...] + more

    def pass_on(s):
        out = (cpo, cpi)[s]
        out[...] = total(1, s).astype(BF16)
        cross_copy(s).start()

    near_part, far_part = (0, half // 2), (half // 2, half // 2)
    pl.when(inner == 1)(weights)
    arrive(first, *near_part)
    process(first, *near_part)
    reply(first, *near_part)
    arrive(first, *far_part)

    @pl.when(inner == 1)
    def _():
        for step in far_steps:
            send(first, step)

    process(first, *far_part)
    pl.when(outer)(lambda: reply(first, *far_part))
    exchange(first, True)
    pl.when(outer)(weights)
    arrive(second, *near_part)
    process(second, *near_part)
    reply(second, *near_part)
    arrive(second, *far_part)
    for step in far_steps:
        xg_copy(0, first, step).wait_send()
        xg_copy(1, first, step).wait_send()
    pl.when(inner == 1)(lambda: reply(first, *far_part))
    process(second, *far_part)
    reply(second, *far_part)

    @pl.when(inner == 1)
    def _():
        pass_on(0)
        pass_on(1)

    exchange(second, False)

    @pl.when(outer)
    def _():
        for t in others:
            row_copy(first, 1, t).start()
        pass_on(0)
        pass_on(1)

    scatter(first, 0, half // 2, True)
    scatter(second, 0, half // 2)
    scatter(second, half // 2, half // 2)
    for s, out in enumerate((dwo, dwi)):
        out[0] = total(0, s)
    scatter(first, half // 2, half // 2)
    for h in range(heads):
        dx[:, pl.ds(h * sub, sub)] = acc[pl.ds(h * tokens, tokens), :].astype(BF16)
    for s, (out, got) in enumerate(((dwo, gpo), (dwi, gpi))):
        landed(got, c_recv.at[s]).wait()
        out[0] = out[0] + got[...].astype(F32)

    for step in far_steps:
        xg_copy(0, second, step).wait_send()
        xg_copy(1, second, step).wait_send()
    for f in range(2):
        for step in near:
            if step < half // 2:
                xg_copy(0, f, step).wait_send()
                xg_copy(1, f, step).wait_send()
            r_copy(f, step).wait_send()
        for s in range(2):
            for t in range(halves):
                twin_copy(f, s, 2 * t + (1 - side), t).wait_send()
            for t in others:
                row_copy(f, s, t).wait_send()
    for m, n in pieces:
        w_cross(m, n).wait_send()
        for t in range(halves):
            w_twin(m, n, t).wait_send()
        for t in others:
            w_row(m, n, t).wait_send()
    for s in range(2):
        cross_copy(s).wait_send()


def paired_call(
    sub_inputs,
    out_grads,
    expert_outputs,
    combine_weights,
    expert_ids,
    slot_ids,
    expert_input_weight,
    expert_output_weight,
):
    tokens, heads, top = expert_ids.shape
    _, sub, ff = expert_input_weight.shape
    groups = lax.axis_size("expert")
    replicas = lax.axis_size("dp")
    cap = top * heads * tokens // groups

    def flat(a):
        return a.transpose(2, 1, 0).reshape(top, heads * tokens)

    slots = groups * cap
    half = groups // 2
    halves = replicas // 2
    part = sub // replicas
    part_out = ff // replicas
    dims = (groups, replicas, cap, heads, tokens, sub, ff)
    any_spec = pl.BlockSpec(memory_space=pltpu.HBM)
    vmem = pl.BlockSpec(memory_space=pltpu.VMEM)
    dma = pltpu.SemaphoreType.DMA
    rows = heads * tokens
    d_inputs, dw_in, dw_out, gate_dots = pl.pallas_call(
        functools.partial(paired, dims),
        out_shape=(
            jax.ShapeDtypeStruct((tokens, heads * sub), BF16),
            jax.ShapeDtypeStruct((1, part, ff), F32),
            jax.ShapeDtypeStruct((1, part_out, sub), F32),
            jax.ShapeDtypeStruct((top, heads * tokens), F32),
        ),
        in_specs=[vmem, vmem, vmem, any_spec, any_spec, any_spec, any_spec, any_spec],
        out_specs=(vmem, vmem, vmem, vmem),
        scratch_shapes=[
            pltpu.VMEM((top, rows), jnp.int32),
            pltpu.VMEM((rows, sub), BF16),
            pltpu.VMEM((rows, sub), BF16),
            pltpu.VMEM((2, sub, ff), BF16),
            pltpu.VMEM((2, ff, sub), BF16),
            *[pltpu.VMEM((slots, sub), BF16)] * 6,
            pltpu.VMEM((slots, ff), BF16),
            pltpu.VMEM((slots, ff), BF16),
            pltpu.VMEM((rows, sub), F32),
            pltpu.VMEM((2, replicas, part_out, sub), BF16),
            pltpu.VMEM((2, replicas, part, ff), BF16),
            *[pltpu.VMEM((2, halves, part_out, sub), BF16), pltpu.VMEM((2, halves, part, ff), BF16)] * 3,
            *[pltpu.VMEM((part_out, sub), BF16), pltpu.VMEM((part, ff), BF16)] * 2,
            pltpu.VMEM((tokens, heads, top, sub), BF16),
            pltpu.VMEM((tokens, 128), F32),
            dma((2 * heads + 3,)),
            *[dma((2, 2, half))] * 2,
            *[dma((2, half))] * 2,
            *[dma((2, PIECES))] * 2,
            *[dma((2, PIECES, halves))] * 4,
            *[dma((2, 2, halves))] * 4,
            *[dma((2,))] * 2,
        ],
        compiler_params=pltpu.CompilerParams(
            collective_id=0, has_side_effects=True, vmem_limit_bytes=63 * 1024 * 1024
        ),
        cost_estimate=pl.CostEstimate(flops=20 * 10**9, bytes_accessed=2**24, transcendentals=0),
    )(
        flat(expert_ids), flat(slot_ids), flat(combine_weights),
        sub_inputs, out_grads, expert_input_weight, expert_output_weight, expert_outputs,
    )
    d_gates = gate_dots.reshape(top, heads, tokens).transpose(2, 1, 0)
    return (d_inputs, d_gates, dw_in, dw_out)


def on_device(*args):
    tokens, heads, top = args[4].shape
    _, sub, ff = args[6].shape
    groups = lax.axis_size("expert")
    replicas = lax.axis_size("dp")
    cap = top * heads * tokens // groups
    half = groups // 2
    fits = half >= 4 and half & (half - 1) == 0 and replicas % 2 == 0 and cap % 128 == 0 and tokens % 128 == 0
    tokens_cross = half * replicas * cap * 3 * sub
    weights_cross = 4 * sub * ff
    if fits and weights_cross < tokens_cross:
        return paired_call(*args)
    return plain_call(*args)


def solution(mesh):
    rows = P(("expert", "dp"), None)
    table = P(("expert", "dp"), None, None)
    return jax.shard_map(
        on_device,
        mesh=mesh,
        in_specs=(
            rows,
            rows,
            P(("expert", "dp"), None, None, None),
            table,
            table,
            table,
            P("expert", None, None),
            P("expert", None, None),
        ),
        out_specs=(rows, table, P("expert", "dp", None), P("expert", "dp", None)),
        check_vma=False,
    )
```

```python
import functools

import jax
import jax.numpy as jnp
from jax import lax
from jax.experimental import pallas as pl
from jax.experimental.pallas import tpu as pltpu
from jax.sharding import PartitionSpec as P

MESH = pl.DeviceIdType.MESH
F32 = jnp.float32
BF16 = jnp.bfloat16
ROOT = 0.7978845608028654
CUBE = 0.044715


def partner(me, step, count):
    if count & (count - 1):
        return lax.rem(step - me + count, count)
    out, bit = 0, 1
    while bit < count:
        out = out + ((me // bit + step // bit) % 2) * bit
        bit *= 2
    return out


def spread(i, count):
    return lax.rem(i + 1, count)


def dot(a, b, ca, cb):
    return lax.dot_general(a, b, (((ca,), (cb,)), ((), ())), preferred_element_type=F32)


def kernel(
    dims,
    tgt, cw, x_hbm, g_hbm, win_hbm, wout_hbm, eo_hbm,
    dx, dwi, dwo, dg,
    xs, gs, win, wout, sx, sg, rx, rg, rs, rr, hb, fb, acc, po, pi, tpo, tpi, so, si, rpo, rpi,
    ev, load_sem, xg_send, xg_recv, r_send, r_recv, t_send, t_recv, w_send, w_recv,
):
    groups, replicas, cap, heads, tokens, sub, ff = dims
    chunk = max(cap, 128)
    per = chunk // cap
    chunks = groups * cap // chunk
    tile = 256
    me = lax.axis_index("expert")
    mine = lax.axis_index("dp")
    my_chunk = me // per
    halves = replicas // 2
    row, side = mine // 2, mine % 2
    twin = row * 2 + (1 - side)

    loads = []
    for h in range(heads):
        for s, (src, dst) in enumerate(((x_hbm, xs), (g_hbm, gs))):
            loads.append(
                pltpu.make_async_copy(
                    src.at[:, pl.ds(h * sub, sub)], dst.at[pl.ds(h * tokens, tokens)], load_sem.at[2 * h + s]
                )
            )
    wloads = [
        pltpu.make_async_copy(win_hbm.at[0], win, load_sem.at[2 * heads]),
        pltpu.make_async_copy(wout_hbm.at[0], wout, load_sem.at[2 * heads + 1]),
        pltpu.make_async_copy(eo_hbm, ev, load_sem.at[2 * heads + 2]),
    ]
    for c in loads + wloads:
        c.start()

    barrier = pltpu.get_barrier_semaphore()

    @pl.loop(1, groups)
    def _(i):
        pl.semaphore_signal(barrier, inc=1, device_id={"expert": lax.rem(me + i, groups)}, device_id_type=MESH)

    @pl.loop(1, replicas)
    def _(i):
        pl.semaphore_signal(barrier, inc=1, device_id={"dp": lax.rem(mine + i, replicas)}, device_id_type=MESH)

    pl.semaphore_wait(barrier, groups + replicas - 2)
    for c in loads:
        c.wait()

    def rows_of(index, size):
        return pl.ds(pl.multiple_of(index * size, size), size)

    def hot(j):
        slots = lax.broadcasted_iota(jnp.int32, (chunk, tgt.shape[1]), 0) + j * chunk
        return tgt[0:1, :] == slots, tgt[1:2, :] == slots

    def xg_copy(s, peer):
        src, dst = ((sx, rx), (sg, rg))[s]
        return pltpu.make_async_remote_copy(
            src_ref=src.at[rows_of(peer, cap)], dst_ref=dst.at[rows_of(me, cap)],
            send_sem=xg_send.at[s, peer], recv_sem=xg_recv.at[s, me],
            device_id={"expert": peer}, device_id_type=MESH,
        )

    def xg_local(s, src_dev):
        src, dst = ((sx, rx), (sg, rg))[s]
        return pltpu.make_async_copy(
            src.at[rows_of(src_dev, cap)], dst.at[rows_of(src_dev, cap)], xg_recv.at[s, src_dev]
        )

    def r_copy(peer):
        return pltpu.make_async_remote_copy(
            src_ref=rs.at[rows_of(peer, cap)], dst_ref=rr.at[rows_of(me, cap)],
            send_sem=r_send.at[peer], recv_sem=r_recv.at[me],
            device_id={"expert": peer}, device_id_type=MESH,
        )

    def r_local(src_dev):
        return pltpu.make_async_copy(
            rs.at[rows_of(src_dev, cap)], rr.at[rows_of(src_dev, cap)], r_recv.at[src_dev]
        )

    def twin_copy(s, q, t):
        src, dst = ((po, tpo), (pi, tpi))[s]
        return pltpu.make_async_remote_copy(
            src_ref=src.at[q], dst_ref=dst.at[t],
            send_sem=t_send.at[s, t], recv_sem=t_recv.at[s, t],
            device_id={"dp": twin}, device_id_type=MESH,
        )

    def row_copy(s, t):
        src, dst = ((so, rpo), (si, rpi))[s]
        return pltpu.make_async_remote_copy(
            src_ref=src.at[t], dst_ref=dst.at[row],
            send_sem=w_send.at[s, t], recv_sem=w_recv.at[s, row],
            device_id={"dp": 2 * t + side}, device_id_type=MESH,
        )

    def row_got(s, t):
        dst = (rpo, rpi)[s]
        return pltpu.make_async_copy(dst.at[t], dst.at[t], w_recv.at[s, t])

    @pl.loop(0, chunks)
    def _(i):
        j = partner(my_chunk, spread(i, chunks), chunks)
        h0, h1 = hot(j)
        one = (h0 | h1).astype(F32).astype(BF16)
        w = jnp.sum(jnp.where(h0, cw[0:1, :], 0.0) + jnp.where(h1, cw[1:2, :], 0.0), axis=1, keepdims=True)
        sx[rows_of(j, chunk), :] = dot(one, xs[...], 1, 0).astype(BF16)
        sg[rows_of(j, chunk), :] = (dot(one, gs[...], 1, 0) * w).astype(BF16)
        for p in range(per):
            peer = j * per + p

            @pl.when(peer != me)
            def _():
                xg_copy(0, peer).start()
                xg_copy(1, peer).start()

            @pl.when(peer == me)
            def _():
                xg_local(0, me).start()
                xg_local(1, me).start()

    for c in wloads:
        c.wait()

    span = 16
    for h in range(heads):

        @pl.loop(0, tokens // span)
        def _(b):
            grads = gs[rows_of(h * (tokens // span) + b, span), :].astype(F32)
            terms = ev[rows_of(b, span), h].astype(F32) * grads[:, None, :]
            dg[h, rows_of(b, span), :] = jnp.sum(terms, axis=-1)

    @pl.loop(0, chunks)
    def _(i):
        j = partner(my_chunk, spread(lax.rem(i + chunks - 1, chunks), chunks), chunks)
        for p in range(per):
            xg_local(0, j * per + p).wait()
            xg_local(1, j * per + p).wait()
        rows = rows_of(j, chunk)
        for n in range(ff // tile):
            cols = pl.ds(n * tile, tile)
            z = dot(rx[rows, :], win[:, cols], 1, 0)
            e = dot(rg[rows, :], wout[cols, :], 1, 1)
            zz = z * z
            t = jnp.tanh(ROOT * (z + CUBE * (zz * z)))
            half = 0.5 * (1.0 + t)
            hb[rows, cols] = (z * half).astype(BF16)
            slope = half + 0.5 * z * (1.0 - t * t) * (ROOT * (1.0 + 3.0 * CUBE * zz))
            fb[rows, cols] = (e * slope).astype(BF16)
        for n in range(sub // tile):
            cols = pl.ds(n * tile, tile)
            rs[rows, cols] = dot(fb[rows, :], win[cols, :], 1, 1).astype(BF16)
        for p in range(per):
            peer = j * per + p

            @pl.when(peer != me)
            def _():
                r_copy(peer).start()

            @pl.when(peer == me)
            def _():
                r_local(me).start()

    block = dwo.shape[1]
    def product(q):
        cols = rows_of(q, block)
        po[q] = dot(hb[:, cols], rg[...], 0, 0).astype(BF16)
        pi[q] = dot(rx[:, cols], fb[...], 0, 0).astype(BF16)

    @pl.loop(0, halves)
    def _(i):
        t = lax.rem(row + 1 + i, halves)
        product(2 * t + (1 - side))
        twin_copy(0, 2 * t + (1 - side), t).start()
        twin_copy(1, 2 * t + (1 - side), t).start()
        product(2 * t + side)

        @pl.when(t != row)
        def _():
            for s, (own, got, out) in enumerate(((po, tpo, so), (pi, tpi, si))):
                twin_copy(s, 2 * t + side, t).wait_recv()
                out[t] = (own[2 * t + side].astype(F32) + got[t].astype(F32)).astype(BF16)
                row_copy(s, t).start()

    acc[...] = jnp.zeros_like(acc)

    @pl.loop(0, chunks)
    def _(i):
        j = partner(my_chunk, spread(lax.rem(i + chunks - 1, chunks), chunks), chunks)
        for p in range(per):
            r_local(j * per + p).wait()
        h0, h1 = hot(j)
        one = (h0 | h1).astype(F32).astype(BF16)
        acc[...] += dot(one, rr[rows_of(j, chunk), :], 0, 0)

    for h in range(heads):
        dx[:, pl.ds(h * sub, sub)] = acc[pl.ds(h * tokens, tokens), :].astype(BF16)

    for s, (out, own, got, sums) in enumerate(((dwo, po, tpo, rpo), (dwi, pi, tpi, rpi))):
        twin_copy(s, mine, row).wait_recv()
        out[0] = own[mine].astype(F32) + got[row].astype(F32)

        @pl.loop(1, halves)
        def _(i):
            t = lax.rem(row + i, halves)
            row_got(s, t).wait()
            out[0] = out[0] + sums[t].astype(F32)

    @pl.loop(1, groups)
    def _(i):
        peer = lax.rem(me + i, groups)
        xg_copy(0, peer).wait_send()
        xg_copy(1, peer).wait_send()
        r_copy(peer).wait_send()

    for s in range(2):

        @pl.loop(0, halves)
        def _(i):
            twin_copy(s, 2 * i + (1 - side), i).wait_send()

        @pl.loop(1, halves)
        def _(i):
            row_copy(s, lax.rem(row + i, halves)).wait_send()


def plain_call(
    sub_inputs,
    out_grads,
    expert_outputs,
    combine_weights,
    expert_ids,
    slot_ids,
    expert_input_weight,
    expert_output_weight,
):
    tokens, heads, top = expert_ids.shape
    _, sub, ff = expert_input_weight.shape
    groups = lax.axis_size("expert")
    replicas = lax.axis_size("dp")
    cap = top * heads * tokens // groups
    kept = slot_ids >= 0
    target = jnp.where(kept, expert_ids * cap + slot_ids, -1)
    target = target.transpose(2, 1, 0).reshape(top, heads * tokens)
    weight = combine_weights.transpose(2, 1, 0).reshape(top, heads * tokens)
    slots = groups * cap
    part = sub // replicas
    part_out = ff // replicas
    dims = (groups, replicas, cap, heads, tokens, sub, ff)
    any_spec = pl.BlockSpec(memory_space=pltpu.HBM)
    vmem = pl.BlockSpec(memory_space=pltpu.VMEM)
    dma = pltpu.SemaphoreType.DMA
    d_inputs, dw_in, dw_out, gate_dots = pl.pallas_call(
        functools.partial(kernel, dims),
        out_shape=(
            jax.ShapeDtypeStruct((tokens, heads * sub), BF16),
            jax.ShapeDtypeStruct((1, part, ff), F32),
            jax.ShapeDtypeStruct((1, part_out, sub), F32),
            jax.ShapeDtypeStruct((heads, tokens, top), F32),
        ),
        in_specs=[vmem, vmem, any_spec, any_spec, any_spec, any_spec, any_spec],
        out_specs=(vmem, vmem, vmem, vmem),
        scratch_shapes=[
            pltpu.VMEM((heads * tokens, sub), BF16),
            pltpu.VMEM((heads * tokens, sub), BF16),
            pltpu.VMEM((sub, ff), BF16),
            pltpu.VMEM((ff, sub), BF16),
            pltpu.VMEM((slots, sub), BF16),
            pltpu.VMEM((slots, sub), BF16),
            pltpu.VMEM((slots, sub), BF16),
            pltpu.VMEM((slots, sub), BF16),
            pltpu.VMEM((slots, sub), BF16),
            pltpu.VMEM((slots, sub), BF16),
            pltpu.VMEM((slots, ff), BF16),
            pltpu.VMEM((slots, ff), BF16),
            pltpu.VMEM((heads * tokens, sub), F32),
            pltpu.VMEM((replicas, part_out, sub), BF16),
            pltpu.VMEM((replicas, part, ff), BF16),
            *[pltpu.VMEM((replicas // 2, part_out, sub), BF16), pltpu.VMEM((replicas // 2, part, ff), BF16)] * 3,
            pltpu.VMEM((tokens, heads, top, sub), BF16),
            dma((2 * heads + 3,)),
            dma((2, groups)),
            dma((2, groups)),
            dma((groups,)),
            dma((groups,)),
            *[dma((2, replicas // 2))] * 4,
        ],
        compiler_params=pltpu.CompilerParams(
            collective_id=0, has_side_effects=True, vmem_limit_bytes=60 * 1024 * 1024
        ),
        cost_estimate=pl.CostEstimate(flops=20 * 10**9, bytes_accessed=2**24, transcendentals=0),
    )(target, weight, sub_inputs, out_grads, expert_input_weight, expert_output_weight, expert_outputs)
    d_gates = jnp.where(kept, gate_dots.transpose(1, 0, 2), jnp.float32(0.0))
    return (d_inputs, d_gates, dw_in, dw_out)


PIECES = 2


def paired(
    dims,
    ids, slot, cw, x_hbm, g_hbm, win_hbm, wout_hbm, eo_hbm,
    dx, dwi, dwo, dg,
    tgt, xs, gs, win, wout, sx, sg, rx, rg, rs, rr, hb, fb, acc, po, pi, tpo, tpi, so, si, rpo, rpi,
    cpo, cpi, gpo, gpi, ev, gates,
    load_sem, xg_send, xg_recv, r_send, r_recv, wz_send, wz_recv, wt_send, wt_recv, wy_send, wy_recv,
    t_send, t_recv, y_send, y_recv, c_send, c_recv,
):
    groups, replicas, cap, heads, tokens, sub, ff = dims
    tile = 256
    me = lax.axis_index("expert")
    mine = lax.axis_index("dp")
    half = groups // 2
    halves = replicas // 2
    low = lax.rem(me, half)
    base = me - low
    opposite = lax.rem(me + half, groups)
    inner = lax.rem(me // half + low // (half // 2), 2)
    outer = inner == 0
    first, second = inner, 1 - inner
    row, side = mine // 2, mine % 2
    twin = row * 2 + (1 - side)
    near = range(1, half)

    def rows_of(index, size):
        return pl.ds(pl.multiple_of(index * size, size), size)

    def fixed(f, s, n=1):
        return pl.ds(pl.multiple_of((f * half + s) * cap, cap), n * cap)

    def landed(ref, sem):
        return pltpu.make_async_copy(ref, ref, sem)

    def remote(src, dst, send, recv, where):
        return pltpu.make_async_remote_copy(
            src_ref=src, dst_ref=dst, send_sem=send, recv_sem=recv, device_id=where, device_id_type=MESH
        )

    loads = []
    for h in range(heads):
        for s, (src, dst) in enumerate(((x_hbm, xs), (g_hbm, gs))):
            loads.append(
                pltpu.make_async_copy(
                    src.at[:, pl.ds(h * sub, sub)], dst.at[pl.ds(h * tokens, tokens)], load_sem.at[2 * h + s]
                )
            )
    wloads = [
        pltpu.make_async_copy(win_hbm.at[0], win.at[0], load_sem.at[2 * heads]),
        pltpu.make_async_copy(wout_hbm.at[0], wout.at[0], load_sem.at[2 * heads + 1]),
    ]
    eload = pltpu.make_async_copy(eo_hbm, ev, load_sem.at[2 * heads + 2])
    for c in loads + wloads + [eload]:
        c.start()

    barrier = pltpu.get_barrier_semaphore()
    for s in near:
        pl.semaphore_signal(
            barrier, inc=1, device_id={"expert": base + partner(low, s, half)}, device_id_type=MESH
        )
    pl.semaphore_signal(barrier, inc=1, device_id={"expert": opposite}, device_id_type=MESH)
    for i in range(1, replicas):
        pl.semaphore_signal(barrier, inc=1, device_id={"dp": lax.rem(mine + i, replicas)}, device_id_type=MESH)
    def owner(s):
        return base + partner(low, s, half)

    def part_of(m, quarter, n):
        size = (sub, ff)[m] // replicas // PIECES
        return rows_of(quarter * PIECES + n, size)

    def held(m, quarter, n):
        return (win, wout)[m].at[1, part_of(m, quarter, n)]

    def w_cross(m, n):
        return remote(
            (win_hbm, wout_hbm)[m].at[0, part_of(m, mine, n)], held(m, mine, n),
            wz_send.at[m, n], wz_recv.at[m, n], {"expert": opposite},
        )

    def w_twin(m, n, t):
        ref = held(m, 2 * t + side, n)
        return remote(ref, ref, wt_send.at[m, n, t], wt_recv.at[m, n, t], {"dp": twin})

    def w_row(m, n, t):
        ref = held(m, mine, n)
        return remote(ref, ref, wy_send.at[m, n, t], wy_recv.at[m, n, row], {"dp": 2 * t + side})

    def xg_copy(s, f, step):
        src, dst = ((sx, rx), (sg, rg))[s]
        return remote(
            src.at[fixed(f, step)], dst.at[fixed(f, step)],
            xg_send.at[s, f, step], xg_recv.at[s, f, step], {"expert": owner(step)},
        )

    def r_copy(f, step):
        return remote(
            rs.at[fixed(f, step)], rr.at[fixed(f, step)],
            r_send.at[f, step], r_recv.at[f, step], {"expert": owner(step)},
        )

    def twin_copy(f, s, q, t):
        src, dst = ((po, tpo), (pi, tpi))[s]
        return remote(src.at[f, q], dst.at[f, t], t_send.at[f, s, t], t_recv.at[f, s, t], {"dp": twin})

    def cut(s, n):
        size = (dwo, dwi)[s].shape[1] // PIECES
        return pl.ds(n * size, size)

    def row_copy(f, s, t, n):
        src, dst = ((so, rpo), (si, rpi))[s]
        return remote(
            src.at[f, t, cut(s, n)], dst.at[f, row, cut(s, n)],
            y_send.at[f, s, n, t], y_recv.at[f, s, n, row], {"dp": 2 * t + side},
        )

    def cross_copy(s, n):
        src, dst = ((cpo, gpo), (cpi, gpi))[s]
        return remote(
            src.at[cut(s, n)], dst.at[cut(s, n)], c_send.at[s, n], c_recv.at[s, n], {"expert": opposite}
        )

    pieces = [(m, n) for m in range(2) for n in range(PIECES)]

    tgt[...] = jnp.where(slot[...] >= 0, ids[...] * cap + slot[...], -1)

    def hot(f, step):
        first = lax.rem(owner(step) + f * half, groups) * cap
        slots = lax.broadcasted_iota(jnp.int32, (cap, tgt.shape[1]), 0) + first
        return tgt[0:1, :] == slots, tgt[1:2, :] == slots

    def gather(f, step, out_x, out_g):
        h0, h1 = hot(f, step)
        one = (h0 | h1).astype(F32).astype(BF16)
        w = jnp.sum(jnp.where(h0, cw[0:1, :], 0.0) + jnp.where(h1, cw[1:2, :], 0.0), axis=1, keepdims=True)
        rows = rows_of(f * half + step, cap)
        out_x[rows, :] = dot(one, xs[...], 1, 0).astype(BF16)
        out_g[rows, :] = (dot(one, gs[...], 1, 0) * w).astype(BF16)

    for c in loads:
        c.wait()
    far_steps = range(half // 2, half)

    def send(f, step):
        xg_copy(0, f, step).start()
        xg_copy(1, f, step).start()

    @pl.loop(half // 2, half)
    def _(step):
        gather(second, step, sx, sg)

    pl.semaphore_wait(barrier, half + replicas - 1)

    @pl.when(outer)
    def _():
        for m, n in pieces:
            w_cross(m, n).start()

    for step in far_steps:
        send(second, step)

    @pl.loop(0, 2)
    def _(i):
        f = first + i * (second - first)

        @pl.loop(1, half // 2)
        def _(step):
            gather(f, step, sx, sg)
            send(f, step)

        gather(f, 0, rx, rg)

    @pl.loop(half // 2, half)
    def _(step):
        gather(first, step, sx, sg)
        pl.when(outer)(lambda: send(first, step))

    eload.wait()
    span = 16
    lane = lax.broadcasted_iota(jnp.int32, (span, gates.shape[1]), 1)

    @pl.loop(0, tokens // span)
    def _(b):
        found = jnp.zeros((span, gates.shape[1]), F32)
        for h in range(heads):
            grads = gs[rows_of(h * (tokens // span) + b, span), :].astype(F32)
            terms = ev[rows_of(b, span), h].astype(F32) * grads[:, None, :]
            sums = jnp.sum(terms, axis=-1)
            for k in range(2):
                found = jnp.where(lane == 2 * h + k, sums[:, k : k + 1], found)
        gates[rows_of(b, span), :] = found

    turned = gates[...].T
    for h in range(heads):
        cols = pl.ds(h * tokens, tokens)
        dg[:, cols] = jnp.where(slot[:, cols] >= 0, turned[2 * h : 2 * h + 2, :], 0.0)

    for c in wloads:
        c.wait()

    others = [lax.rem(row + i, halves) for i in range(1, halves)]

    def from_rows(m, n):
        for t in others:
            landed(held(m, 2 * t + side, n), wy_recv.at[m, n, t]).wait()
            w_twin(m, n, t).start()

    def weights():
        before = None
        for m, n in pieces:
            landed(held(m, mine, n), wz_recv.at[m, n]).wait()
            w_twin(m, n, row).start()
            for t in others:
                w_row(m, n, t).start()
            if before is not None:
                from_rows(*before)
            before = (m, n)
            if before == pieces[-1]:

                @pl.when(inner == 1)
                def _():
                    xg_copy(0, first, half // 2).start()
                    for piece in pieces:
                        w_cross(*piece).start()

        from_rows(*before)
        for m, n in pieces:
            for t in range(halves):
                landed(held(m, 2 * t + (1 - side), n), wt_recv.at[m, n, t]).wait()

    def arrive(f, s, n):
        for step in range(s, s + n):
            if step > 0:
                for v, dst in enumerate((rx, rg)):
                    landed(dst.at[fixed(f, step)], xg_recv.at[v, f, step]).wait()

    def process(f, s, n):
        rows = fixed(f, s, n)
        for c in range(ff // tile):
            cols = pl.ds(c * tile, tile)
            z = dot(rx[rows, :], win[f, :, cols], 1, 0)
            e = dot(rg[rows, :], wout[f, cols, :], 1, 1)
            zz = z * z
            t = jnp.tanh(ROOT * (z + CUBE * (zz * z)))
            part = 0.5 * (1.0 + t)
            hb[rows, cols] = (z * part).astype(BF16)
            slope = part + 0.5 * z * (1.0 - t * t) * (ROOT * (1.0 + 3.0 * CUBE * zz))
            fb[rows, cols] = (e * slope).astype(BF16)
        for c in range(sub // tile):
            cols = pl.ds(c * tile, tile)
            back = dot(fb[rows, :], win[f, cols, :], 1, 1).astype(BF16)
            for step in range(s, s + n):
                piece = back[(step - s) * cap : (step - s + 1) * cap]
                if step == 0:
                    rr[fixed(f, step), cols] = piece
                else:
                    rs[fixed(f, step), cols] = piece

    def reply(f, s, n):
        for step in range(s, s + n):
            if step > 0:
                r_copy(f, step).start()

    block = dwo.shape[1]

    def product(f, q):
        cols = rows_of(q, block)
        rows = fixed(f, 0, half)
        po[f, q] = dot(hb[rows, cols], rg[rows, :], 0, 0).astype(BF16)
        pi[f, q] = dot(rx[rows, cols], fb[rows, :], 0, 0).astype(BF16)

    def rows_out(f, s, t):
        for n in range(PIECES):
            row_copy(f, s, t, n).start()

    def exchange(f, early):
        @pl.loop(0, halves)
        def _(i):
            t = lax.rem(row + 1 + i, halves)
            product(f, 2 * t + (1 - side))
            twin_copy(f, 0, 2 * t + (1 - side), t).start()
            twin_copy(f, 1, 2 * t + (1 - side), t).start()
            product(f, 2 * t + side)

            @pl.when(t != row)
            def _():
                for s, (own, got, out) in enumerate(((po, tpo, so), (pi, tpi, si))):
                    landed(got.at[f, t], t_recv.at[f, s, t]).wait()
                    out[f, t] = (own[f, 2 * t + side].astype(F32) + got[f, t].astype(F32)).astype(BF16)
                    if s == 0 or not early:
                        rows_out(f, s, t)
                    else:
                        pl.when(inner == 1)(lambda s=s: rows_out(f, s, t))

    def total(f, s, n):
        own, got, sums = ((po, tpo, rpo), (pi, tpi, rpi))[s]
        if n == 0:
            landed(got.at[f, row], t_recv.at[f, s, row]).wait()
        out = own[f, mine, cut(s, n)].astype(F32) + got[f, row, cut(s, n)].astype(F32)
        for t in others:
            landed(sums.at[f, t, cut(s, n)], y_recv.at[f, s, n, t]).wait()
            out = out + sums[f, t, cut(s, n)].astype(F32)
        return out

    def scatter(f, s, n, start=False):
        ones = []
        for step in range(s, s + n):
            if step > 0:
                landed(rr.at[fixed(f, step)], r_recv.at[f, step]).wait()
            h0, h1 = hot(f, step)
            ones.append((h0 | h1).astype(F32).astype(BF16))
        more = dot(jnp.concatenate(ones, axis=0), rr[fixed(f, s, n), :], 0, 0)
        acc[...] = more if start else acc[...] + more

    def pass_on(s):
        out = (cpo, cpi)[s]
        for n in range(PIECES):
            out[cut(s, n)] = total(1, s, n).astype(BF16)
            cross_copy(s, n).start()

    near_part, far_part = (0, half // 2), (half // 2, half // 2)
    pl.when(inner == 1)(weights)
    arrive(first, *near_part)
    process(first, *near_part)
    reply(first, *near_part)
    arrive(first, *far_part)

    @pl.when(inner == 1)
    def _():
        xg_copy(1, first, half // 2).start()
        for step in far_steps[1:]:
            send(first, step)

    process(first, *far_part)
    pl.when(outer)(lambda: reply(first, *far_part))
    exchange(first, True)
    pl.when(outer)(weights)
    arrive(second, *near_part)
    process(second, *near_part)
    reply(second, *near_part)
    arrive(second, *far_part)
    for step in far_steps:
        xg_copy(0, first, step).wait_send()
        xg_copy(1, first, step).wait_send()
    pl.when(inner == 1)(lambda: reply(first, *far_part))
    process(second, *far_part)
    reply(second, *far_part)

    @pl.when(inner == 1)
    def _():
        pass_on(0)
        pass_on(1)

    exchange(second, False)

    @pl.when(outer)
    def _():
        for t in others:
            rows_out(first, 1, t)
        pass_on(0)
        pass_on(1)

    scatter(first, 0, half // 2, True)
    scatter(second, 0, half // 2)
    scatter(second, half // 2, half // 2)
    for s, out in enumerate((dwo, dwi)):
        for n in range(PIECES):
            out[0, cut(s, n)] = total(0, s, n)
    scatter(first, half // 2, half // 2)
    for h in range(heads):
        dx[:, pl.ds(h * sub, sub)] = acc[pl.ds(h * tokens, tokens), :].astype(BF16)
    for s, (out, got) in enumerate(((dwo, gpo), (dwi, gpi))):
        for n in range(PIECES):
            landed(got.at[cut(s, n)], c_recv.at[s, n]).wait()
            out[0, cut(s, n)] = out[0, cut(s, n)] + got[cut(s, n)].astype(F32)

    for step in far_steps:
        xg_copy(0, second, step).wait_send()
        xg_copy(1, second, step).wait_send()
    for f in range(2):
        for step in near:
            if step < half // 2:
                xg_copy(0, f, step).wait_send()
                xg_copy(1, f, step).wait_send()
            r_copy(f, step).wait_send()
        for s in range(2):
            for t in range(halves):
                twin_copy(f, s, 2 * t + (1 - side), t).wait_send()
            for t in others:
                for n in range(PIECES):
                    row_copy(f, s, t, n).wait_send()
    for m, n in pieces:
        w_cross(m, n).wait_send()
        for t in range(halves):
            w_twin(m, n, t).wait_send()
        for t in others:
            w_row(m, n, t).wait_send()
    for s in range(2):
        for n in range(PIECES):
            cross_copy(s, n).wait_send()


def put_out(*refs):
    count = len(refs) // 2
    sems = refs[-1]
    copies = [pltpu.make_async_copy(refs[i], refs[count + i], sems.at[i]) for i in range(count)]
    for c in copies:
        c.start()
    for c in copies:
        c.wait()


def paired_call(
    sub_inputs,
    out_grads,
    expert_outputs,
    combine_weights,
    expert_ids,
    slot_ids,
    expert_input_weight,
    expert_output_weight,
):
    tokens, heads, top = expert_ids.shape
    _, sub, ff = expert_input_weight.shape
    groups = lax.axis_size("expert")
    replicas = lax.axis_size("dp")
    cap = top * heads * tokens // groups

    def flat(a):
        return a.transpose(2, 1, 0).reshape(top, heads * tokens)

    slots = groups * cap
    half = groups // 2
    halves = replicas // 2
    part = sub // replicas
    part_out = ff // replicas
    dims = (groups, replicas, cap, heads, tokens, sub, ff)
    any_spec = pl.BlockSpec(memory_space=pltpu.HBM)
    vmem = pl.BlockSpec(memory_space=pltpu.VMEM)
    dma = pltpu.SemaphoreType.DMA
    rows = heads * tokens
    shapes = (
        ((tokens, heads * sub), BF16),
        ((1, part, ff), F32),
        ((1, part_out, sub), F32),
        ((top, heads * tokens), F32),
    )
    results = pl.pallas_call(
        functools.partial(paired, dims),
        out_shape=tuple(pltpu.VMEM(shape, kind) for shape, kind in shapes),
        in_specs=[vmem, vmem, vmem, any_spec, any_spec, any_spec, any_spec, any_spec],
        out_specs=(vmem, vmem, vmem, vmem),
        scratch_shapes=[
            pltpu.VMEM((top, rows), jnp.int32),
            pltpu.VMEM((rows, sub), BF16),
            pltpu.VMEM((rows, sub), BF16),
            pltpu.VMEM((2, sub, ff), BF16),
            pltpu.VMEM((2, ff, sub), BF16),
            *[pltpu.VMEM((slots, sub), BF16)] * 6,
            pltpu.VMEM((slots, ff), BF16),
            pltpu.VMEM((slots, ff), BF16),
            pltpu.VMEM((rows, sub), F32),
            pltpu.VMEM((2, replicas, part_out, sub), BF16),
            pltpu.VMEM((2, replicas, part, ff), BF16),
            *[pltpu.VMEM((2, halves, part_out, sub), BF16), pltpu.VMEM((2, halves, part, ff), BF16)] * 3,
            *[pltpu.VMEM((part_out, sub), BF16), pltpu.VMEM((part, ff), BF16)] * 2,
            pltpu.VMEM((tokens, heads, top, sub), BF16),
            pltpu.VMEM((tokens, 128), F32),
            dma((2 * heads + 3,)),
            *[dma((2, 2, half))] * 2,
            *[dma((2, half))] * 2,
            *[dma((2, PIECES))] * 2,
            *[dma((2, PIECES, halves))] * 4,
            *[dma((2, 2, halves))] * 2,
            *[dma((2, 2, PIECES, halves))] * 2,
            *[dma((2, PIECES))] * 2,
        ],
        compiler_params=pltpu.CompilerParams(
            collective_id=0, has_side_effects=True, vmem_limit_bytes=59 * 1024 * 1024
        ),
        cost_estimate=pl.CostEstimate(flops=20 * 10**9, bytes_accessed=2**24, transcendentals=0),
    )(
        flat(expert_ids), flat(slot_ids), flat(combine_weights),
        sub_inputs, out_grads, expert_input_weight, expert_output_weight, expert_outputs,
    )
    d_inputs, dw_in, dw_out, gate_dots = pl.pallas_call(
        put_out,
        out_shape=tuple(jax.ShapeDtypeStruct(shape, kind) for shape, kind in shapes),
        in_specs=[vmem] * len(shapes),
        out_specs=(any_spec,) * len(shapes),
        scratch_shapes=[dma((len(shapes),))],
        compiler_params=pltpu.CompilerParams(vmem_limit_bytes=1024 * 1024),
    )(*results)
    d_gates = gate_dots.reshape(top, heads, tokens).transpose(2, 1, 0)
    return (d_inputs, d_gates, dw_in, dw_out)


def on_device(*args):
    tokens, heads, top = args[4].shape
    _, sub, ff = args[6].shape
    groups = lax.axis_size("expert")
    replicas = lax.axis_size("dp")
    cap = top * heads * tokens // groups
    half = groups // 2
    fits = half >= 4 and half & (half - 1) == 0 and replicas % 2 == 0 and cap % 128 == 0 and tokens % 128 == 0
    tokens_cross = half * replicas * cap * 3 * sub
    weights_cross = 4 * sub * ff
    if fits and weights_cross < tokens_cross:
        return paired_call(*args)
    return plain_call(*args)


def solution(mesh):
    rows = P(("expert", "dp"), None)
    table = P(("expert", "dp"), None, None)
    return jax.shard_map(
        on_device,
        mesh=mesh,
        in_specs=(
            rows,
            rows,
            P(("expert", "dp"), None, None, None),
            table,
            table,
            table,
            P("expert", None, None),
            P("expert", None, None),
        ),
        out_specs=(rows, table, P("expert", "dp", None), P("expert", "dp", None)),
        check_vma=False,
    )
```

```python
import functools

import jax
import jax.numpy as jnp
from jax import lax
from jax.experimental import pallas as pl
from jax.experimental.pallas import tpu as pltpu
from jax.sharding import PartitionSpec as P

MESH = pl.DeviceIdType.MESH
F32 = jnp.float32
BF16 = jnp.bfloat16
ROOT = 0.7978845608028654
CUBE = 0.044715


def partner(me, step, count):
    if count & (count - 1):
        return lax.rem(step - me + count, count)
    out, bit = 0, 1
    while bit < count:
        out = out + ((me // bit + step // bit) % 2) * bit
        bit *= 2
    return out


def spread(i, count):
    return lax.rem(i + 1, count)


def dot(a, b, ca, cb):
    return lax.dot_general(a, b, (((ca,), (cb,)), ((), ())), preferred_element_type=F32)


def kernel(
    dims,
    tgt, cw, x_hbm, g_hbm, win_hbm, wout_hbm, eo_hbm,
    dx, dwi, dwo, dg,
    xs, gs, win, wout, sx, sg, rx, rg, rs, rr, hb, fb, acc, po, pi, tpo, tpi, so, si, rpo, rpi,
    ev, load_sem, xg_send, xg_recv, r_send, r_recv, t_send, t_recv, w_send, w_recv,
):
    groups, replicas, cap, heads, tokens, sub, ff = dims
    chunk = max(cap, 128)
    per = chunk // cap
    chunks = groups * cap // chunk
    tile = 256
    me = lax.axis_index("expert")
    mine = lax.axis_index("dp")
    my_chunk = me // per
    halves = replicas // 2
    row, side = mine // 2, mine % 2
    twin = row * 2 + (1 - side)

    loads = []
    for h in range(heads):
        for s, (src, dst) in enumerate(((x_hbm, xs), (g_hbm, gs))):
            loads.append(
                pltpu.make_async_copy(
                    src.at[:, pl.ds(h * sub, sub)], dst.at[pl.ds(h * tokens, tokens)], load_sem.at[2 * h + s]
                )
            )
    wloads = [
        pltpu.make_async_copy(win_hbm.at[0], win, load_sem.at[2 * heads]),
        pltpu.make_async_copy(wout_hbm.at[0], wout, load_sem.at[2 * heads + 1]),
        pltpu.make_async_copy(eo_hbm, ev, load_sem.at[2 * heads + 2]),
    ]
    for c in loads + wloads:
        c.start()

    barrier = pltpu.get_barrier_semaphore()

    @pl.loop(1, groups)
    def _(i):
        pl.semaphore_signal(barrier, inc=1, device_id={"expert": lax.rem(me + i, groups)}, device_id_type=MESH)

    @pl.loop(1, replicas)
    def _(i):
        pl.semaphore_signal(barrier, inc=1, device_id={"dp": lax.rem(mine + i, replicas)}, device_id_type=MESH)

    pl.semaphore_wait(barrier, groups + replicas - 2)
    for c in loads:
        c.wait()

    def rows_of(index, size):
        return pl.ds(pl.multiple_of(index * size, size), size)

    def hot(j):
        slots = lax.broadcasted_iota(jnp.int32, (chunk, tgt.shape[1]), 0) + j * chunk
        return tgt[0:1, :] == slots, tgt[1:2, :] == slots

    def xg_copy(s, peer):
        src, dst = ((sx, rx), (sg, rg))[s]
        return pltpu.make_async_remote_copy(
            src_ref=src.at[rows_of(peer, cap)], dst_ref=dst.at[rows_of(me, cap)],
            send_sem=xg_send.at[s, peer], recv_sem=xg_recv.at[s, me],
            device_id={"expert": peer}, device_id_type=MESH,
        )

    def xg_local(s, src_dev):
        src, dst = ((sx, rx), (sg, rg))[s]
        return pltpu.make_async_copy(
            src.at[rows_of(src_dev, cap)], dst.at[rows_of(src_dev, cap)], xg_recv.at[s, src_dev]
        )

    def r_copy(peer):
        return pltpu.make_async_remote_copy(
            src_ref=rs.at[rows_of(peer, cap)], dst_ref=rr.at[rows_of(me, cap)],
            send_sem=r_send.at[peer], recv_sem=r_recv.at[me],
            device_id={"expert": peer}, device_id_type=MESH,
        )

    def r_local(src_dev):
        return pltpu.make_async_copy(
            rs.at[rows_of(src_dev, cap)], rr.at[rows_of(src_dev, cap)], r_recv.at[src_dev]
        )

    def twin_copy(s, q, t):
        src, dst = ((po, tpo), (pi, tpi))[s]
        return pltpu.make_async_remote_copy(
            src_ref=src.at[q], dst_ref=dst.at[t],
            send_sem=t_send.at[s, t], recv_sem=t_recv.at[s, t],
            device_id={"dp": twin}, device_id_type=MESH,
        )

    def row_copy(s, t):
        src, dst = ((so, rpo), (si, rpi))[s]
        return pltpu.make_async_remote_copy(
            src_ref=src.at[t], dst_ref=dst.at[row],
            send_sem=w_send.at[s, t], recv_sem=w_recv.at[s, row],
            device_id={"dp": 2 * t + side}, device_id_type=MESH,
        )

    def row_got(s, t):
        dst = (rpo, rpi)[s]
        return pltpu.make_async_copy(dst.at[t], dst.at[t], w_recv.at[s, t])

    @pl.loop(0, chunks)
    def _(i):
        j = partner(my_chunk, spread(i, chunks), chunks)
        h0, h1 = hot(j)
        one = (h0 | h1).astype(F32).astype(BF16)
        w = jnp.sum(jnp.where(h0, cw[0:1, :], 0.0) + jnp.where(h1, cw[1:2, :], 0.0), axis=1, keepdims=True)
        sx[rows_of(j, chunk), :] = dot(one, xs[...], 1, 0).astype(BF16)
        sg[rows_of(j, chunk), :] = (dot(one, gs[...], 1, 0) * w).astype(BF16)
        for p in range(per):
            peer = j * per + p

            @pl.when(peer != me)
            def _():
                xg_copy(0, peer).start()
                xg_copy(1, peer).start()

            @pl.when(peer == me)
            def _():
                xg_local(0, me).start()
                xg_local(1, me).start()

    for c in wloads:
        c.wait()

    span = 16
    for h in range(heads):

        @pl.loop(0, tokens // span)
        def _(b):
            grads = gs[rows_of(h * (tokens // span) + b, span), :].astype(F32)
            terms = ev[rows_of(b, span), h].astype(F32) * grads[:, None, :]
            dg[h, rows_of(b, span), :] = jnp.sum(terms, axis=-1)

    @pl.loop(0, chunks)
    def _(i):
        j = partner(my_chunk, spread(lax.rem(i + chunks - 1, chunks), chunks), chunks)
        for p in range(per):
            xg_local(0, j * per + p).wait()
            xg_local(1, j * per + p).wait()
        rows = rows_of(j, chunk)
        for n in range(ff // tile):
            cols = pl.ds(n * tile, tile)
            z = dot(rx[rows, :], win[:, cols], 1, 0)
            e = dot(rg[rows, :], wout[cols, :], 1, 1)
            zz = z * z
            t = jnp.tanh(ROOT * (z + CUBE * (zz * z)))
            half = 0.5 * (1.0 + t)
            hb[rows, cols] = (z * half).astype(BF16)
            slope = half + 0.5 * z * (1.0 - t * t) * (ROOT * (1.0 + 3.0 * CUBE * zz))
            fb[rows, cols] = (e * slope).astype(BF16)
        for n in range(sub // tile):
            cols = pl.ds(n * tile, tile)
            rs[rows, cols] = dot(fb[rows, :], win[cols, :], 1, 1).astype(BF16)
        for p in range(per):
            peer = j * per + p

            @pl.when(peer != me)
            def _():
                r_copy(peer).start()

            @pl.when(peer == me)
            def _():
                r_local(me).start()

    block = dwo.shape[1]
    def product(q):
        cols = rows_of(q, block)
        po[q] = dot(hb[:, cols], rg[...], 0, 0).astype(BF16)
        pi[q] = dot(rx[:, cols], fb[...], 0, 0).astype(BF16)

    @pl.loop(0, halves)
    def _(i):
        t = lax.rem(row + 1 + i, halves)
        product(2 * t + (1 - side))
        twin_copy(0, 2 * t + (1 - side), t).start()
        twin_copy(1, 2 * t + (1 - side), t).start()
        product(2 * t + side)

        @pl.when(t != row)
        def _():
            for s, (own, got, out) in enumerate(((po, tpo, so), (pi, tpi, si))):
                twin_copy(s, 2 * t + side, t).wait_recv()
                out[t] = (own[2 * t + side].astype(F32) + got[t].astype(F32)).astype(BF16)
                row_copy(s, t).start()

    acc[...] = jnp.zeros_like(acc)

    @pl.loop(0, chunks)
    def _(i):
        j = partner(my_chunk, spread(lax.rem(i + chunks - 1, chunks), chunks), chunks)
        for p in range(per):
            r_local(j * per + p).wait()
        h0, h1 = hot(j)
        one = (h0 | h1).astype(F32).astype(BF16)
        acc[...] += dot(one, rr[rows_of(j, chunk), :], 0, 0)

    for h in range(heads):
        dx[:, pl.ds(h * sub, sub)] = acc[pl.ds(h * tokens, tokens), :].astype(BF16)

    for s, (out, own, got, sums) in enumerate(((dwo, po, tpo, rpo), (dwi, pi, tpi, rpi))):
        twin_copy(s, mine, row).wait_recv()
        out[0] = own[mine].astype(F32) + got[row].astype(F32)

        @pl.loop(1, halves)
        def _(i):
            t = lax.rem(row + i, halves)
            row_got(s, t).wait()
            out[0] = out[0] + sums[t].astype(F32)

    @pl.loop(1, groups)
    def _(i):
        peer = lax.rem(me + i, groups)
        xg_copy(0, peer).wait_send()
        xg_copy(1, peer).wait_send()
        r_copy(peer).wait_send()

    for s in range(2):

        @pl.loop(0, halves)
        def _(i):
            twin_copy(s, 2 * i + (1 - side), i).wait_send()

        @pl.loop(1, halves)
        def _(i):
            row_copy(s, lax.rem(row + i, halves)).wait_send()


def plain_call(
    sub_inputs,
    out_grads,
    expert_outputs,
    combine_weights,
    expert_ids,
    slot_ids,
    expert_input_weight,
    expert_output_weight,
):
    tokens, heads, top = expert_ids.shape
    _, sub, ff = expert_input_weight.shape
    groups = lax.axis_size("expert")
    replicas = lax.axis_size("dp")
    cap = top * heads * tokens // groups
    kept = slot_ids >= 0
    target = jnp.where(kept, expert_ids * cap + slot_ids, -1)
    target = target.transpose(2, 1, 0).reshape(top, heads * tokens)
    weight = combine_weights.transpose(2, 1, 0).reshape(top, heads * tokens)
    slots = groups * cap
    part = sub // replicas
    part_out = ff // replicas
    dims = (groups, replicas, cap, heads, tokens, sub, ff)
    any_spec = pl.BlockSpec(memory_space=pltpu.HBM)
    vmem = pl.BlockSpec(memory_space=pltpu.VMEM)
    dma = pltpu.SemaphoreType.DMA
    d_inputs, dw_in, dw_out, gate_dots = pl.pallas_call(
        functools.partial(kernel, dims),
        out_shape=(
            jax.ShapeDtypeStruct((tokens, heads * sub), BF16),
            jax.ShapeDtypeStruct((1, part, ff), F32),
            jax.ShapeDtypeStruct((1, part_out, sub), F32),
            jax.ShapeDtypeStruct((heads, tokens, top), F32),
        ),
        in_specs=[vmem, vmem, any_spec, any_spec, any_spec, any_spec, any_spec],
        out_specs=(vmem, vmem, vmem, vmem),
        scratch_shapes=[
            pltpu.VMEM((heads * tokens, sub), BF16),
            pltpu.VMEM((heads * tokens, sub), BF16),
            pltpu.VMEM((sub, ff), BF16),
            pltpu.VMEM((ff, sub), BF16),
            pltpu.VMEM((slots, sub), BF16),
            pltpu.VMEM((slots, sub), BF16),
            pltpu.VMEM((slots, sub), BF16),
            pltpu.VMEM((slots, sub), BF16),
            pltpu.VMEM((slots, sub), BF16),
            pltpu.VMEM((slots, sub), BF16),
            pltpu.VMEM((slots, ff), BF16),
            pltpu.VMEM((slots, ff), BF16),
            pltpu.VMEM((heads * tokens, sub), F32),
            pltpu.VMEM((replicas, part_out, sub), BF16),
            pltpu.VMEM((replicas, part, ff), BF16),
            *[pltpu.VMEM((replicas // 2, part_out, sub), BF16), pltpu.VMEM((replicas // 2, part, ff), BF16)] * 3,
            pltpu.VMEM((tokens, heads, top, sub), BF16),
            dma((2 * heads + 3,)),
            dma((2, groups)),
            dma((2, groups)),
            dma((groups,)),
            dma((groups,)),
            *[dma((2, replicas // 2))] * 4,
        ],
        compiler_params=pltpu.CompilerParams(
            collective_id=0, has_side_effects=True, vmem_limit_bytes=60 * 1024 * 1024
        ),
        cost_estimate=pl.CostEstimate(flops=20 * 10**9, bytes_accessed=2**24, transcendentals=0),
    )(target, weight, sub_inputs, out_grads, expert_input_weight, expert_output_weight, expert_outputs)
    d_gates = jnp.where(kept, gate_dots.transpose(1, 0, 2), jnp.float32(0.0))
    return (d_inputs, d_gates, dw_in, dw_out)


PIECES = 2


def paired(
    dims,
    ids, slot, cw, x_hbm, g_hbm, win_hbm, wout_hbm, eo_hbm,
    dx, dwi, dwo, dg,
    tgt, xs, gs, win, wout, sx, sg, rx, rg, rs, rr, hb, fb, acc, po, pi, tpo, tpi, so, si, rpo, rpi,
    cpo, cpi, gpo, gpi, ev, gates,
    load_sem, xg_send, xg_recv, r_send, r_recv, wz_send, wz_recv, wt_send, wt_recv, wy_send, wy_recv,
    t_send, t_recv, y_send, y_recv, c_send, c_recv, a_send, a_recv,
):
    groups, replicas, cap, heads, tokens, sub, ff = dims
    tile = 256
    me = lax.axis_index("expert")
    mine = lax.axis_index("dp")
    half = groups // 2
    halves = replicas // 2
    low = lax.rem(me, half)
    base = me - low
    opposite = lax.rem(me + half, groups)
    inner = lax.rem(me // half + low // (half // 2), 2)
    outer = inner == 0
    first, second = inner, 1 - inner
    row, side = mine // 2, mine % 2
    twin = row * 2 + (1 - side)
    near = range(1, half)

    def rows_of(index, size):
        return pl.ds(pl.multiple_of(index * size, size), size)

    def fixed(f, s, n=1):
        return pl.ds(pl.multiple_of((f * (half + 1) + s) * cap, cap), n * cap)

    def landed(ref, sem):
        return pltpu.make_async_copy(ref, ref, sem)

    def remote(src, dst, send, recv, where):
        return pltpu.make_async_remote_copy(
            src_ref=src, dst_ref=dst, send_sem=send, recv_sem=recv, device_id=where, device_id_type=MESH
        )

    loads = []
    for h in range(heads):
        for s, (src, dst) in enumerate(((x_hbm, xs), (g_hbm, gs))):
            loads.append(
                pltpu.make_async_copy(
                    src.at[:, pl.ds(h * sub, sub)], dst.at[pl.ds(h * tokens, tokens)], load_sem.at[2 * h + s]
                )
            )
    wloads = [
        pltpu.make_async_copy(win_hbm.at[0], win.at[0], load_sem.at[2 * heads]),
        pltpu.make_async_copy(wout_hbm.at[0], wout.at[0], load_sem.at[2 * heads + 1]),
    ]
    eload = pltpu.make_async_copy(eo_hbm, ev, load_sem.at[2 * heads + 2])
    for c in loads + wloads + [eload]:
        c.start()

    barrier = pltpu.get_barrier_semaphore()
    for s in near:
        pl.semaphore_signal(
            barrier, inc=1, device_id={"expert": base + partner(low, s, half)}, device_id_type=MESH
        )
    pl.semaphore_signal(barrier, inc=1, device_id={"expert": opposite}, device_id_type=MESH)
    for i in range(1, replicas):
        pl.semaphore_signal(barrier, inc=1, device_id={"dp": lax.rem(mine + i, replicas)}, device_id_type=MESH)
    turn = half // 2
    across = lax.rem(base + partner(low, turn, half) + half, groups)

    @pl.when(inner == 1)
    def _():
        pl.semaphore_signal(barrier, inc=1, device_id={"expert": across}, device_id_type=MESH)
    def owner(s):
        return base + partner(low, s, half)

    def part_of(m, quarter, n):
        size = (sub, ff)[m] // replicas // PIECES
        return rows_of(quarter * PIECES + n, size)

    def held(m, quarter, n):
        return (win, wout)[m].at[1, part_of(m, quarter, n)]

    def w_cross(m, n):
        return remote(
            (win_hbm, wout_hbm)[m].at[0, part_of(m, mine, n)], held(m, mine, n),
            wz_send.at[m, n], wz_recv.at[m, n], {"expert": opposite},
        )

    def w_twin(m, n, t):
        ref = held(m, 2 * t + side, n)
        return remote(ref, ref, wt_send.at[m, n, t], wt_recv.at[m, n, t], {"dp": twin})

    def w_row(m, n, t):
        ref = held(m, mine, n)
        return remote(ref, ref, wy_send.at[m, n, t], wy_recv.at[m, n, row], {"dp": 2 * t + side})

    def xg_copy(s, f, step):
        src, dst = ((sx, rx), (sg, rg))[s]
        return remote(
            src.at[fixed(f, step)], dst.at[fixed(f, step)],
            xg_send.at[s, f, step], xg_recv.at[s, f, step], {"expert": owner(step)},
        )

    def across_copy(s):
        src, dst = ((sx, rx), (sg, rg))[s]
        return remote(
            src.at[fixed(1, turn)], dst.at[fixed(0, half)], a_send.at[s], a_recv.at[s], {"expert": across}
        )

    def across_reply():
        return remote(
            rs.at[fixed(0, half)], rr.at[fixed(1, turn)], a_send.at[2], r_recv.at[1, turn], {"expert": across}
        )

    def r_copy(f, step):
        return remote(
            rs.at[fixed(f, step)], rr.at[fixed(f, step)],
            r_send.at[f, step], r_recv.at[f, step], {"expert": owner(step)},
        )

    def twin_copy(f, s, q, t):
        src, dst = ((po, tpo), (pi, tpi))[s]
        return remote(src.at[f, q], dst.at[f, t], t_send.at[f, s, t], t_recv.at[f, s, t], {"dp": twin})

    def cut(s, n):
        size = (dwo, dwi)[s].shape[1] // PIECES
        return pl.ds(n * size, size)

    def row_copy(f, s, t, n):
        src, dst = ((so, rpo), (si, rpi))[s]
        return remote(
            src.at[f, t, cut(s, n)], dst.at[f, row, cut(s, n)],
            y_send.at[f, s, n, t], y_recv.at[f, s, n, row], {"dp": 2 * t + side},
        )

    def cross_copy(s, n):
        src, dst = ((cpo, gpo), (cpi, gpi))[s]
        return remote(
            src.at[cut(s, n)], dst.at[cut(s, n)], c_send.at[s, n], c_recv.at[s, n], {"expert": opposite}
        )

    pieces = [(m, n) for m in range(2) for n in range(PIECES)]

    tgt[...] = jnp.where(slot[...] >= 0, ids[...] * cap + slot[...], -1)

    def hot(f, step):
        first = lax.rem(owner(step) + f * half, groups) * cap
        slots = lax.broadcasted_iota(jnp.int32, (cap, tgt.shape[1]), 0) + first
        return tgt[0:1, :] == slots, tgt[1:2, :] == slots

    def gather(f, step, out_x, out_g):
        h0, h1 = hot(f, step)
        one = (h0 | h1).astype(F32).astype(BF16)
        w = jnp.sum(jnp.where(h0, cw[0:1, :], 0.0) + jnp.where(h1, cw[1:2, :], 0.0), axis=1, keepdims=True)
        rows = fixed(f, step)
        out_x[rows, :] = dot(one, xs[...], 1, 0).astype(BF16)
        out_g[rows, :] = (dot(one, gs[...], 1, 0) * w).astype(BF16)

    for c in loads:
        c.wait()
    far_steps = range(half // 2, half)

    def send(f, step):
        xg_copy(0, f, step).start()
        xg_copy(1, f, step).start()

    @pl.loop(half // 2, half)
    def _(step):
        gather(second, step, sx, sg)

    pl.semaphore_wait(barrier, half + replicas - 1 + inner)

    @pl.when(outer)
    def _():
        for m, n in pieces:
            w_cross(m, n).start()

    for step in far_steps:
        send(second, step)

    @pl.loop(0, 2)
    def _(i):
        f = first + i * (second - first)

        @pl.loop(1, half // 2)
        def _(step):
            gather(f, step, sx, sg)
            send(f, step)

        gather(f, 0, rx, rg)

    @pl.loop(half // 2, half)
    def _(step):
        gather(first, step, sx, sg)
        pl.when(outer)(lambda: send(first, step))

    eload.wait()
    span = 16
    lane = lax.broadcasted_iota(jnp.int32, (span, gates.shape[1]), 1)

    @pl.loop(0, tokens // span)
    def _(b):
        found = jnp.zeros((span, gates.shape[1]), F32)
        for h in range(heads):
            grads = gs[rows_of(h * (tokens // span) + b, span), :].astype(F32)
            terms = ev[rows_of(b, span), h].astype(F32) * grads[:, None, :]
            sums = jnp.sum(terms, axis=-1)
            for k in range(2):
                found = jnp.where(lane == 2 * h + k, sums[:, k : k + 1], found)
        gates[rows_of(b, span), :] = found

    turned = gates[...].T
    for h in range(heads):
        cols = pl.ds(h * tokens, tokens)
        dg[:, cols] = jnp.where(slot[:, cols] >= 0, turned[2 * h : 2 * h + 2, :], 0.0)

    for c in wloads:
        c.wait()

    others = [lax.rem(row + i, halves) for i in range(1, halves)]

    def from_rows(m, n):
        for t in others:
            landed(held(m, 2 * t + side, n), wy_recv.at[m, n, t]).wait()
            w_twin(m, n, t).start()

    def rows_out(f, s, t):
        for n in range(PIECES):
            row_copy(f, s, t, n).start()

    def weights():
        before = None
        for m, n in pieces:
            landed(held(m, mine, n), wz_recv.at[m, n]).wait()
            w_twin(m, n, row).start()
            for t in others:
                w_row(m, n, t).start()
            if before is not None:
                from_rows(*before)
            before = (m, n)
            if before == pieces[-1]:

                @pl.when(outer)
                def _():
                    for t in others:
                        rows_out(first, 0, t)

                @pl.when(inner == 1)
                def _():
                    for piece in pieces:
                        w_cross(*piece).start()

        from_rows(*before)
        for m, n in pieces:
            for t in range(halves):
                landed(held(m, 2 * t + (1 - side), n), wt_recv.at[m, n, t]).wait()

    def arrive(f, s, n):
        for step in range(s, s + n):
            if step > 0:
                for v, dst in enumerate((rx, rg)):
                    landed(dst.at[fixed(f, step)], xg_recv.at[v, f, step]).wait()

    def arrive_across():
        for v, dst in enumerate((rx, rg)):
            landed(dst.at[fixed(0, half)], a_recv.at[v]).wait()

    def process(f, s, n):
        rows = fixed(f, s, n)
        for c in range(ff // tile):
            cols = pl.ds(c * tile, tile)
            z = dot(rx[rows, :], win[f, :, cols], 1, 0)
            e = dot(rg[rows, :], wout[f, cols, :], 1, 1)
            zz = z * z
            t = jnp.tanh(ROOT * (z + CUBE * (zz * z)))
            part = 0.5 * (1.0 + t)
            hb[rows, cols] = (z * part).astype(BF16)
            slope = part + 0.5 * z * (1.0 - t * t) * (ROOT * (1.0 + 3.0 * CUBE * zz))
            fb[rows, cols] = (e * slope).astype(BF16)
        for c in range(sub // tile):
            cols = pl.ds(c * tile, tile)
            back = dot(fb[rows, :], win[f, cols, :], 1, 1).astype(BF16)
            for step in range(s, s + n):
                piece = back[(step - s) * cap : (step - s + 1) * cap]
                if step == 0:
                    rr[fixed(f, step), cols] = piece
                else:
                    rs[fixed(f, step), cols] = piece

    def reply(f, s, n):
        for step in range(s, s + n):
            if step > 0:
                r_copy(f, step).start()

    block = dwo.shape[1]

    def product(f, q, n):
        cols = rows_of(q, block)
        rows = fixed(f, 0, n)
        po[f, q] = dot(hb[rows, cols], rg[rows, :], 0, 0).astype(BF16)
        pi[f, q] = dot(rx[rows, cols], fb[rows, :], 0, 0).astype(BF16)

    def exchange(f, early, n):
        @pl.loop(0, halves)
        def _(i):
            t = lax.rem(row + 1 + i, halves)
            product(f, 2 * t + (1 - side), n)
            twin_copy(f, 0, 2 * t + (1 - side), t).start()
            twin_copy(f, 1, 2 * t + (1 - side), t).start()
            product(f, 2 * t + side, n)

            @pl.when(t != row)
            def _():
                for s, (own, got, out) in enumerate(((po, tpo, so), (pi, tpi, si))):
                    landed(got.at[f, t], t_recv.at[f, s, t]).wait()
                    out[f, t] = (own[f, 2 * t + side].astype(F32) + got[f, t].astype(F32)).astype(BF16)
                    if early:
                        pl.when(inner == 1)(lambda s=s: rows_out(f, s, t))
                    else:
                        rows_out(f, s, t)

    def total(f, s, n):
        own, got, sums = ((po, tpo, rpo), (pi, tpi, rpi))[s]
        if n == 0:
            landed(got.at[f, row], t_recv.at[f, s, row]).wait()
        out = own[f, mine, cut(s, n)].astype(F32) + got[f, row, cut(s, n)].astype(F32)
        for t in others:
            landed(sums.at[f, t, cut(s, n)], y_recv.at[f, s, n, t]).wait()
            out = out + sums[f, t, cut(s, n)].astype(F32)
        return out

    def scatter(f, s, n, start=False):
        ones = []
        for step in range(s, s + n):
            if step > 0:
                landed(rr.at[fixed(f, step)], r_recv.at[f, step]).wait()
            h0, h1 = hot(f, step)
            ones.append((h0 | h1).astype(F32).astype(BF16))
        more = dot(jnp.concatenate(ones, axis=0), rr[fixed(f, s, n), :], 0, 0)
        acc[...] = more if start else acc[...] + more

    def pass_on(s):
        out = (cpo, cpi)[s]
        for n in range(PIECES):
            out[cut(s, n)] = total(1, s, n).astype(BF16)
            cross_copy(s, n).start()

    near_part, far_part = (0, turn), (turn, turn)
    last_part = (turn + 1, turn - 1)

    @pl.when(outer)
    def _():
        rx[fixed(1, turn), :] = jnp.zeros((cap, sub), BF16)
        rg[fixed(1, turn), :] = jnp.zeros((cap, sub), BF16)

    pl.when(inner == 1)(weights)
    arrive(first, *near_part)
    process(first, *near_part)
    reply(first, *near_part)
    arrive(first, *far_part)

    @pl.when(inner == 1)
    def _():
        for step in far_steps[1:]:
            send(first, step)
        across_copy(0).start()
        across_copy(1).start()

    process(first, *far_part)
    pl.when(outer)(lambda: reply(first, *far_part))
    exchange(first, True, half)
    pl.when(outer)(weights)
    arrive(second, *near_part)
    process(second, *near_part)
    reply(second, *near_part)

    @pl.when(inner == 1)
    def _():
        for step in far_steps[1:]:
            xg_copy(0, first, step).wait_send()
            xg_copy(1, first, step).wait_send()
        reply(first, *far_part)
        arrive_across()
        process(0, half, 1)
        across_reply().start()
        pass_on(0)
        arrive(second, turn, 1)

    arrive(second, *last_part)
    process(second, *far_part)
    pl.when(inner == 1)(lambda: reply(second, turn, 1))
    reply(second, *last_part)

    @pl.when(inner == 1)
    def _():
        pass_on(1)
        exchange(0, False, half + 1)

    @pl.when(outer)
    def _():
        exchange(1, False, half)
        for t in others:
            rows_out(first, 1, t)
        pass_on(0)
        pass_on(1)

    scatter(first, 0, half // 2, True)
    scatter(second, 0, half // 2)
    scatter(second, half // 2, half // 2)
    for s, out in enumerate((dwo, dwi)):
        for n in range(PIECES):
            out[0, cut(s, n)] = total(0, s, n)
    scatter(first, half // 2, half // 2)
    for h in range(heads):
        dx[:, pl.ds(h * sub, sub)] = acc[pl.ds(h * tokens, tokens), :].astype(BF16)
    for s, (out, got) in enumerate(((dwo, gpo), (dwi, gpi))):
        for n in range(PIECES):
            landed(got.at[cut(s, n)], c_recv.at[s, n]).wait()
            out[0, cut(s, n)] = out[0, cut(s, n)] + got[cut(s, n)].astype(F32)

    for step in far_steps:
        xg_copy(0, second, step).wait_send()
        xg_copy(1, second, step).wait_send()

    @pl.when(outer)
    def _():
        for step in far_steps:
            xg_copy(0, first, step).wait_send()
            xg_copy(1, first, step).wait_send()
        r_copy(first, turn).wait_send()

    @pl.when(inner == 1)
    def _():
        across_copy(0).wait_send()
        across_copy(1).wait_send()
        across_reply().wait_send()
        r_copy(first, turn).wait_send()
        r_copy(second, turn).wait_send()

    for f in range(2):
        for step in near:
            if step < turn:
                xg_copy(0, f, step).wait_send()
                xg_copy(1, f, step).wait_send()
            if step != turn:
                r_copy(f, step).wait_send()
        for s in range(2):
            for t in range(halves):
                twin_copy(f, s, 2 * t + (1 - side), t).wait_send()
            for t in others:
                for n in range(PIECES):
                    row_copy(f, s, t, n).wait_send()
    for m, n in pieces:
        w_cross(m, n).wait_send()
        for t in range(halves):
            w_twin(m, n, t).wait_send()
        for t in others:
            w_row(m, n, t).wait_send()
    for s in range(2):
        for n in range(PIECES):
            cross_copy(s, n).wait_send()


def put_out(*refs):
    count = len(refs) // 2
    sems = refs[-1]
    copies = [pltpu.make_async_copy(refs[i], refs[count + i], sems.at[i]) for i in range(count)]
    for c in copies:
        c.start()
    for c in copies:
        c.wait()


def paired_call(
    sub_inputs,
    out_grads,
    expert_outputs,
    combine_weights,
    expert_ids,
    slot_ids,
    expert_input_weight,
    expert_output_weight,
):
    tokens, heads, top = expert_ids.shape
    _, sub, ff = expert_input_weight.shape
    groups = lax.axis_size("expert")
    replicas = lax.axis_size("dp")
    cap = top * heads * tokens // groups

    def flat(a):
        return a.transpose(2, 1, 0).reshape(top, heads * tokens)

    slots = (groups + 1) * cap
    half = groups // 2
    halves = replicas // 2
    part = sub // replicas
    part_out = ff // replicas
    dims = (groups, replicas, cap, heads, tokens, sub, ff)
    any_spec = pl.BlockSpec(memory_space=pltpu.HBM)
    vmem = pl.BlockSpec(memory_space=pltpu.VMEM)
    dma = pltpu.SemaphoreType.DMA
    rows = heads * tokens
    shapes = (
        ((tokens, heads * sub), BF16),
        ((1, part, ff), F32),
        ((1, part_out, sub), F32),
        ((top, heads * tokens), F32),
    )
    results = pl.pallas_call(
        functools.partial(paired, dims),
        out_shape=tuple(pltpu.VMEM(shape, kind) for shape, kind in shapes),
        in_specs=[vmem, vmem, vmem, any_spec, any_spec, any_spec, any_spec, any_spec],
        out_specs=(vmem, vmem, vmem, vmem),
        scratch_shapes=[
            pltpu.VMEM((top, rows), jnp.int32),
            pltpu.VMEM((rows, sub), BF16),
            pltpu.VMEM((rows, sub), BF16),
            pltpu.VMEM((2, sub, ff), BF16),
            pltpu.VMEM((2, ff, sub), BF16),
            *[pltpu.VMEM((slots, sub), BF16)] * 6,
            pltpu.VMEM((slots, ff), BF16),
            pltpu.VMEM((slots, ff), BF16),
            pltpu.VMEM((rows, sub), F32),
            pltpu.VMEM((2, replicas, part_out, sub), BF16),
            pltpu.VMEM((2, replicas, part, ff), BF16),
            *[pltpu.VMEM((2, halves, part_out, sub), BF16), pltpu.VMEM((2, halves, part, ff), BF16)] * 3,
            *[pltpu.VMEM((part_out, sub), BF16), pltpu.VMEM((part, ff), BF16)] * 2,
            pltpu.VMEM((tokens, heads, top, sub), BF16),
            pltpu.VMEM((tokens, 128), F32),
            dma((2 * heads + 3,)),
            *[dma((2, 2, half))] * 2,
            *[dma((2, half))] * 2,
            *[dma((2, PIECES))] * 2,
            *[dma((2, PIECES, halves))] * 4,
            *[dma((2, 2, halves))] * 2,
            *[dma((2, 2, PIECES, halves))] * 2,
            *[dma((2, PIECES))] * 2,
            dma((3,)),
            dma((2,)),
        ],
        compiler_params=pltpu.CompilerParams(
            collective_id=0, has_side_effects=True, vmem_limit_bytes=59 * 1024 * 1024
        ),
        cost_estimate=pl.CostEstimate(flops=20 * 10**9, bytes_accessed=2**24, transcendentals=0),
    )(
        flat(expert_ids), flat(slot_ids), flat(combine_weights),
        sub_inputs, out_grads, expert_input_weight, expert_output_weight, expert_outputs,
    )
    d_inputs, dw_in, dw_out, gate_dots = pl.pallas_call(
        put_out,
        out_shape=tuple(jax.ShapeDtypeStruct(shape, kind) for shape, kind in shapes),
        in_specs=[vmem] * len(shapes),
        out_specs=(any_spec,) * len(shapes),
        scratch_shapes=[dma((len(shapes),))],
        compiler_params=pltpu.CompilerParams(vmem_limit_bytes=1024 * 1024),
    )(*results)
    d_gates = gate_dots.reshape(top, heads, tokens).transpose(2, 1, 0)
    return (d_inputs, d_gates, dw_in, dw_out)


def on_device(*args):
    tokens, heads, top = args[4].shape
    _, sub, ff = args[6].shape
    groups = lax.axis_size("expert")
    replicas = lax.axis_size("dp")
    cap = top * heads * tokens // groups
    half = groups // 2
    fits = half >= 4 and half & (half - 1) == 0 and replicas % 2 == 0 and cap % 128 == 0 and tokens % 128 == 0
    tokens_cross = half * replicas * cap * 3 * sub
    weights_cross = 4 * sub * ff
    if fits and weights_cross < tokens_cross:
        return paired_call(*args)
    return plain_call(*args)


def solution(mesh):
    rows = P(("expert", "dp"), None)
    table = P(("expert", "dp"), None, None)
    return jax.shard_map(
        on_device,
        mesh=mesh,
        in_specs=(
            rows,
            rows,
            P(("expert", "dp"), None, None, None),
            table,
            table,
            table,
            P("expert", None, None),
            P("expert", None, None),
        ),
        out_specs=(rows, table, P("expert", "dp", None), P("expert", "dp", None)),
        check_vma=False,
    )
```

```python
import functools

import jax
import jax.numpy as jnp
from jax import lax
from jax.experimental import pallas as pl
from jax.experimental.pallas import tpu as pltpu
from jax.sharding import PartitionSpec as P

MESH = pl.DeviceIdType.MESH
F32 = jnp.float32
BF16 = jnp.bfloat16
ROOT = 0.7978845608028654
CUBE = 0.044715


def partner(me, step, count):
    if count & (count - 1):
        return lax.rem(step - me + count, count)
    out, bit = 0, 1
    while bit < count:
        out = out + ((me // bit + step // bit) % 2) * bit
        bit *= 2
    return out


def spread(i, count):
    return lax.rem(i + 1, count)


def dot(a, b, ca, cb):
    return lax.dot_general(a, b, (((ca,), (cb,)), ((), ())), preferred_element_type=F32)


def kernel(
    dims,
    tgt, cw, x_hbm, g_hbm, win_hbm, wout_hbm, eo_hbm,
    dx, dwi, dwo, dg,
    xs, gs, win, wout, sx, sg, rx, rg, rs, rr, hb, fb, acc, po, pi, tpo, tpi, so, si, rpo, rpi,
    ev, load_sem, xg_send, xg_recv, r_send, r_recv, t_send, t_recv, w_send, w_recv,
):
    groups, replicas, cap, heads, tokens, sub, ff = dims
    chunk = max(cap, 128)
    per = chunk // cap
    chunks = groups * cap // chunk
    tile = 256
    me = lax.axis_index("expert")
    mine = lax.axis_index("dp")
    my_chunk = me // per
    halves = replicas // 2
    row, side = mine // 2, mine % 2
    twin = row * 2 + (1 - side)

    loads = []
    for h in range(heads):
        for s, (src, dst) in enumerate(((x_hbm, xs), (g_hbm, gs))):
            loads.append(
                pltpu.make_async_copy(
                    src.at[:, pl.ds(h * sub, sub)], dst.at[pl.ds(h * tokens, tokens)], load_sem.at[2 * h + s]
                )
            )
    wloads = [
        pltpu.make_async_copy(win_hbm.at[0], win, load_sem.at[2 * heads]),
        pltpu.make_async_copy(wout_hbm.at[0], wout, load_sem.at[2 * heads + 1]),
        pltpu.make_async_copy(eo_hbm, ev, load_sem.at[2 * heads + 2]),
    ]
    for c in loads + wloads:
        c.start()

    barrier = pltpu.get_barrier_semaphore()

    @pl.loop(1, groups)
    def _(i):
        pl.semaphore_signal(barrier, inc=1, device_id={"expert": lax.rem(me + i, groups)}, device_id_type=MESH)

    @pl.loop(1, replicas)
    def _(i):
        pl.semaphore_signal(barrier, inc=1, device_id={"dp": lax.rem(mine + i, replicas)}, device_id_type=MESH)

    pl.semaphore_wait(barrier, groups + replicas - 2)
    for c in loads:
        c.wait()

    def rows_of(index, size):
        return pl.ds(pl.multiple_of(index * size, size), size)

    def hot(j):
        slots = lax.broadcasted_iota(jnp.int32, (chunk, tgt.shape[1]), 0) + j * chunk
        return tgt[0:1, :] == slots, tgt[1:2, :] == slots

    def xg_copy(s, peer):
        src, dst = ((sx, rx), (sg, rg))[s]
        return pltpu.make_async_remote_copy(
            src_ref=src.at[rows_of(peer, cap)], dst_ref=dst.at[rows_of(me, cap)],
            send_sem=xg_send.at[s, peer], recv_sem=xg_recv.at[s, me],
            device_id={"expert": peer}, device_id_type=MESH,
        )

    def xg_local(s, src_dev):
        src, dst = ((sx, rx), (sg, rg))[s]
        return pltpu.make_async_copy(
            src.at[rows_of(src_dev, cap)], dst.at[rows_of(src_dev, cap)], xg_recv.at[s, src_dev]
        )

    def r_copy(peer):
        return pltpu.make_async_remote_copy(
            src_ref=rs.at[rows_of(peer, cap)], dst_ref=rr.at[rows_of(me, cap)],
            send_sem=r_send.at[peer], recv_sem=r_recv.at[me],
            device_id={"expert": peer}, device_id_type=MESH,
        )

    def r_local(src_dev):
        return pltpu.make_async_copy(
            rs.at[rows_of(src_dev, cap)], rr.at[rows_of(src_dev, cap)], r_recv.at[src_dev]
        )

    def twin_copy(s, q, t):
        src, dst = ((po, tpo), (pi, tpi))[s]
        return pltpu.make_async_remote_copy(
            src_ref=src.at[q], dst_ref=dst.at[t],
            send_sem=t_send.at[s, t], recv_sem=t_recv.at[s, t],
            device_id={"dp": twin}, device_id_type=MESH,
        )

    def row_copy(s, t):
        src, dst = ((so, rpo), (si, rpi))[s]
        return pltpu.make_async_remote_copy(
            src_ref=src.at[t], dst_ref=dst.at[row],
            send_sem=w_send.at[s, t], recv_sem=w_recv.at[s, row],
            device_id={"dp": 2 * t + side}, device_id_type=MESH,
        )

    def row_got(s, t):
        dst = (rpo, rpi)[s]
        return pltpu.make_async_copy(dst.at[t], dst.at[t], w_recv.at[s, t])

    @pl.loop(0, chunks)
    def _(i):
        j = partner(my_chunk, spread(i, chunks), chunks)
        h0, h1 = hot(j)
        one = (h0 | h1).astype(F32).astype(BF16)
        w = jnp.sum(jnp.where(h0, cw[0:1, :], 0.0) + jnp.where(h1, cw[1:2, :], 0.0), axis=1, keepdims=True)
        sx[rows_of(j, chunk), :] = dot(one, xs[...], 1, 0).astype(BF16)
        sg[rows_of(j, chunk), :] = (dot(one, gs[...], 1, 0) * w).astype(BF16)
        for p in range(per):
            peer = j * per + p

            @pl.when(peer != me)
            def _():
                xg_copy(0, peer).start()
                xg_copy(1, peer).start()

            @pl.when(peer == me)
            def _():
                xg_local(0, me).start()
                xg_local(1, me).start()

    for c in wloads:
        c.wait()

    span = 16
    for h in range(heads):

        @pl.loop(0, tokens // span)
        def _(b):
            grads = gs[rows_of(h * (tokens // span) + b, span), :].astype(F32)
            terms = ev[rows_of(b, span), h].astype(F32) * grads[:, None, :]
            dg[h, rows_of(b, span), :] = jnp.sum(terms, axis=-1)

    @pl.loop(0, chunks)
    def _(i):
        j = partner(my_chunk, spread(lax.rem(i + chunks - 1, chunks), chunks), chunks)
        for p in range(per):
            xg_local(0, j * per + p).wait()
            xg_local(1, j * per + p).wait()
        rows = rows_of(j, chunk)
        for n in range(ff // tile):
            cols = pl.ds(n * tile, tile)
            z = dot(rx[rows, :], win[:, cols], 1, 0)
            e = dot(rg[rows, :], wout[cols, :], 1, 1)
            zz = z * z
            t = jnp.tanh(ROOT * (z + CUBE * (zz * z)))
            half = 0.5 * (1.0 + t)
            hb[rows, cols] = (z * half).astype(BF16)
            slope = half + 0.5 * z * (1.0 - t * t) * (ROOT * (1.0 + 3.0 * CUBE * zz))
            fb[rows, cols] = (e * slope).astype(BF16)
        for n in range(sub // tile):
            cols = pl.ds(n * tile, tile)
            rs[rows, cols] = dot(fb[rows, :], win[cols, :], 1, 1).astype(BF16)
        for p in range(per):
            peer = j * per + p

            @pl.when(peer != me)
            def _():
                r_copy(peer).start()

            @pl.when(peer == me)
            def _():
                r_local(me).start()

    block = dwo.shape[1]
    def product(q):
        cols = rows_of(q, block)
        po[q] = dot(hb[:, cols], rg[...], 0, 0).astype(BF16)
        pi[q] = dot(rx[:, cols], fb[...], 0, 0).astype(BF16)

    @pl.loop(0, halves)
    def _(i):
        t = lax.rem(row + 1 + i, halves)
        product(2 * t + (1 - side))
        twin_copy(0, 2 * t + (1 - side), t).start()
        twin_copy(1, 2 * t + (1 - side), t).start()
        product(2 * t + side)

        @pl.when(t != row)
        def _():
            for s, (own, got, out) in enumerate(((po, tpo, so), (pi, tpi, si))):
                twin_copy(s, 2 * t + side, t).wait_recv()
                out[t] = (own[2 * t + side].astype(F32) + got[t].astype(F32)).astype(BF16)
                row_copy(s, t).start()

    acc[...] = jnp.zeros_like(acc)

    @pl.loop(0, chunks)
    def _(i):
        j = partner(my_chunk, spread(lax.rem(i + chunks - 1, chunks), chunks), chunks)
        for p in range(per):
            r_local(j * per + p).wait()
        h0, h1 = hot(j)
        one = (h0 | h1).astype(F32).astype(BF16)
        acc[...] += dot(one, rr[rows_of(j, chunk), :], 0, 0)

    for h in range(heads):
        dx[:, pl.ds(h * sub, sub)] = acc[pl.ds(h * tokens, tokens), :].astype(BF16)

    for s, (out, own, got, sums) in enumerate(((dwo, po, tpo, rpo), (dwi, pi, tpi, rpi))):
        twin_copy(s, mine, row).wait_recv()
        out[0] = own[mine].astype(F32) + got[row].astype(F32)

        @pl.loop(1, halves)
        def _(i):
            t = lax.rem(row + i, halves)
            row_got(s, t).wait()
            out[0] = out[0] + sums[t].astype(F32)

    @pl.loop(1, groups)
    def _(i):
        peer = lax.rem(me + i, groups)
        xg_copy(0, peer).wait_send()
        xg_copy(1, peer).wait_send()
        r_copy(peer).wait_send()

    for s in range(2):

        @pl.loop(0, halves)
        def _(i):
            twin_copy(s, 2 * i + (1 - side), i).wait_send()

        @pl.loop(1, halves)
        def _(i):
            row_copy(s, lax.rem(row + i, halves)).wait_send()


def plain_call(
    sub_inputs,
    out_grads,
    expert_outputs,
    combine_weights,
    expert_ids,
    slot_ids,
    expert_input_weight,
    expert_output_weight,
):
    tokens, heads, top = expert_ids.shape
    _, sub, ff = expert_input_weight.shape
    groups = lax.axis_size("expert")
    replicas = lax.axis_size("dp")
    cap = top * heads * tokens // groups
    kept = slot_ids >= 0
    target = jnp.where(kept, expert_ids * cap + slot_ids, -1)
    target = target.transpose(2, 1, 0).reshape(top, heads * tokens)
    weight = combine_weights.transpose(2, 1, 0).reshape(top, heads * tokens)
    slots = groups * cap
    part = sub // replicas
    part_out = ff // replicas
    dims = (groups, replicas, cap, heads, tokens, sub, ff)
    any_spec = pl.BlockSpec(memory_space=pltpu.HBM)
    vmem = pl.BlockSpec(memory_space=pltpu.VMEM)
    dma = pltpu.SemaphoreType.DMA
    d_inputs, dw_in, dw_out, gate_dots = pl.pallas_call(
        functools.partial(kernel, dims),
        out_shape=(
            jax.ShapeDtypeStruct((tokens, heads * sub), BF16),
            jax.ShapeDtypeStruct((1, part, ff), F32),
            jax.ShapeDtypeStruct((1, part_out, sub), F32),
            jax.ShapeDtypeStruct((heads, tokens, top), F32),
        ),
        in_specs=[vmem, vmem, any_spec, any_spec, any_spec, any_spec, any_spec],
        out_specs=(vmem, vmem, vmem, vmem),
        scratch_shapes=[
            pltpu.VMEM((heads * tokens, sub), BF16),
            pltpu.VMEM((heads * tokens, sub), BF16),
            pltpu.VMEM((sub, ff), BF16),
            pltpu.VMEM((ff, sub), BF16),
            pltpu.VMEM((slots, sub), BF16),
            pltpu.VMEM((slots, sub), BF16),
            pltpu.VMEM((slots, sub), BF16),
            pltpu.VMEM((slots, sub), BF16),
            pltpu.VMEM((slots, sub), BF16),
            pltpu.VMEM((slots, sub), BF16),
            pltpu.VMEM((slots, ff), BF16),
            pltpu.VMEM((slots, ff), BF16),
            pltpu.VMEM((heads * tokens, sub), F32),
            pltpu.VMEM((replicas, part_out, sub), BF16),
            pltpu.VMEM((replicas, part, ff), BF16),
            *[pltpu.VMEM((replicas // 2, part_out, sub), BF16), pltpu.VMEM((replicas // 2, part, ff), BF16)] * 3,
            pltpu.VMEM((tokens, heads, top, sub), BF16),
            dma((2 * heads + 3,)),
            dma((2, groups)),
            dma((2, groups)),
            dma((groups,)),
            dma((groups,)),
            *[dma((2, replicas // 2))] * 4,
        ],
        compiler_params=pltpu.CompilerParams(
            collective_id=0, has_side_effects=True, vmem_limit_bytes=60 * 1024 * 1024
        ),
        cost_estimate=pl.CostEstimate(flops=20 * 10**9, bytes_accessed=2**24, transcendentals=0),
    )(target, weight, sub_inputs, out_grads, expert_input_weight, expert_output_weight, expert_outputs)
    d_gates = jnp.where(kept, gate_dots.transpose(1, 0, 2), jnp.float32(0.0))
    return (d_inputs, d_gates, dw_in, dw_out)


PIECES = 2


def paired(
    dims,
    ids_hbm, slot_hbm, cw_hbm, x_hbm, g_hbm, win_hbm, wout_hbm, eo_hbm,
    dx, dwi, dwo, dg,
    ids, slot, cw, tgt, xs, gs, win, wout, sx, sg, rx, rg, rs, rr, hb, fb, acc, po, pi, tpo, tpi, so, si, rpo, rpi,
    cpo, cpi, gpo, gpi, ev, gates,
    load_sem, xg_send, xg_recv, r_send, r_recv, wz_send, wz_recv, wt_send, wt_recv, wy_send, wy_recv,
    t_send, t_recv, y_send, y_recv, c_send, c_recv, a_send, a_recv,
):
    groups, replicas, cap, heads, tokens, sub, ff = dims
    tile = 256
    me = lax.axis_index("expert")
    mine = lax.axis_index("dp")
    half = groups // 2
    halves = replicas // 2
    low = lax.rem(me, half)
    base = me - low
    opposite = lax.rem(me + half, groups)
    inner = lax.rem(me // half + low // (half // 2), 2)
    outer = inner == 0
    first, second = inner, 1 - inner
    row, side = mine // 2, mine % 2
    twin = row * 2 + (1 - side)
    near = range(1, half)

    def rows_of(index, size):
        return pl.ds(pl.multiple_of(index * size, size), size)

    def fixed(f, s, n=1):
        return pl.ds(pl.multiple_of((f * (half + 1) + s) * cap, cap), n * cap)

    def landed(ref, sem):
        return pltpu.make_async_copy(ref, ref, sem)

    def remote(src, dst, send, recv, where):
        return pltpu.make_async_remote_copy(
            src_ref=src, dst_ref=dst, send_sem=send, recv_sem=recv, device_id=where, device_id_type=MESH
        )

    loads = []
    for h in range(heads):
        for s, (src, dst) in enumerate(((x_hbm, xs), (g_hbm, gs))):
            loads.append(
                pltpu.make_async_copy(
                    src.at[:, pl.ds(h * sub, sub)], dst.at[pl.ds(h * tokens, tokens)], load_sem.at[2 * h + s]
                )
            )
    wloads = [
        pltpu.make_async_copy(win_hbm.at[0], win.at[0], load_sem.at[2 * heads]),
        pltpu.make_async_copy(wout_hbm.at[0], wout.at[0], load_sem.at[2 * heads + 1]),
    ]
    eload = pltpu.make_async_copy(eo_hbm, ev, load_sem.at[2 * heads + 2])
    tables = [
        pltpu.make_async_copy(src, dst, load_sem.at[2 * heads + 3 + i])
        for i, (src, dst) in enumerate(((ids_hbm, ids), (slot_hbm, slot), (cw_hbm, cw)))
    ]
    barrier = pltpu.get_barrier_semaphore()
    for s in near:
        pl.semaphore_signal(
            barrier, inc=1, device_id={"expert": base + partner(low, s, half)}, device_id_type=MESH
        )
    pl.semaphore_signal(barrier, inc=1, device_id={"expert": opposite}, device_id_type=MESH)
    for i in range(1, replicas):
        pl.semaphore_signal(barrier, inc=1, device_id={"dp": lax.rem(mine + i, replicas)}, device_id_type=MESH)
    turn = half // 2
    across = lax.rem(base + partner(low, turn, half) + half, groups)

    @pl.when(inner == 1)
    def _():
        pl.semaphore_signal(barrier, inc=1, device_id={"expert": across}, device_id_type=MESH)
    for c in tables + loads + wloads + [eload]:
        c.start()

    def owner(s):
        return base + partner(low, s, half)

    def part_of(m, quarter, n):
        size = (sub, ff)[m] // replicas // PIECES
        return rows_of(quarter * PIECES + n, size)

    def held(m, quarter, n):
        return (win, wout)[m].at[1, part_of(m, quarter, n)]

    def w_cross(m, n):
        return remote(
            (win_hbm, wout_hbm)[m].at[0, part_of(m, mine, n)], held(m, mine, n),
            wz_send.at[m, n], wz_recv.at[m, n], {"expert": opposite},
        )

    def w_twin(m, n, t):
        ref = held(m, 2 * t + side, n)
        return remote(ref, ref, wt_send.at[m, n, t], wt_recv.at[m, n, t], {"dp": twin})

    def w_row(m, n, t):
        ref = held(m, mine, n)
        return remote(ref, ref, wy_send.at[m, n, t], wy_recv.at[m, n, row], {"dp": 2 * t + side})

    def xg_copy(s, f, step):
        src, dst = ((sx, rx), (sg, rg))[s]
        return remote(
            src.at[fixed(f, step)], dst.at[fixed(f, step)],
            xg_send.at[s, f, step], xg_recv.at[s, f, step], {"expert": owner(step)},
        )

    def across_copy(s):
        src, dst = ((sx, rx), (sg, rg))[s]
        return remote(
            src.at[fixed(1, turn)], dst.at[fixed(0, half)], a_send.at[s], a_recv.at[s], {"expert": across}
        )

    def across_reply():
        return remote(
            rs.at[fixed(0, half)], rr.at[fixed(1, turn)], a_send.at[2], r_recv.at[1, turn], {"expert": across}
        )

    def r_copy(f, step):
        return remote(
            rs.at[fixed(f, step)], rr.at[fixed(f, step)],
            r_send.at[f, step], r_recv.at[f, step], {"expert": owner(step)},
        )

    def twin_copy(f, s, q, t):
        src, dst = ((po, tpo), (pi, tpi))[s]
        return remote(src.at[f, q], dst.at[f, t], t_send.at[f, s, t], t_recv.at[f, s, t], {"dp": twin})

    def cut(s, n):
        size = (dwo, dwi)[s].shape[1] // PIECES
        return pl.ds(n * size, size)

    def row_copy(f, s, t, n):
        src, dst = ((so, rpo), (si, rpi))[s]
        return remote(
            src.at[f, t, cut(s, n)], dst.at[f, row, cut(s, n)],
            y_send.at[f, s, n, t], y_recv.at[f, s, n, row], {"dp": 2 * t + side},
        )

    def cross_copy(s, n):
        src, dst = ((cpo, gpo), (cpi, gpi))[s]
        return remote(
            src.at[cut(s, n)], dst.at[cut(s, n)], c_send.at[s, n], c_recv.at[s, n], {"expert": opposite}
        )

    pieces = [(m, n) for m in range(2) for n in range(PIECES)]

    @pl.when(outer)
    def _():
        pl.semaphore_wait(barrier, half + replicas - 1)
        for m, n in pieces:
            w_cross(m, n).start()

    for c in tables:
        c.wait()
    tgt[...] = jnp.where(slot[...] >= 0, ids[...] * cap + slot[...], -1)

    def hot(f, step):
        first = lax.rem(owner(step) + f * half, groups) * cap
        slots = lax.broadcasted_iota(jnp.int32, (cap, tgt.shape[1]), 0) + first
        return tgt[0:1, :] == slots, tgt[1:2, :] == slots

    def gather(f, step, out_x, out_g):
        h0, h1 = hot(f, step)
        one = (h0 | h1).astype(F32).astype(BF16)
        w = jnp.sum(jnp.where(h0, cw[0:1, :], 0.0) + jnp.where(h1, cw[1:2, :], 0.0), axis=1, keepdims=True)
        rows = fixed(f, step)
        out_x[rows, :] = dot(one, xs[...], 1, 0).astype(BF16)
        out_g[rows, :] = (dot(one, gs[...], 1, 0) * w).astype(BF16)

    for c in loads:
        c.wait()
    far_steps = range(half // 2, half)

    def send(f, step):
        xg_copy(0, f, step).start()
        xg_copy(1, f, step).start()

    @pl.loop(half // 2, half)
    def _(step):
        gather(second, step, sx, sg)

    @pl.when(inner == 1)
    def _():
        pl.semaphore_wait(barrier, half + replicas)

    for step in far_steps:
        send(second, step)

    @pl.loop(0, 2)
    def _(i):
        f = first + i * (second - first)

        @pl.loop(1, half // 2)
        def _(step):
            gather(f, step, sx, sg)
            send(f, step)

        gather(f, 0, rx, rg)

    @pl.loop(half // 2, half)
    def _(step):
        gather(first, step, sx, sg)
        pl.when(outer)(lambda: send(first, step))

    eload.wait()
    span = 16
    lane = lax.broadcasted_iota(jnp.int32, (span, gates.shape[1]), 1)

    @pl.loop(0, tokens // span)
    def _(b):
        found = jnp.zeros((span, gates.shape[1]), F32)
        for h in range(heads):
            grads = gs[rows_of(h * (tokens // span) + b, span), :].astype(F32)
            terms = ev[rows_of(b, span), h].astype(F32) * grads[:, None, :]
            sums = jnp.sum(terms, axis=-1)
            for k in range(2):
                found = jnp.where(lane == 2 * h + k, sums[:, k : k + 1], found)
        gates[rows_of(b, span), :] = found

    turned = gates[...].T
    for h in range(heads):
        cols = pl.ds(h * tokens, tokens)
        dg[:, cols] = jnp.where(slot[:, cols] >= 0, turned[2 * h : 2 * h + 2, :], 0.0)

    for c in wloads:
        c.wait()

    others = [lax.rem(row + i, halves) for i in range(1, halves)]

    def from_rows(m, n):
        for t in others:
            landed(held(m, 2 * t + side, n), wy_recv.at[m, n, t]).wait()
            w_twin(m, n, t).start()

    def rows_out(f, s, t, parts=range(PIECES)):
        for n in parts:
            row_copy(f, s, t, n).start()

    def weights():
        before = None
        for m, n in pieces:
            landed(held(m, mine, n), wz_recv.at[m, n]).wait()
            w_twin(m, n, row).start()
            for t in others:
                w_row(m, n, t).start()
            if before is not None:
                from_rows(*before)
            before = (m, n)
            if before == pieces[-1]:

                @pl.when(outer)
                def _():
                    for t in others:
                        rows_out(first, 0, t)

                @pl.when(inner == 1)
                def _():
                    for piece in pieces:
                        w_cross(*piece).start()

        from_rows(*before)
        for m, n in pieces:
            for t in range(halves):
                landed(held(m, 2 * t + (1 - side), n), wt_recv.at[m, n, t]).wait()

    def arrive(f, s, n):
        for step in range(s, s + n):
            if step > 0:
                for v, dst in enumerate((rx, rg)):
                    landed(dst.at[fixed(f, step)], xg_recv.at[v, f, step]).wait()

    def arrive_across():
        for v, dst in enumerate((rx, rg)):
            landed(dst.at[fixed(0, half)], a_recv.at[v]).wait()

    def process(f, s, n):
        rows = fixed(f, s, n)
        for c in range(ff // tile):
            cols = pl.ds(c * tile, tile)
            z = dot(rx[rows, :], win[f, :, cols], 1, 0)
            e = dot(rg[rows, :], wout[f, cols, :], 1, 1)
            zz = z * z
            t = jnp.tanh(ROOT * (z + CUBE * (zz * z)))
            part = 0.5 * (1.0 + t)
            hb[rows, cols] = (z * part).astype(BF16)
            slope = part + 0.5 * z * (1.0 - t * t) * (ROOT * (1.0 + 3.0 * CUBE * zz))
            fb[rows, cols] = (e * slope).astype(BF16)
        for c in range(sub // tile):
            cols = pl.ds(c * tile, tile)
            back = dot(fb[rows, :], win[f, cols, :], 1, 1).astype(BF16)
            for step in range(s, s + n):
                piece = back[(step - s) * cap : (step - s + 1) * cap]
                if step == 0:
                    rr[fixed(f, step), cols] = piece
                else:
                    rs[fixed(f, step), cols] = piece

    def reply(f, s, n):
        for step in range(s, s + n):
            if step > 0:
                r_copy(f, step).start()

    block = dwo.shape[1]

    def product(f, q, n):
        cols = rows_of(q, block)
        rows = fixed(f, 0, n)
        po[f, q] = dot(hb[rows, cols], rg[rows, :], 0, 0).astype(BF16)
        pi[f, q] = dot(rx[rows, cols], fb[rows, :], 0, 0).astype(BF16)

    def exchange(f, early, n):
        @pl.loop(0, halves)
        def _(i):
            t = lax.rem(row + 1 + i, halves)
            product(f, 2 * t + (1 - side), n)
            twin_copy(f, 0, 2 * t + (1 - side), t).start()
            twin_copy(f, 1, 2 * t + (1 - side), t).start()
            product(f, 2 * t + side, n)

            @pl.when(t != row)
            def _():
                for s, (own, got, out) in enumerate(((po, tpo, so), (pi, tpi, si))):
                    landed(got.at[f, t], t_recv.at[f, s, t]).wait()
                    out[f, t] = (own[f, 2 * t + side].astype(F32) + got[f, t].astype(F32)).astype(BF16)
                    if early:
                        pl.when(inner == 1)(lambda s=s: rows_out(f, s, t))
                    else:
                        rows_out(f, s, t)

    def total(f, s, n):
        own, got, sums = ((po, tpo, rpo), (pi, tpi, rpi))[s]
        if n == 0:
            landed(got.at[f, row], t_recv.at[f, s, row]).wait()
        out = own[f, mine, cut(s, n)].astype(F32) + got[f, row, cut(s, n)].astype(F32)
        for t in others:
            landed(sums.at[f, t, cut(s, n)], y_recv.at[f, s, n, t]).wait()
            out = out + sums[f, t, cut(s, n)].astype(F32)
        return out

    def scatter(f, s, n, start=False):
        ones = []
        for step in range(s, s + n):
            if step > 0:
                landed(rr.at[fixed(f, step)], r_recv.at[f, step]).wait()
            h0, h1 = hot(f, step)
            ones.append((h0 | h1).astype(F32).astype(BF16))
        more = dot(jnp.concatenate(ones, axis=0), rr[fixed(f, s, n), :], 0, 0)
        acc[...] = more if start else acc[...] + more

    def pass_on(s, parts):
        out = (cpo, cpi)[s]
        for n in parts:
            out[cut(s, n)] = total(1, s, n).astype(BF16)
            cross_copy(s, n).start()

    near_part, far_part = (0, turn), (turn, turn)
    last_part = (turn + 1, turn - 1)

    @pl.when(outer)
    def _():
        rx[fixed(1, turn), :] = jnp.zeros((cap, sub), BF16)
        rg[fixed(1, turn), :] = jnp.zeros((cap, sub), BF16)

    pl.when(inner == 1)(weights)
    arrive(first, *near_part)
    process(first, *near_part)
    reply(first, *near_part)
    arrive(first, *far_part)

    @pl.when(inner == 1)
    def _():
        for step in far_steps[1:]:
            send(first, step)
        across_copy(0).start()
        across_copy(1).start()

    process(first, *far_part)
    pl.when(outer)(lambda: reply(first, *far_part))
    exchange(first, True, half)
    pl.when(outer)(weights)
    arrive(second, *near_part)
    process(second, *near_part)
    reply(second, *near_part)

    @pl.when(inner == 1)
    def _():
        pass_on(0, (0,))
        for step in far_steps[1:]:
            xg_copy(0, first, step).wait_send()
            xg_copy(1, first, step).wait_send()
        arrive_across()
        process(0, half, 1)
        across_reply().start()
        pass_on(0, range(1, PIECES))
        reply(first, *far_part)
        arrive(second, turn, 1)

    arrive(second, *last_part)
    process(second, *far_part)

    @pl.when(inner == 1)
    def _():
        pass_on(1, range(PIECES))
        reply(second, turn, 1)

    reply(second, *last_part)
    pl.when(inner == 1)(lambda: exchange(0, False, half + 1))

    @pl.when(outer)
    def _():
        exchange(1, False, half)
        for t in others:
            rows_out(first, 1, t)
        pass_on(0, range(PIECES))
        pass_on(1, range(PIECES))

    scatter(first, 0, half // 2, True)
    scatter(second, 0, half // 2)

    for step in far_steps:
        xg_copy(0, second, step).wait_send()
        xg_copy(1, second, step).wait_send()

    @pl.when(outer)
    def _():
        for step in far_steps:
            xg_copy(0, first, step).wait_send()
            xg_copy(1, first, step).wait_send()

    @pl.when(inner == 1)
    def _():
        across_copy(0).wait_send()
        across_copy(1).wait_send()

    for f in range(2):
        for step in near:
            if step < turn:
                xg_copy(0, f, step).wait_send()
                xg_copy(1, f, step).wait_send()
        for s in range(2):
            for t in range(halves):
                twin_copy(f, s, 2 * t + (1 - side), t).wait_send()
    for m, n in pieces:
        w_cross(m, n).wait_send()
        for t in range(halves):
            w_twin(m, n, t).wait_send()
        for t in others:
            w_row(m, n, t).wait_send()

    scatter(second, half // 2, half // 2)
    for s, out in enumerate((dwo, dwi)):
        for n in range(PIECES):
            out[0, cut(s, n)] = total(0, s, n)
    scatter(first, half // 2, half // 2)
    for h in range(heads):
        dx[:, pl.ds(h * sub, sub)] = acc[pl.ds(h * tokens, tokens), :].astype(BF16)

    @pl.when(inner == 1)
    def _():
        across_reply().wait_send()
        r_copy(second, turn).wait_send()

    r_copy(first, turn).wait_send()
    for f in range(2):
        for step in near:
            if step != turn:
                r_copy(f, step).wait_send()
        for s in range(2):
            for t in others:
                for n in range(PIECES):
                    row_copy(f, s, t, n).wait_send()
    for s, (out, got) in enumerate(((dwo, gpo), (dwi, gpi))):
        for n in range(PIECES):
            landed(got.at[cut(s, n)], c_recv.at[s, n]).wait()
            out[0, cut(s, n)] = out[0, cut(s, n)] + got[cut(s, n)].astype(F32)

    for s in range(2):
        for n in range(PIECES):
            cross_copy(s, n).wait_send()


def put_out(*refs):
    count = len(refs) // 2
    sems = refs[-1]
    copies = [pltpu.make_async_copy(refs[i], refs[count + i], sems.at[i]) for i in range(count)]
    for c in copies:
        c.start()
    for c in copies:
        c.wait()


def paired_call(
    sub_inputs,
    out_grads,
    expert_outputs,
    combine_weights,
    expert_ids,
    slot_ids,
    expert_input_weight,
    expert_output_weight,
):
    tokens, heads, top = expert_ids.shape
    _, sub, ff = expert_input_weight.shape
    groups = lax.axis_size("expert")
    replicas = lax.axis_size("dp")
    cap = top * heads * tokens // groups

    def flat(a):
        return a.transpose(2, 1, 0).reshape(top, heads * tokens)

    slots = (groups + 1) * cap
    half = groups // 2
    halves = replicas // 2
    part = sub // replicas
    part_out = ff // replicas
    dims = (groups, replicas, cap, heads, tokens, sub, ff)
    any_spec = pl.BlockSpec(memory_space=pltpu.HBM)
    vmem = pl.BlockSpec(memory_space=pltpu.VMEM)
    dma = pltpu.SemaphoreType.DMA
    rows = heads * tokens
    shapes = (
        ((tokens, heads * sub), BF16),
        ((1, part, ff), F32),
        ((1, part_out, sub), F32),
        ((top, heads * tokens), F32),
    )
    results = pl.pallas_call(
        functools.partial(paired, dims),
        out_shape=tuple(pltpu.VMEM(shape, kind) for shape, kind in shapes),
        in_specs=[any_spec] * 8,
        out_specs=(vmem, vmem, vmem, vmem),
        scratch_shapes=[
            pltpu.VMEM((top, rows), jnp.int32),
            pltpu.VMEM((top, rows), jnp.int32),
            pltpu.VMEM((top, rows), F32),
            pltpu.VMEM((top, rows), jnp.int32),
            pltpu.VMEM((rows, sub), BF16),
            pltpu.VMEM((rows, sub), BF16),
            pltpu.VMEM((2, sub, ff), BF16),
            pltpu.VMEM((2, ff, sub), BF16),
            *[pltpu.VMEM((slots, sub), BF16)] * 6,
            pltpu.VMEM((slots, ff), BF16),
            pltpu.VMEM((slots, ff), BF16),
            pltpu.VMEM((rows, sub), F32),
            pltpu.VMEM((2, replicas, part_out, sub), BF16),
            pltpu.VMEM((2, replicas, part, ff), BF16),
            *[pltpu.VMEM((2, halves, part_out, sub), BF16), pltpu.VMEM((2, halves, part, ff), BF16)] * 3,
            *[pltpu.VMEM((part_out, sub), BF16), pltpu.VMEM((part, ff), BF16)] * 2,
            pltpu.VMEM((tokens, heads, top, sub), BF16),
            pltpu.VMEM((tokens, 128), F32),
            dma((2 * heads + 6,)),
            *[dma((2, 2, half))] * 2,
            *[dma((2, half))] * 2,
            *[dma((2, PIECES))] * 2,
            *[dma((2, PIECES, halves))] * 4,
            *[dma((2, 2, halves))] * 2,
            *[dma((2, 2, PIECES, halves))] * 2,
            *[dma((2, PIECES))] * 2,
            dma((3,)),
            dma((2,)),
        ],
        compiler_params=pltpu.CompilerParams(
            collective_id=0, has_side_effects=True, vmem_limit_bytes=59 * 1024 * 1024
        ),
        cost_estimate=pl.CostEstimate(flops=20 * 10**9, bytes_accessed=2**24, transcendentals=0),
    )(
        flat(expert_ids), flat(slot_ids), flat(combine_weights),
        sub_inputs, out_grads, expert_input_weight, expert_output_weight, expert_outputs,
    )
    d_inputs, dw_in, dw_out, gate_dots = pl.pallas_call(
        put_out,
        out_shape=tuple(jax.ShapeDtypeStruct(shape, kind) for shape, kind in shapes),
        in_specs=[vmem] * len(shapes),
        out_specs=(any_spec,) * len(shapes),
        scratch_shapes=[dma((len(shapes),))],
        compiler_params=pltpu.CompilerParams(vmem_limit_bytes=1024 * 1024),
    )(*results)
    d_gates = gate_dots.reshape(top, heads, tokens).transpose(2, 1, 0)
    return (d_inputs, d_gates, dw_in, dw_out)


def on_device(*args):
    tokens, heads, top = args[4].shape
    _, sub, ff = args[6].shape
    groups = lax.axis_size("expert")
    replicas = lax.axis_size("dp")
    cap = top * heads * tokens // groups
    half = groups // 2
    fits = half >= 4 and half & (half - 1) == 0 and replicas % 2 == 0 and cap % 128 == 0 and tokens % 128 == 0
    tokens_cross = half * replicas * cap * 3 * sub
    weights_cross = 4 * sub * ff
    if fits and weights_cross < tokens_cross:
        return paired_call(*args)
    return plain_call(*args)


def solution(mesh):
    rows = P(("expert", "dp"), None)
    table = P(("expert", "dp"), None, None)
    return jax.shard_map(
        on_device,
        mesh=mesh,
        in_specs=(
            rows,
            rows,
            P(("expert", "dp"), None, None, None),
            table,
            table,
            table,
            P("expert", None, None),
            P("expert", None, None),
        ),
        out_specs=(rows, table, P("expert", "dp", None), P("expert", "dp", None)),
        check_vma=False,
    )
```

```python
import functools

import jax
import jax.numpy as jnp
from jax import lax
from jax.experimental import pallas as pl
from jax.experimental.pallas import tpu as pltpu
from jax.sharding import PartitionSpec as P

MESH = pl.DeviceIdType.MESH
F32 = jnp.float32
BF16 = jnp.bfloat16
ROOT = 0.7978845608028654
CUBE = 0.044715


def partner(me, step, count):
    if count & (count - 1):
        return lax.rem(step - me + count, count)
    out, bit = 0, 1
    while bit < count:
        out = out + ((me // bit + step // bit) % 2) * bit
        bit *= 2
    return out


def spread(i, count):
    return lax.rem(i + 1, count)


def dot(a, b, ca, cb):
    return lax.dot_general(a, b, (((ca,), (cb,)), ((), ())), preferred_element_type=F32)


def kernel(
    dims,
    tgt, cw, x_hbm, g_hbm, win_hbm, wout_hbm, eo_hbm,
    dx, dwi, dwo, dg,
    xs, gs, win, wout, sx, sg, rx, rg, rs, rr, hb, fb, acc, po, pi, tpo, tpi, so, si, rpo, rpi,
    ev, load_sem, xg_send, xg_recv, r_send, r_recv, t_send, t_recv, w_send, w_recv,
):
    groups, replicas, cap, heads, tokens, sub, ff = dims
    chunk = max(cap, 128)
    per = chunk // cap
    chunks = groups * cap // chunk
    tile = 256
    me = lax.axis_index("expert")
    mine = lax.axis_index("dp")
    my_chunk = me // per
    halves = replicas // 2
    row, side = mine // 2, mine % 2
    twin = row * 2 + (1 - side)

    loads = []
    for h in range(heads):
        for s, (src, dst) in enumerate(((x_hbm, xs), (g_hbm, gs))):
            loads.append(
                pltpu.make_async_copy(
                    src.at[:, pl.ds(h * sub, sub)], dst.at[pl.ds(h * tokens, tokens)], load_sem.at[2 * h + s]
                )
            )
    wloads = [
        pltpu.make_async_copy(win_hbm.at[0], win, load_sem.at[2 * heads]),
        pltpu.make_async_copy(wout_hbm.at[0], wout, load_sem.at[2 * heads + 1]),
        pltpu.make_async_copy(eo_hbm, ev, load_sem.at[2 * heads + 2]),
    ]
    for c in loads + wloads:
        c.start()

    barrier = pltpu.get_barrier_semaphore()

    @pl.loop(1, groups)
    def _(i):
        pl.semaphore_signal(barrier, inc=1, device_id={"expert": lax.rem(me + i, groups)}, device_id_type=MESH)

    @pl.loop(1, replicas)
    def _(i):
        pl.semaphore_signal(barrier, inc=1, device_id={"dp": lax.rem(mine + i, replicas)}, device_id_type=MESH)

    pl.semaphore_wait(barrier, groups + replicas - 2)
    for c in loads:
        c.wait()

    def rows_of(index, size):
        return pl.ds(pl.multiple_of(index * size, size), size)

    def hot(j):
        slots = lax.broadcasted_iota(jnp.int32, (chunk, tgt.shape[1]), 0) + j * chunk
        return tgt[0:1, :] == slots, tgt[1:2, :] == slots

    def xg_copy(s, peer):
        src, dst = ((sx, rx), (sg, rg))[s]
        return pltpu.make_async_remote_copy(
            src_ref=src.at[rows_of(peer, cap)], dst_ref=dst.at[rows_of(me, cap)],
            send_sem=xg_send.at[s, peer], recv_sem=xg_recv.at[s, me],
            device_id={"expert": peer}, device_id_type=MESH,
        )

    def xg_local(s, src_dev):
        src, dst = ((sx, rx), (sg, rg))[s]
        return pltpu.make_async_copy(
            src.at[rows_of(src_dev, cap)], dst.at[rows_of(src_dev, cap)], xg_recv.at[s, src_dev]
        )

    def r_copy(peer):
        return pltpu.make_async_remote_copy(
            src_ref=rs.at[rows_of(peer, cap)], dst_ref=rr.at[rows_of(me, cap)],
            send_sem=r_send.at[peer], recv_sem=r_recv.at[me],
            device_id={"expert": peer}, device_id_type=MESH,
        )

    def r_local(src_dev):
        return pltpu.make_async_copy(
            rs.at[rows_of(src_dev, cap)], rr.at[rows_of(src_dev, cap)], r_recv.at[src_dev]
        )

    def twin_copy(s, q, t):
        src, dst = ((po, tpo), (pi, tpi))[s]
        return pltpu.make_async_remote_copy(
            src_ref=src.at[q], dst_ref=dst.at[t],
            send_sem=t_send.at[s, t], recv_sem=t_recv.at[s, t],
            device_id={"dp": twin}, device_id_type=MESH,
        )

    def row_copy(s, t):
        src, dst = ((so, rpo), (si, rpi))[s]
        return pltpu.make_async_remote_copy(
            src_ref=src.at[t], dst_ref=dst.at[row],
            send_sem=w_send.at[s, t], recv_sem=w_recv.at[s, row],
            device_id={"dp": 2 * t + side}, device_id_type=MESH,
        )

    def row_got(s, t):
        dst = (rpo, rpi)[s]
        return pltpu.make_async_copy(dst.at[t], dst.at[t], w_recv.at[s, t])

    @pl.loop(0, chunks)
    def _(i):
        j = partner(my_chunk, spread(i, chunks), chunks)
        h0, h1 = hot(j)
        one = (h0 | h1).astype(F32).astype(BF16)
        w = jnp.sum(jnp.where(h0, cw[0:1, :], 0.0) + jnp.where(h1, cw[1:2, :], 0.0), axis=1, keepdims=True)
        sx[rows_of(j, chunk), :] = dot(one, xs[...], 1, 0).astype(BF16)
        sg[rows_of(j, chunk), :] = (dot(one, gs[...], 1, 0) * w).astype(BF16)
        for p in range(per):
            peer = j * per + p

            @pl.when(peer != me)
            def _():
                xg_copy(0, peer).start()
                xg_copy(1, peer).start()

            @pl.when(peer == me)
            def _():
                xg_local(0, me).start()
                xg_local(1, me).start()

    for c in wloads:
        c.wait()

    span = 16
    for h in range(heads):

        @pl.loop(0, tokens // span)
        def _(b):
            grads = gs[rows_of(h * (tokens // span) + b, span), :].astype(F32)
            terms = ev[rows_of(b, span), h].astype(F32) * grads[:, None, :]
            dg[h, rows_of(b, span), :] = jnp.sum(terms, axis=-1)

    @pl.loop(0, chunks)
    def _(i):
        j = partner(my_chunk, spread(lax.rem(i + chunks - 1, chunks), chunks), chunks)
        for p in range(per):
            xg_local(0, j * per + p).wait()
            xg_local(1, j * per + p).wait()
        rows = rows_of(j, chunk)
        for n in range(ff // tile):
            cols = pl.ds(n * tile, tile)
            z = dot(rx[rows, :], win[:, cols], 1, 0)
            e = dot(rg[rows, :], wout[cols, :], 1, 1)
            zz = z * z
            t = jnp.tanh(ROOT * (z + CUBE * (zz * z)))
            half = 0.5 * (1.0 + t)
            hb[rows, cols] = (z * half).astype(BF16)
            slope = half + 0.5 * z * (1.0 - t * t) * (ROOT * (1.0 + 3.0 * CUBE * zz))
            fb[rows, cols] = (e * slope).astype(BF16)
        for n in range(sub // tile):
            cols = pl.ds(n * tile, tile)
            rs[rows, cols] = dot(fb[rows, :], win[cols, :], 1, 1).astype(BF16)
        for p in range(per):
            peer = j * per + p

            @pl.when(peer != me)
            def _():
                r_copy(peer).start()

            @pl.when(peer == me)
            def _():
                r_local(me).start()

    block = dwo.shape[1]
    def product(q):
        cols = rows_of(q, block)
        po[q] = dot(hb[:, cols], rg[...], 0, 0).astype(BF16)
        pi[q] = dot(rx[:, cols], fb[...], 0, 0).astype(BF16)

    @pl.loop(0, halves)
    def _(i):
        t = lax.rem(row + 1 + i, halves)
        product(2 * t + (1 - side))
        twin_copy(0, 2 * t + (1 - side), t).start()
        twin_copy(1, 2 * t + (1 - side), t).start()
        product(2 * t + side)

        @pl.when(t != row)
        def _():
            for s, (own, got, out) in enumerate(((po, tpo, so), (pi, tpi, si))):
                twin_copy(s, 2 * t + side, t).wait_recv()
                out[t] = (own[2 * t + side].astype(F32) + got[t].astype(F32)).astype(BF16)
                row_copy(s, t).start()

    acc[...] = jnp.zeros_like(acc)

    @pl.loop(0, chunks)
    def _(i):
        j = partner(my_chunk, spread(lax.rem(i + chunks - 1, chunks), chunks), chunks)
        for p in range(per):
            r_local(j * per + p).wait()
        h0, h1 = hot(j)
        one = (h0 | h1).astype(F32).astype(BF16)
        acc[...] += dot(one, rr[rows_of(j, chunk), :], 0, 0)

    for h in range(heads):
        dx[:, pl.ds(h * sub, sub)] = acc[pl.ds(h * tokens, tokens), :].astype(BF16)

    for s, (out, own, got, sums) in enumerate(((dwo, po, tpo, rpo), (dwi, pi, tpi, rpi))):
        twin_copy(s, mine, row).wait_recv()
        out[0] = own[mine].astype(F32) + got[row].astype(F32)

        @pl.loop(1, halves)
        def _(i):
            t = lax.rem(row + i, halves)
            row_got(s, t).wait()
            out[0] = out[0] + sums[t].astype(F32)

    @pl.loop(1, groups)
    def _(i):
        peer = lax.rem(me + i, groups)
        xg_copy(0, peer).wait_send()
        xg_copy(1, peer).wait_send()
        r_copy(peer).wait_send()

    for s in range(2):

        @pl.loop(0, halves)
        def _(i):
            twin_copy(s, 2 * i + (1 - side), i).wait_send()

        @pl.loop(1, halves)
        def _(i):
            row_copy(s, lax.rem(row + i, halves)).wait_send()


def plain_call(
    sub_inputs,
    out_grads,
    expert_outputs,
    combine_weights,
    expert_ids,
    slot_ids,
    expert_input_weight,
    expert_output_weight,
):
    tokens, heads, top = expert_ids.shape
    _, sub, ff = expert_input_weight.shape
    groups = lax.axis_size("expert")
    replicas = lax.axis_size("dp")
    cap = top * heads * tokens // groups
    kept = slot_ids >= 0
    target = jnp.where(kept, expert_ids * cap + slot_ids, -1)
    target = target.transpose(2, 1, 0).reshape(top, heads * tokens)
    weight = combine_weights.transpose(2, 1, 0).reshape(top, heads * tokens)
    slots = groups * cap
    part = sub // replicas
    part_out = ff // replicas
    dims = (groups, replicas, cap, heads, tokens, sub, ff)
    any_spec = pl.BlockSpec(memory_space=pltpu.HBM)
    vmem = pl.BlockSpec(memory_space=pltpu.VMEM)
    dma = pltpu.SemaphoreType.DMA
    d_inputs, dw_in, dw_out, gate_dots = pl.pallas_call(
        functools.partial(kernel, dims),
        out_shape=(
            jax.ShapeDtypeStruct((tokens, heads * sub), BF16),
            jax.ShapeDtypeStruct((1, part, ff), F32),
            jax.ShapeDtypeStruct((1, part_out, sub), F32),
            jax.ShapeDtypeStruct((heads, tokens, top), F32),
        ),
        in_specs=[vmem, vmem, any_spec, any_spec, any_spec, any_spec, any_spec],
        out_specs=(vmem, vmem, vmem, vmem),
        scratch_shapes=[
            pltpu.VMEM((heads * tokens, sub), BF16),
            pltpu.VMEM((heads * tokens, sub), BF16),
            pltpu.VMEM((sub, ff), BF16),
            pltpu.VMEM((ff, sub), BF16),
            pltpu.VMEM((slots, sub), BF16),
            pltpu.VMEM((slots, sub), BF16),
            pltpu.VMEM((slots, sub), BF16),
            pltpu.VMEM((slots, sub), BF16),
            pltpu.VMEM((slots, sub), BF16),
            pltpu.VMEM((slots, sub), BF16),
            pltpu.VMEM((slots, ff), BF16),
            pltpu.VMEM((slots, ff), BF16),
            pltpu.VMEM((heads * tokens, sub), F32),
            pltpu.VMEM((replicas, part_out, sub), BF16),
            pltpu.VMEM((replicas, part, ff), BF16),
            *[pltpu.VMEM((replicas // 2, part_out, sub), BF16), pltpu.VMEM((replicas // 2, part, ff), BF16)] * 3,
            pltpu.VMEM((tokens, heads, top, sub), BF16),
            dma((2 * heads + 3,)),
            dma((2, groups)),
            dma((2, groups)),
            dma((groups,)),
            dma((groups,)),
            *[dma((2, replicas // 2))] * 4,
        ],
        compiler_params=pltpu.CompilerParams(
            collective_id=0, has_side_effects=True, vmem_limit_bytes=60 * 1024 * 1024
        ),
        cost_estimate=pl.CostEstimate(flops=20 * 10**9, bytes_accessed=2**24, transcendentals=0),
    )(target, weight, sub_inputs, out_grads, expert_input_weight, expert_output_weight, expert_outputs)
    d_gates = jnp.where(kept, gate_dots.transpose(1, 0, 2), jnp.float32(0.0))
    return (d_inputs, d_gates, dw_in, dw_out)


PIECES = 2
WEIGHT_PIECES = 4


def paired(
    dims,
    ids_hbm, slot_hbm, cw_hbm, x_hbm, g_hbm, win_hbm, wout_hbm, eo_hbm,
    dx, dwi, dwo, dg,
    ids, slot, cw, tgt, xs, gs, win, wout, sx, sg, rx, rg, rs, rr, hb, fb, acc, po, pi, tpo, tpi, so, si, rpo, rpi,
    cpo, cpi, gpo, gpi, ev, gates,
    load_sem, xg_send, xg_recv, r_send, r_recv, wz_send, wz_recv, wt_send, wt_recv, wy_send, wy_recv,
    t_send, t_recv, y_send, y_recv, c_send, c_recv, a_send, a_recv,
):
    groups, replicas, cap, heads, tokens, sub, ff = dims
    tile = 256
    me = lax.axis_index("expert")
    mine = lax.axis_index("dp")
    half = groups // 2
    halves = replicas // 2
    low = lax.rem(me, half)
    base = me - low
    opposite = lax.rem(me + half, groups)
    inner = lax.rem(me // half + low // (half // 2), 2)
    outer = inner == 0
    first, second = inner, 1 - inner
    row, side = mine // 2, mine % 2
    twin = row * 2 + (1 - side)
    near = range(1, half)

    def rows_of(index, size):
        return pl.ds(pl.multiple_of(index * size, size), size)

    def fixed(f, s, n=1):
        return pl.ds(pl.multiple_of((f * (half + 1) + s) * cap, cap), n * cap)

    def landed(ref, sem):
        return pltpu.make_async_copy(ref, ref, sem)

    def remote(src, dst, send, recv, where):
        return pltpu.make_async_remote_copy(
            src_ref=src, dst_ref=dst, send_sem=send, recv_sem=recv, device_id=where, device_id_type=MESH
        )

    loads = []
    for h in range(heads):
        for s, (src, dst) in enumerate(((x_hbm, xs), (g_hbm, gs))):
            loads.append(
                pltpu.make_async_copy(
                    src.at[:, pl.ds(h * sub, sub)], dst.at[pl.ds(h * tokens, tokens)], load_sem.at[2 * h + s]
                )
            )
    wloads = [
        pltpu.make_async_copy(win_hbm.at[0], win.at[0], load_sem.at[2 * heads]),
        pltpu.make_async_copy(wout_hbm.at[0], wout.at[0], load_sem.at[2 * heads + 1]),
    ]
    eload = pltpu.make_async_copy(eo_hbm, ev, load_sem.at[2 * heads + 2])
    tables = [
        pltpu.make_async_copy(src, dst, load_sem.at[2 * heads + 3 + i])
        for i, (src, dst) in enumerate(((ids_hbm, ids), (slot_hbm, slot), (cw_hbm, cw)))
    ]
    barrier = pltpu.get_barrier_semaphore()
    for s in near:
        pl.semaphore_signal(
            barrier, inc=1, device_id={"expert": base + partner(low, s, half)}, device_id_type=MESH
        )
    pl.semaphore_signal(barrier, inc=1, device_id={"expert": opposite}, device_id_type=MESH)
    for i in range(1, replicas):
        pl.semaphore_signal(barrier, inc=1, device_id={"dp": lax.rem(mine + i, replicas)}, device_id_type=MESH)
    turn = half // 2
    across = lax.rem(base + partner(low, turn, half) + half, groups)

    @pl.when(inner == 1)
    def _():
        pl.semaphore_signal(barrier, inc=1, device_id={"expert": across}, device_id_type=MESH)
    for c in tables + loads + wloads + [eload]:
        c.start()

    def owner(s):
        return base + partner(low, s, half)

    def part_of(m, quarter, n):
        size = (sub, ff)[m] // replicas // WEIGHT_PIECES
        return rows_of(quarter * WEIGHT_PIECES + n, size)

    def held(m, quarter, n):
        return (win, wout)[m].at[1, part_of(m, quarter, n)]

    def rows_held(m, quarters):
        return (win, wout)[m].at[1, pl.ds(0, quarters * ((sub, ff)[m] // replicas))]

    def w_cross(m, n):
        return remote(
            (win_hbm, wout_hbm)[m].at[0, part_of(m, mine, n)], held(m, mine, n),
            wz_send.at[m], wz_recv.at[m, n], {"expert": opposite},
        )

    def w_twin(m, n, t):
        ref = held(m, 2 * t + side, n)
        return remote(ref, ref, wt_send.at[m], wt_recv.at[m], {"dp": twin})

    def w_row(m, n, t):
        ref = held(m, mine, n)
        return remote(ref, ref, wy_send.at[m], wy_recv.at[m, n, row], {"dp": 2 * t + side})

    def xg_copy(s, f, step):
        src, dst = ((sx, rx), (sg, rg))[s]
        return remote(
            src.at[fixed(f, step)], dst.at[fixed(f, step)],
            xg_send.at[s, f, step], xg_recv.at[s, f, step], {"expert": owner(step)},
        )

    def across_copy(s):
        src, dst = ((sx, rx), (sg, rg))[s]
        return remote(
            src.at[fixed(1, turn)], dst.at[fixed(0, half)], a_send.at[s], a_recv.at[s], {"expert": across}
        )

    def across_reply():
        return remote(
            rs.at[fixed(0, half)], rr.at[fixed(1, turn)], a_send.at[2], r_recv.at[1, turn], {"expert": across}
        )

    def r_copy(f, step):
        return remote(
            rs.at[fixed(f, step)], rr.at[fixed(f, step)],
            r_send.at[f, step], r_recv.at[f, step], {"expert": owner(step)},
        )

    def twin_copy(f, s, q, t):
        src, dst = ((po, tpo), (pi, tpi))[s]
        return remote(src.at[f, q], dst.at[f, t], t_send.at[s], t_recv.at[f, s, t], {"dp": twin})

    def cut(s, n):
        size = (dwo, dwi)[s].shape[1] // PIECES
        return pl.ds(n * size, size)

    def row_copy(f, s, t, n):
        src, dst = ((so, rpo), (si, rpi))[s]
        return remote(
            src.at[f, t, cut(s, n)], dst.at[f, row, cut(s, n)],
            y_send.at[s], y_recv.at[f, s, n, row], {"dp": 2 * t + side},
        )

    def cross_copy(s, n):
        src, dst = ((cpo, gpo), (cpi, gpi))[s]
        return remote(
            src.at[cut(s, n)], dst.at[cut(s, n)], c_send.at[s], c_recv.at[s, n], {"expert": opposite}
        )

    pieces = [(m, n) for m in range(2) for n in range(WEIGHT_PIECES)]

    @pl.when(outer)
    def _():
        pl.semaphore_wait(barrier, half + replicas - 1)
        for m, n in pieces:
            w_cross(m, n).start()

    for c in tables:
        c.wait()
    tgt[...] = jnp.where(slot[...] >= 0, ids[...] * cap + slot[...], -1)

    def hot(f, step):
        first = lax.rem(owner(step) + f * half, groups) * cap
        slots = lax.broadcasted_iota(jnp.int32, (cap, tgt.shape[1]), 0) + first
        return tgt[0:1, :] == slots, tgt[1:2, :] == slots

    def gather(f, step, out_x, out_g):
        h0, h1 = hot(f, step)
        one = (h0 | h1).astype(F32).astype(BF16)
        w = jnp.sum(jnp.where(h0, cw[0:1, :], 0.0) + jnp.where(h1, cw[1:2, :], 0.0), axis=1, keepdims=True)
        rows = fixed(f, step)
        out_x[rows, :] = dot(one, xs[...], 1, 0).astype(BF16)
        out_g[rows, :] = (dot(one, gs[...], 1, 0) * w).astype(BF16)

    for c in loads:
        c.wait()
    far_steps = range(half // 2, half)

    def send(f, step):
        xg_copy(0, f, step).start()
        xg_copy(1, f, step).start()

    @pl.loop(half // 2, half)
    def _(step):
        gather(second, step, sx, sg)

    @pl.when(inner == 1)
    def _():
        pl.semaphore_wait(barrier, half + replicas)

    for step in far_steps:
        send(second, step)

    @pl.loop(0, 2)
    def _(i):
        f = first + i * (second - first)

        @pl.loop(1, half // 2)
        def _(step):
            gather(f, step, sx, sg)
            send(f, step)

        gather(f, 0, rx, rg)

    @pl.loop(half // 2, half)
    def _(step):
        gather(first, step, sx, sg)
        pl.when(outer)(lambda: send(first, step))

    eload.wait()
    span = 16
    lane = lax.broadcasted_iota(jnp.int32, (span, gates.shape[1]), 1)

    @pl.loop(0, tokens // span)
    def _(b):
        found = jnp.zeros((span, gates.shape[1]), F32)
        for h in range(heads):
            grads = gs[rows_of(h * (tokens // span) + b, span), :].astype(F32)
            terms = ev[rows_of(b, span), h].astype(F32) * grads[:, None, :]
            sums = jnp.sum(terms, axis=-1)
            for k in range(2):
                found = jnp.where(lane == 2 * h + k, sums[:, k : k + 1], found)
        gates[rows_of(b, span), :] = found

    turned = gates[...].T
    for h in range(heads):
        cols = pl.ds(h * tokens, tokens)
        dg[:, cols] = jnp.where(slot[:, cols] >= 0, turned[2 * h : 2 * h + 2, :], 0.0)

    for c in wloads:
        c.wait()

    others = [lax.rem(row + i, halves) for i in range(1, halves)]

    def from_rows(m, n):
        for t in others:
            landed(held(m, 2 * t + side, n), wy_recv.at[m, n, t]).wait()
            w_twin(m, n, t).start()

    def rows_out(f, s, t, parts=range(PIECES)):
        for n in parts:
            row_copy(f, s, t, n).start()

    def weights():
        before = None
        for m, n in pieces:
            landed(held(m, mine, n), wz_recv.at[m, n]).wait()
            w_twin(m, n, row).start()
            for t in others:
                w_row(m, n, t).start()
            if before is not None:
                from_rows(*before)
            before = (m, n)
            if before == pieces[-2]:

                @pl.when(inner == 1)
                def _():
                    for piece in pieces:
                        w_cross(*piece).start()

            if before == pieces[-1]:

                @pl.when(outer)
                def _():
                    for t in others:
                        rows_out(first, 0, t)

        from_rows(*before)
        for m in range(2):
            landed(rows_held(m, halves), wt_recv.at[m]).wait()

    def arrive(f, s, n):
        for step in range(s, s + n):
            if step > 0:
                for v, dst in enumerate((rx, rg)):
                    landed(dst.at[fixed(f, step)], xg_recv.at[v, f, step]).wait()

    def arrive_across():
        for v, dst in enumerate((rx, rg)):
            landed(dst.at[fixed(0, half)], a_recv.at[v]).wait()

    def process(f, s, n):
        rows = fixed(f, s, n)
        for c in range(ff // tile):
            cols = pl.ds(c * tile, tile)
            z = dot(rx[rows, :], win[f, :, cols], 1, 0)
            e = dot(rg[rows, :], wout[f, cols, :], 1, 1)
            zz = z * z
            t = jnp.tanh(ROOT * (z + CUBE * (zz * z)))
            part = 0.5 * (1.0 + t)
            hb[rows, cols] = (z * part).astype(BF16)
            slope = part + 0.5 * z * (1.0 - t * t) * (ROOT * (1.0 + 3.0 * CUBE * zz))
            fb[rows, cols] = (e * slope).astype(BF16)
        for c in range(sub // tile):
            cols = pl.ds(c * tile, tile)
            back = dot(fb[rows, :], win[f, cols, :], 1, 1).astype(BF16)
            for step in range(s, s + n):
                piece = back[(step - s) * cap : (step - s + 1) * cap]
                if step == 0:
                    rr[fixed(f, step), cols] = piece
                else:
                    rs[fixed(f, step), cols] = piece

    def reply(f, s, n):
        for step in range(s, s + n):
            if step > 0:
                r_copy(f, step).start()

    block = dwo.shape[1]

    def product(f, q, n):
        cols = rows_of(q, block)
        rows = fixed(f, 0, n)
        po[f, q] = dot(hb[rows, cols], rg[rows, :], 0, 0).astype(BF16)
        pi[f, q] = dot(rx[rows, cols], fb[rows, :], 0, 0).astype(BF16)

    def exchange(f, early, n):
        @pl.loop(0, halves)
        def _(i):
            t = lax.rem(row + 1 + i, halves)
            product(f, 2 * t + (1 - side), n)
            twin_copy(f, 0, 2 * t + (1 - side), t).start()
            twin_copy(f, 1, 2 * t + (1 - side), t).start()
            product(f, 2 * t + side, n)

            @pl.when(t != row)
            def _():
                for s, (own, got, out) in enumerate(((po, tpo, so), (pi, tpi, si))):
                    landed(got.at[f, t], t_recv.at[f, s, t]).wait()
                    out[f, t] = (own[f, 2 * t + side].astype(F32) + got[f, t].astype(F32)).astype(BF16)
                    if early:
                        pl.when(inner == 1)(lambda s=s: rows_out(f, s, t))
                    else:
                        rows_out(f, s, t)

    def total(f, s, n):
        own, got, sums = ((po, tpo, rpo), (pi, tpi, rpi))[s]
        if n == 0:
            landed(got.at[f, row], t_recv.at[f, s, row]).wait()
        out = own[f, mine, cut(s, n)].astype(F32) + got[f, row, cut(s, n)].astype(F32)
        for t in others:
            landed(sums.at[f, t, cut(s, n)], y_recv.at[f, s, n, t]).wait()
            out = out + sums[f, t, cut(s, n)].astype(F32)
        return out

    def scatter(f, s, n, start=False):
        ones = []
        for step in range(s, s + n):
            if step > 0:
                landed(rr.at[fixed(f, step)], r_recv.at[f, step]).wait()
            h0, h1 = hot(f, step)
            ones.append((h0 | h1).astype(F32).astype(BF16))
        more = dot(jnp.concatenate(ones, axis=0), rr[fixed(f, s, n), :], 0, 0)
        acc[...] = more if start else acc[...] + more

    def pass_on(s, parts):
        out = (cpo, cpi)[s]
        for n in parts:
            out[cut(s, n)] = total(1, s, n).astype(BF16)
            cross_copy(s, n).start()

    near_part, far_part = (0, turn), (turn, turn)
    last_part = (turn + 1, turn - 1)

    @pl.when(outer)
    def _():
        rx[fixed(1, turn), :] = jnp.zeros((cap, sub), BF16)
        rg[fixed(1, turn), :] = jnp.zeros((cap, sub), BF16)

    pl.when(inner == 1)(weights)
    arrive(first, *near_part)
    process(first, *near_part)
    reply(first, *near_part)
    arrive(first, *far_part)

    @pl.when(inner == 1)
    def _():
        for step in far_steps[1:]:
            send(first, step)
        across_copy(0).start()
        across_copy(1).start()

    process(first, *far_part)
    pl.when(outer)(lambda: reply(first, *far_part))
    exchange(first, True, half)
    pl.when(outer)(weights)
    arrive(second, *near_part)
    process(second, *near_part)
    reply(second, *near_part)

    @pl.when(inner == 1)
    def _():
        pass_on(0, (0,))
        for step in far_steps[1:]:
            xg_copy(0, first, step).wait_send()
            xg_copy(1, first, step).wait_send()
        arrive_across()
        process(0, half, 1)
        across_reply().start()
        pass_on(0, range(1, PIECES))
        reply(first, *far_part)
        arrive(second, turn, 1)

    arrive(second, *last_part)
    process(second, *far_part)

    @pl.when(inner == 1)
    def _():
        pass_on(1, range(PIECES))
        reply(second, turn, 1)

    reply(second, *last_part)
    pl.when(inner == 1)(lambda: exchange(0, False, half + 1))

    @pl.when(outer)
    def _():
        exchange(1, False, half)
        for t in others:
            rows_out(first, 1, t)
        pass_on(0, range(PIECES))
        pass_on(1, range(PIECES))

    scatter(first, 0, half // 2, True)
    scatter(second, 0, half // 2)

    for step in far_steps:
        xg_copy(0, second, step).wait_send()
        xg_copy(1, second, step).wait_send()

    @pl.when(outer)
    def _():
        for step in far_steps:
            xg_copy(0, first, step).wait_send()
            xg_copy(1, first, step).wait_send()

    @pl.when(inner == 1)
    def _():
        across_copy(0).wait_send()
        across_copy(1).wait_send()

    for f in range(2):
        for step in near:
            if step < turn:
                xg_copy(0, f, step).wait_send()
                xg_copy(1, f, step).wait_send()
    for m in range(2):
        landed(rows_held(m, 1), wz_send.at[m]).wait()
        landed(rows_held(m, halves), wt_send.at[m]).wait()
        landed(rows_held(m, halves - 1), wy_send.at[m]).wait()
        landed((po, pi)[m].at[0], t_send.at[m]).wait()

    scatter(second, half // 2, half // 2)
    for s, out in enumerate((dwo, dwi)):
        for n in range(PIECES):
            out[0, cut(s, n)] = total(0, s, n)
    scatter(first, half // 2, half // 2)
    for h in range(heads):
        dx[:, pl.ds(h * sub, sub)] = acc[pl.ds(h * tokens, tokens), :].astype(BF16)

    @pl.when(inner == 1)
    def _():
        across_reply().wait_send()
        r_copy(second, turn).wait_send()

    r_copy(first, turn).wait_send()
    for f in range(2):
        for step in near:
            if step != turn:
                r_copy(f, step).wait_send()
    for s in range(2):
        landed((po, pi)[s].at[0, pl.ds(0, 2 * (halves - 1))], y_send.at[s]).wait()
    for s, (out, got) in enumerate(((dwo, gpo), (dwi, gpi))):
        for n in range(PIECES):
            landed(got.at[cut(s, n)], c_recv.at[s, n]).wait()
            out[0, cut(s, n)] = out[0, cut(s, n)] + got[cut(s, n)].astype(F32)

    for s in range(2):
        landed((cpo, cpi)[s], c_send.at[s]).wait()


def put_out(*refs):
    count = len(refs) // 2
    sems = refs[-1]
    copies = [pltpu.make_async_copy(refs[i], refs[count + i], sems.at[i]) for i in range(count)]
    for c in copies:
        c.start()
    for c in copies:
        c.wait()


def paired_call(
    sub_inputs,
    out_grads,
    expert_outputs,
    combine_weights,
    expert_ids,
    slot_ids,
    expert_input_weight,
    expert_output_weight,
):
    tokens, heads, top = expert_ids.shape
    _, sub, ff = expert_input_weight.shape
    groups = lax.axis_size("expert")
    replicas = lax.axis_size("dp")
    cap = top * heads * tokens // groups

    def flat(a):
        return a.transpose(2, 1, 0).reshape(top, heads * tokens)

    slots = (groups + 1) * cap
    half = groups // 2
    halves = replicas // 2
    part = sub // replicas
    part_out = ff // replicas
    dims = (groups, replicas, cap, heads, tokens, sub, ff)
    any_spec = pl.BlockSpec(memory_space=pltpu.HBM)
    vmem = pl.BlockSpec(memory_space=pltpu.VMEM)
    dma = pltpu.SemaphoreType.DMA
    rows = heads * tokens
    shapes = (
        ((tokens, heads * sub), BF16),
        ((1, part, ff), F32),
        ((1, part_out, sub), F32),
        ((top, heads * tokens), F32),
    )
    results = pl.pallas_call(
        functools.partial(paired, dims),
        out_shape=tuple(pltpu.VMEM(shape, kind) for shape, kind in shapes),
        in_specs=[any_spec] * 8,
        out_specs=(vmem, vmem, vmem, vmem),
        scratch_shapes=[
            pltpu.VMEM((top, rows), jnp.int32),
            pltpu.VMEM((top, rows), jnp.int32),
            pltpu.VMEM((top, rows), F32),
            pltpu.VMEM((top, rows), jnp.int32),
            pltpu.VMEM((rows, sub), BF16),
            pltpu.VMEM((rows, sub), BF16),
            pltpu.VMEM((2, sub, ff), BF16),
            pltpu.VMEM((2, ff, sub), BF16),
            *[pltpu.VMEM((slots, sub), BF16)] * 6,
            pltpu.VMEM((slots, ff), BF16),
            pltpu.VMEM((slots, ff), BF16),
            pltpu.VMEM((rows, sub), F32),
            pltpu.VMEM((2, replicas, part_out, sub), BF16),
            pltpu.VMEM((2, replicas, part, ff), BF16),
            *[pltpu.VMEM((2, halves, part_out, sub), BF16), pltpu.VMEM((2, halves, part, ff), BF16)] * 3,
            *[pltpu.VMEM((part_out, sub), BF16), pltpu.VMEM((part, ff), BF16)] * 2,
            pltpu.VMEM((tokens, heads, top, sub), BF16),
            pltpu.VMEM((tokens, 128), F32),
            dma((2 * heads + 6,)),
            *[dma((2, 2, half))] * 2,
            *[dma((2, half))] * 2,
            dma((2,)),
            dma((2, WEIGHT_PIECES)),
            dma((2,)),
            dma((2,)),
            dma((2,)),
            dma((2, WEIGHT_PIECES, halves)),
            dma((2,)),
            dma((2, 2, halves)),
            dma((2,)),
            dma((2, 2, PIECES, halves)),
            dma((2,)),
            dma((2, PIECES)),
            dma((3,)),
            dma((2,)),
        ],
        compiler_params=pltpu.CompilerParams(
            collective_id=0, has_side_effects=True, vmem_limit_bytes=59 * 1024 * 1024
        ),
        cost_estimate=pl.CostEstimate(flops=20 * 10**9, bytes_accessed=2**24, transcendentals=0),
    )(
        flat(expert_ids), flat(slot_ids), flat(combine_weights),
        sub_inputs, out_grads, expert_input_weight, expert_output_weight, expert_outputs,
    )
    d_inputs, dw_in, dw_out, gate_dots = pl.pallas_call(
        put_out,
        out_shape=tuple(jax.ShapeDtypeStruct(shape, kind) for shape, kind in shapes),
        in_specs=[vmem] * len(shapes),
        out_specs=(any_spec,) * len(shapes),
        scratch_shapes=[dma((len(shapes),))],
        compiler_params=pltpu.CompilerParams(vmem_limit_bytes=1024 * 1024),
    )(*results)
    d_gates = gate_dots.reshape(top, heads, tokens).transpose(2, 1, 0)
    return (d_inputs, d_gates, dw_in, dw_out)


def on_device(*args):
    tokens, heads, top = args[4].shape
    _, sub, ff = args[6].shape
    groups = lax.axis_size("expert")
    replicas = lax.axis_size("dp")
    cap = top * heads * tokens // groups
    half = groups // 2
    fits = half >= 4 and half & (half - 1) == 0 and replicas % 2 == 0 and cap % 128 == 0 and tokens % 128 == 0
    tokens_cross = half * replicas * cap * 3 * sub
    weights_cross = 4 * sub * ff
    if fits and weights_cross < tokens_cross:
        return paired_call(*args)
    return plain_call(*args)


def solution(mesh):
    rows = P(("expert", "dp"), None)
    table = P(("expert", "dp"), None, None)
    return jax.shard_map(
        on_device,
        mesh=mesh,
        in_specs=(
            rows,
            rows,
            P(("expert", "dp"), None, None, None),
            table,
            table,
            table,
            P("expert", None, None),
            P("expert", None, None),
        ),
        out_specs=(rows, table, P("expert", "dp", None), P("expert", "dp", None)),
        check_vma=False,
    )
```
